32 devices in a mesh: lon: 4 (over y, x), lat: 8 (over z, core).
Axes of the slice: x: 2, y: 2, z: 4, core: 2. Of those that a mesh axis runs over, the one named last changes fastest.
Arguments:
- spectrum: float32 [32, 512, 648], P('lon', 'lat'), may hold values from 0.01 to 1
- sea_mask: int32 [32, 512], P('lon', 'lat'), may hold values from 0 to 1, as said below
- ice_flags: int32 [32, 512], P('lon', 'lat'), may hold values 0 or 1
- wind_forcing: float32 [32, 512], P('lon', 'lat'), may hold values from 0.1 to 1.5
- group_speed: float32 [18], replicated, may hold values from 0.3 to 1
- coupling: bfloat16 [648, 648], replicated, may hold values from -0.25 to 0.25
Outputs:
- field: float32 [32, 512, 648], P('lon', 'lat')
The draws below stay inside these ranges and needn't reach their ends.
Inputs may be any that keep to these rules, and one draw needn't show every extreme that they name: `sea_mask`: each device's block of 8 x 64 cells holds at most 384 sea cells and at least 128; in every draw some block holds exactly 384.
All inputs are finite; a program needn't handle non-finite values. No bound on the sum of `ice_flags` on one device may be relied on, other than what follows from the above.
Results may differ from the reference program's by a relative error of at most 0.00079.
Values sent between devices are 32-bit elements; how exact they have to be, the bound alone decides.
No kernel may reach another device: no remote copies, remote signals or barrier semaphores. Data moves between devices by JAX's collectives and lax.ppermute only.
A program may use at most 64 MiB of HBM per device.

```python
import math
import jax
import jax.numpy as jnp

DIRS = 36
FREQS = 18
BINS = 648
CX = 8
CY = 64
SEA_DEV = 384
STEPS = 4
NX = 32
NY = 512


def draw_sea_mask(key, part):
    blocks_x = NX // CX
    blocks_y = NY // CY
    cells = CX * CY
    blocks = blocks_x * blocks_y
    key_count, key_pick, key_order = jax.random.split(jax.random.fold_in(key, 11), 3)
    counts = jax.random.randint(key_count, (blocks,), SEA_DEV // 3, SEA_DEV + 1)
    chosen = jax.random.randint(key_pick, (), 0, blocks)
    counts = counts.at[chosen].set(SEA_DEV)
    scores = jax.random.randint(key_order, (blocks, cells), 0, 2 ** 20) * cells + jnp.arange(cells, dtype=jnp.int32)[None, :]
    order = jnp.argsort(scores, axis=1, stable=True)
    ranks = jnp.argsort(order, axis=1, stable=True)
    flags = (ranks < counts[:, None]).astype(jnp.int32)
    flags = flags.reshape(blocks_x, blocks_y, CX, CY).transpose(0, 2, 1, 3)
    return flags.reshape(NX, NY)


def set_ends(array, key, low, largest):
    dims = array.shape
    index_at = [jax.random.randint(jax.random.fold_in(key, axis), (), 0, dims[axis]) for axis in range(len(dims))]
    array = array.at[tuple(index_at)].set(low)
    longest = dims.index(max(dims))
    index_at[longest] = (index_at[longest] + 1) % dims[longest]
    return array.at[tuple(index_at)].set(largest)


def levels(key, shape, cuts, least, largest):
    gain = 1.0
    for dim, parts in cuts:
        heights = jax.random.uniform(jax.random.fold_in(jax.random.fold_in(key, 6), dim), (parts,), jnp.float32, least / len(cuts), largest / len(cuts))
        gain = gain * jnp.repeat(jnp.exp(heights), shape[dim] // parts).reshape((-1,) + (1,) * (len(shape) - 1 - dim))
    return gain


def noise(stream_key, extent, scale, limit, kind=jnp.bfloat16):
    return jnp.clip(scale * jax.random.normal(stream_key, extent, jnp.float32), -limit, limit).astype(kind)


def setup_inputs(seed: int = 0) -> dict:
    arg_keys = jax.random.split(jax.random.key(seed), 7)
    spectrum = jnp.clip(jnp.exp(math.log(1.0) - 4.6051702 * jax.random.uniform(arg_keys[0], (NX, NY, BINS), jnp.float32) ** levels(arg_keys[0], (NX, NY, BINS), ((0, 4), (1, 8)), -0.2, 0.2)), 0.01, 1.0)
    sea_mask = draw_sea_mask(jax.random.fold_in(arg_keys[6], 71), 0)
    ice_flags = set_ends((jax.random.randint(arg_keys[2], (NX, NY), 0, 4) < 1).astype(jnp.int32), jax.random.fold_in(arg_keys[2], 1), 0, 1)
    wind_forcing = jnp.clip(jnp.exp(math.log(1.5) - 2.7080502 * jax.random.uniform(arg_keys[3], (NX, NY), jnp.float32) ** levels(arg_keys[3], (NX, NY), ((0, 4), (1, 8)), -0.2, 0.2)), 0.1, 1.5)
    group_speed = jnp.clip(jax.random.uniform(arg_keys[4], (FREQS,), jnp.float32, 0.3, 1.0), 0.3, 1.0)
    coupling = noise(arg_keys[5], (BINS, BINS), BINS ** -0.5, 0.25)
    return {"spectrum": spectrum, "sea_mask": sea_mask, "ice_flags": ice_flags, "wind_forcing": wind_forcing, "group_speed": group_speed, "coupling": coupling}


time_step = 0.2
dissipation = 0.5


def speed_tables(rows, total_rows, group_speed, dirs):
    theta = (jnp.arange(dirs).astype(jnp.float32) + 0.5) * (2.0 * math.pi / dirs)
    latitude = (-60.0 + 120.0 * (rows.astype(jnp.float32) + 0.5) / total_rows) * (math.pi / 180.0)
    scaled = jnp.outer(jnp.cos(theta), group_speed).reshape(-1)
    along_x = (0.225 * scaled)[None, :] / jnp.cos(latitude)[:, None]
    along_y = 0.45 * jnp.outer(jnp.sin(theta), group_speed).reshape(-1)
    return along_x, along_y


def upwind(field, west, east, south, north, along_x, along_y):
    speed_x = along_x[None]
    result = field - jnp.maximum(speed_x, 0.0) * (field - west) - jnp.minimum(speed_x, 0.0) * (east - field)
    return result - jnp.maximum(along_y, 0.0) * (field - south) - jnp.minimum(along_y, 0.0) * (north - field)


def sources(advected, wind_forcing, ice_flags, coupling):
    shape = advected.shape
    energy = jnp.mean(advected, axis=-1, keepdims=True)
    flat = advected.reshape(-1, shape[-1]).astype(jnp.bfloat16)
    transfer = jnp.dot(flat, coupling, preferred_element_type=jnp.float32).reshape(shape)
    forcing = (wind_forcing * (1.0 - ice_flags.astype(jnp.float32)))[..., None]
    return advected + time_step * (forcing * advected + transfer - dissipation * energy * advected)


def reference(spectrum, sea_mask, ice_flags, wind_forcing, group_speed, coupling):
    sea = sea_mask.astype(jnp.float32)[..., None]
    along_x, along_y = speed_tables(jnp.arange(NY), NY, group_speed, DIRS)
    field = spectrum * sea
    for step in range(STEPS):
        west = jnp.roll(field, 1, axis=0)
        east = jnp.roll(field, -1, axis=0)
        edge = jnp.zeros_like(field[:, :1])
        south = jnp.concatenate([edge, field[:, :-1]], axis=1)
        north = jnp.concatenate([field[:, 1:], edge], axis=1)
        advected = upwind(field, west, east, south, north, along_x, along_y)
        field = sources(advected, wind_forcing, ice_flags, coupling) * sea
    return field
```

```python
import functools
import math

import jax
import jax.numpy as jnp
import numpy as np
from jax import lax
from jax.experimental import pallas as pl
from jax.experimental.pallas import tpu as pltpu
from jax.sharding import PartitionSpec as P

DIRS = 36
STEPS = 4
LANES = 128
DEPTH = 4

time_step = 0.2
dissipation = 0.5

VMEM = pltpu.VMEM
SMEM = pltpu.SMEM


def swap_pairs(size, first, wrap):
    pairs = []
    for i in range(first, size, 2):
        j = i + 1
        if j >= size:
            if not wrap:
                continue
            j = j % size
        pairs += [(i, j), (j, i)]
    return pairs


def lane_tiles(bins):
    return pl.cdiv(bins, LANES)


def lanes_of(tile):
    return slice(tile * LANES, (tile + 1) * LANES)


def lane_index(shape):
    return lax.broadcasted_iota(jnp.int32, shape, 1)


def row_index(shape):
    return lax.broadcasted_iota(jnp.int32, shape, 0)


def eastward(bins, tile, shape):
    bin_here = lane_index(shape) + tile * LANES
    quarter = bins // 4
    return (bin_here < quarter) | (bin_here >= bins - quarter)


def northward(bins, tile, shape):
    return lane_index(shape) + tile * LANES < bins // 2


def kinds(bins, tile, test):
    low, high = tile * LANES, min((tile + 1) * LANES, bins)
    return {bool(test(b)) for b in range(low, high)}


def is_east(bins):
    return lambda b: b < bins // 4 or b >= bins - bins // 4


def is_north(bins):
    return lambda b: b < bins // 2


def upwind_lat(f, bins, tile):
    shape = f.shape
    rows = shape[0]
    found = kinds(bins, tile, is_north(bins))
    south = pltpu.roll(f, 1, 0) if True in found else None
    north = pltpu.roll(f, rows - 1, 0) if False in found else None
    if south is None:
        return north
    if north is None:
        return south
    return jnp.where(northward(bins, tile, shape), south, north)


def advect(f, across, stay, go_x, go_y, bins, tile):
    along = upwind_lat(f, bins, tile)
    return stay * f + go_x * across + go_y * along


def pack_half(tiles, west_edge, bins):
    quarter = bins // 4
    split = quarter - LANES
    shape = tiles[0].shape
    lane = lane_index(shape)
    last = jnp.where(lane < split, tiles[1], jnp.where(lane >= LANES // 2, tiles[3], pltpu.roll(tiles[5], split, 1)))
    return (
        jnp.where(west_edge, tiles[2], tiles[0]),
        jnp.where(west_edge, tiles[1], tiles[4]),
        jnp.where(west_edge, tiles[3], last),
    )


def across_edge(halo, inner, west_edge, bins):
    quarter = bins // 4
    split = quarter - LANES
    shape = inner[0].shape
    pick = [eastward(bins, tile, shape) == west_edge for tile in (1, 3)]
    return (
        jnp.where(west_edge, halo[0], inner[0]),
        jnp.where(pick[0], jnp.where(west_edge, halo[2], halo[1]), inner[1]),
        jnp.where(west_edge, inner[2], halo[0]),
        jnp.where(pick[1], halo[2], inner[3]),
        jnp.where(west_edge, halo[1], inner[4]),
        jnp.where(west_edge, pltpu.roll(halo[2], LANES - split, 1), inner[5]),
    )


def west_flag(second):
    odd = lax.rem(lax.axis_index("lon"), 2)
    return (1 - odd if second else odd) == 1


def south_flag(second):
    odd = lax.rem(lax.axis_index("lat"), 2)
    return (1 - odd if second else odd) == 1


def read_tile(ref, where, bins, tile):
    low, high = tile * LANES, min((tile + 1) * LANES, bins)
    value = ref[where + (slice(None), slice(low, high))]
    if high - low == LANES:
        return value
    return jnp.concatenate([value, jnp.zeros((value.shape[0], LANES - (high - low)), value.dtype)], axis=1)


def write_tile(ref, where, bins, tile, value):
    rows, low, high = ref.shape[-2], tile * LANES, min((tile + 1) * LANES, bins)
    ref[where + (slice(None), slice(low, high))] = value[:rows, : high - low]


def masks_kernel_part(sea_ref, ice_ref, wind_ref):
    sea = sea_ref[...].astype(jnp.float32)
    gain = 1.0 + time_step * (wind_ref[...] * (1.0 - ice_ref[...].astype(jnp.float32)))
    columns, rows = sea.shape
    sea = jnp.concatenate([sea, gain], axis=1)
    turned = jnp.transpose(sea)
    return turned[:rows], turned[rows:]


def first_kernel(bins, spectrum, sea_ref, ice_ref, wind_ref, out_a, out_b, edge, sems):
    columns, rows = sea_ref.shape
    copies = []
    for c in range(columns):
        for k, start in enumerate((0, rows - 8)):
            copy = pltpu.make_async_copy(
                spectrum.at[c, pl.ds(start, 8)], edge.at[k, c], sems.at[k]
            )
            copy.start()
            copies.append(copy)
    sea, gain = masks_kernel_part(sea_ref, ice_ref, wind_ref)
    shape = (8, LANES)
    lane = lane_index(shape)
    row = row_index(shape)
    used = bins % LANES
    for copy in copies:
        copy.wait()
    tiles = lane_tiles(bins)
    for second, out in ((False, out_a), (True, out_b)):
        to_south = south_flag(second)
        for pair in range(columns // 2):
            for tile in range(tiles):
                halves = []
                for c in (2 * pair, 2 * pair + 1):
                    low, high = read_tile(edge, (0, c), bins, tile), read_tile(edge, (1, c), bins, tile)
                    here = jnp.where(to_south, low, high)
                    s = jnp.where(to_south, sea[0:8, c : c + 1], sea[rows - 8 : rows, c : c + 1])
                    s = jnp.broadcast_to(s, shape)
                    value = here * s
                    if tile == tiles - 1:
                        g = jnp.where(to_south, gain[0:8, c : c + 1], gain[rows - 8 : rows, c : c + 1])
                        g = jnp.broadcast_to(g, shape)
                        value = jnp.where(lane < used, value, jnp.where(lane == used, s, g))
                    halves.append(value)
                first, other = halves
                keep = (row < DEPTH) == to_south
                out[pair, :, lanes_of(tile)] = jnp.where(keep, first, pltpu.roll(other, DEPTH, 0))


def load_kernel(
    bins, spectrum, sea_ref, ice_ref, wind_ref, speed_ref, angle_ref, coupling_ref,
    edge_a, edge_b, inner, seas, gains, stay, go_x, go_y, wide, sems, landed,
):
    columns, rows = sea_ref.shape
    copy = pltpu.make_async_copy(spectrum, landed, sems.at[0])
    copy.start()
    tiles = lane_tiles(bins)
    padded = tiles * LANES
    used = bins % LANES
    shape = (rows + 2 * DEPTH, LANES)
    row = row_index(shape)
    here = jnp.where(row >= rows + DEPTH, row - rows - 2 * DEPTH, row) + lax.axis_index("lat") * rows
    total = rows * lax.axis_size("lat")
    latitude = (-60.0 + 120.0 * (here.astype(jnp.float32) + 0.5) / total) * (math.pi / 180.0)
    over = 1.0 / jnp.cos(latitude)
    count = speed_ref.shape[0]
    for tile in range(tiles):
        which = angle_ref[2:3, lanes_of(tile)]
        speed = jnp.zeros((1, LANES), jnp.float32)
        for k in range(count):
            speed = jnp.where(which == float(k), speed_ref[k], speed)
        x = (angle_ref[0:1, lanes_of(tile)] * speed) * over
        y = angle_ref[1:2, lanes_of(tile)] * speed
        go_x[:, lanes_of(tile)] = x
        go_y[:, lanes_of(tile)] = jnp.broadcast_to(y, (8, LANES))
        stay[:, lanes_of(tile)] = 1.0 - x - y
    body = bins - used
    wide[:, :body] = jnp.concatenate(
        [coupling_ref[:, :body], jnp.zeros((padded - bins, body), jnp.bfloat16)], axis=0
    )
    tail = jnp.concatenate([coupling_ref[:, body:], jnp.ones((bins, padded - bins), jnp.bfloat16)], axis=1)
    wide[:, body:] = jnp.concatenate([tail, jnp.zeros((padded - bins, LANES), jnp.bfloat16)], axis=0)
    sea, gain = masks_kernel_part(sea_ref, ice_ref, wind_ref)
    for c in range(columns):
        s = jnp.broadcast_to(sea[:, c : c + 1], (rows, LANES))
        seas[c, :rows] = time_step * s
        gains[c, :rows] = s * jnp.broadcast_to(gain[:, c : c + 1], (rows, LANES))
    lane = lane_index((rows, LANES))
    copy.wait()

    def put(target, c):
        s = seas[c, :rows] != 0.0
        for tile in range(tiles):
            value = read_tile(landed, (c,), bins, tile)
            keep = s
            if tile == tiles - 1:
                keep = s & (lane < used)
            target[:rows, lanes_of(tile)] = jnp.where(keep, value, 0.0)

    for c in range(1, columns - 1):
        put(inner.at[c - 1], c)
    for second, target in ((False, edge_a), (True, edge_b)):
        put(target, jnp.where(west_flag(second), 0, columns - 1))


def join_kernel(
    bins, halo_a, halo_b, edge_a_in, edge_b_in, inner_in, seas_in, gains_in,
    edge_a, edge_b, inner, seas, gains, pack_a, pack_b,
):
    columns = seas.shape[0]
    rows = seas.shape[1] - 2 * DEPTH
    tiles = lane_tiles(bins)
    used = bins % LANES
    shape = (8, LANES)
    row = row_index(shape)
    lane = lane_index(shape)
    a_south = south_flag(False)
    top = row < DEPTH
    values = []
    for c in range(columns):
        tile_values = []
        for tile in range(tiles):
            from_a, from_b = halo_a[c // 2, :, lanes_of(tile)], halo_b[c // 2, :, lanes_of(tile)]
            low, high = jnp.where(a_south, from_a, from_b), jnp.where(a_south, from_b, from_a)
            if c % 2:
                low, high = pltpu.roll(low, DEPTH, 0), pltpu.roll(high, DEPTH, 0)
            tile_values.append(jnp.where(top, high, low))
        last = tile_values[-1]
        s = jnp.broadcast_to(last[:, used : used + 1], shape)
        g = jnp.broadcast_to(last[:, used + 1 : used + 2], shape)
        seas[c, rows:] = time_step * s
        gains[c, rows:] = s * g
        tile_values[-1] = jnp.where(lane < used, last, 0.0)
        values.append(tile_values)
    for tile in range(tiles):
        for c in range(1, columns - 1):
            inner[c - 1, rows:, lanes_of(tile)] = values[c][tile]
        for second, target in ((False, edge_a), (True, edge_b)):
            target[rows:, lanes_of(tile)] = jnp.where(
                west_flag(second), values[0][tile], values[columns - 1][tile]
            )
    for second, target, pack in ((False, edge_a, pack_a), (True, edge_b, pack_b)):
        packed = pack_half([target[:, lanes_of(t)] for t in range(tiles)], west_flag(second), bins)
        for k, value in enumerate(packed):
            pack[k] = value


def combine(adv, product, seas, gains, share):
    return adv * (gains - seas * share) + seas * product


def last_edge_kernel(bins, second, *refs):
    edge_step(bins, second, *refs[:10], None, refs[10])


def edge_kernel(bins, second, *refs):
    edge_step(bins, second, *refs)


def edge_step(bins, second, halo, edge, inner, seas, gains, stay, go_x, go_y, wide, out, pack, adv_ref):
    last = pack is None
    tiles = lane_tiles(bins)
    columns = inner.shape[0] + 2
    west = west_flag(second)
    near = jnp.where(west, 0, columns - 3)
    mine = jnp.where(west, 0, columns - 1)
    across = across_edge(
        [halo[k] for k in range(3)], [inner[near, :, lanes_of(t)] for t in range(tiles)], west, bins
    )
    for t in range(tiles):
        here = lanes_of(t)
        adv_ref[:, here] = advect(edge[:, here], across[t], stay[:, here], go_x[:, here], go_y[0:1, here], bins, t)
    product = jnp.dot(adv_ref[...].astype(jnp.bfloat16), wide[...], preferred_element_type=jnp.float32)
    share = jnp.broadcast_to(product[:, -1:], (product.shape[0], LANES)) * (dissipation / bins)
    s, g = seas[mine], gains[mine]
    fresh = []
    for t in range(tiles):
        here = lanes_of(t)
        fresh.append(combine(adv_ref[:, here], product[:, here], s, g, share))
        if last:
            write_tile(out, (), bins, t, fresh[-1])
        else:
            out[:, here] = fresh[-1]
    if not last:
        for k, value in enumerate(pack_half(fresh, west, bins)):
            pack[k] = value


def inner_kernel(bins, last, edge_a, edge_b, inner, seas, gains, stay, go_x, go_y, wide, out, adv_ref, low_ref):
    tiles = lane_tiles(bins)
    count, rows = inner.shape[0], inner.shape[1]
    a_west = west_flag(False)
    shape = (rows, LANES)
    for t in range(tiles):
        here = lanes_of(t)
        found = kinds(bins, t, is_east(bins))
        for c in range(count):
            west = east = None
            if True in found:
                west = inner[c - 1, :, here] if c else jnp.where(a_west, edge_a[:, here], edge_b[:, here])
            if False in found:
                east = inner[c + 1, :, here] if c < count - 1 else jnp.where(a_west, edge_b[:, here], edge_a[:, here])
            if west is None:
                across = east
            elif east is None:
                across = west
            else:
                across = jnp.where(eastward(bins, t, shape), west, east)
            adv = advect(inner[c, :, here], across, stay[:, here], go_x[:, here], go_y[0:1, here], bins, t)
            adv_ref[c, :, here] = adv
            low_ref[c * rows : (c + 1) * rows, here] = adv.astype(jnp.bfloat16)
    product = jnp.dot(low_ref[...], wide[...], preferred_element_type=jnp.float32)
    for c in range(count):
        part = product[c * rows : (c + 1) * rows]
        share = jnp.broadcast_to(part[:, -1:], shape) * (dissipation / bins)
        for t in range(tiles):
            here = lanes_of(t)
            value = combine(adv_ref[c, :, here], part[:, here], seas[c + 1], gains[c + 1], share)
            if last:
                write_tile(out, (c,), bins, t, value)
            else:
                out[c, :, here] = value


def finish_kernel(bins, edge_a, edge_b, inner, out, sems):
    columns, rows = out.shape[0], out.shape[1]
    a_west = west_flag(False)
    west = jnp.where(a_west, 0, columns - 1)
    copies = [
        pltpu.make_async_copy(inner, out.at[pl.ds(1, columns - 2)], sems.at[0]),
        pltpu.make_async_copy(edge_a, out.at[west], sems.at[1]),
        pltpu.make_async_copy(edge_b, out.at[columns - 1 - west], sems.at[2]),
    ]
    for copy in copies:
        copy.start()
    for copy in copies:
        copy.wait()


def angle_table(bins, freqs):
    padded = lane_tiles(bins) * LANES
    table = np.zeros((8, padded), np.float32)
    theta = (np.arange(DIRS) + 0.5) * (2.0 * math.pi / DIRS)
    table[0, :bins] = np.repeat(0.225 * np.abs(np.cos(theta)), freqs)
    table[1, :bins] = np.repeat(0.45 * np.abs(np.sin(theta)), freqs)
    table[2, :] = -1.0
    table[2, :bins] = np.tile(np.arange(freqs), DIRS)
    return table


def on_device(spectrum, sea_mask, ice_flags, wind_forcing, group_speed, coupling):
    columns, rows, bins = spectrum.shape
    tiles = lane_tiles(bins)
    padded = tiles * LANES
    tall = rows + 2 * DEPTH
    f32 = jnp.float32
    lon, lat = lax.axis_size("lon"), lax.axis_size("lat")
    lon_a, lon_b = swap_pairs(lon, 0, True), swap_pairs(lon, 1, True)
    lat_a, lat_b = swap_pairs(lat, 0, False), swap_pairs(lat, 1, False)
    vmem = pl.BlockSpec(memory_space=VMEM)
    smem = pl.BlockSpec(memory_space=SMEM)
    anywhere = pl.BlockSpec(memory_space=pl.ANY)
    edge_shape = VMEM((tall, padded), f32)
    inner_shape = VMEM((columns - 2, tall, padded), f32)
    mask_shape = VMEM((columns, tall, LANES), f32)
    pack_shape = VMEM((3, tall, LANES), f32)
    table_shape = VMEM((tall, padded), f32)

    def call(body, name, outs, ins, specs, scratch=(), aliases=None, flops=0, out_specs=None):
        return pl.pallas_call(
            body,
            name=name,
            out_shape=outs,
            in_specs=specs,
            out_specs=out_specs if out_specs is not None else jax.tree.map(lambda _: vmem, outs),
            scratch_shapes=list(scratch),
            input_output_aliases=aliases or {},
            cost_estimate=pl.CostEstimate(flops=flops, bytes_accessed=0, transcendentals=0),
            compiler_params=pltpu.CompilerParams(vmem_limit_bytes=24 * 1024 * 1024),
        )(*ins)

    send_a, send_b = call(
        functools.partial(first_kernel, bins), "first",
        (VMEM((columns // 2, 8, padded), f32),) * 2,
        (spectrum, sea_mask, ice_flags, wind_forcing),
        [anywhere, vmem, vmem, vmem],
        [VMEM((2, columns, 8, bins), f32), pltpu.SemaphoreType.DMA((2,))],
    )
    halo_a = lax.ppermute(send_a, "lat", lat_a)
    halo_b = lax.ppermute(send_b, "lat", lat_b)
    edge_a, edge_b, inner, seas, gains, stay, go_x, go_y, wide = call(
        functools.partial(load_kernel, bins), "load",
        (edge_shape, edge_shape, inner_shape, mask_shape, mask_shape, table_shape, table_shape,
         VMEM((8, padded), f32), VMEM((padded, padded), jnp.bfloat16)),
        (spectrum, sea_mask, ice_flags, wind_forcing, group_speed, jnp.asarray(angle_table(bins, group_speed.shape[0])), coupling),
        [anywhere, vmem, vmem, vmem, smem, vmem, vmem],
        [pltpu.SemaphoreType.DMA((1,)), VMEM((columns, rows, bins), f32)],
        flops=1 << 24,
    )
    edge_a, edge_b, inner, seas, gains, pack_a, pack_b = call(
        functools.partial(join_kernel, bins), "join",
        (edge_shape, edge_shape, inner_shape, mask_shape, mask_shape, pack_shape, pack_shape),
        (halo_a, halo_b, edge_a, edge_b, inner, seas, gains),
        [vmem] * 7,
        aliases={2: 0, 3: 1, 4: 2, 5: 3, 6: 4},
    )
    tables = (seas, gains, stay, go_x, go_y, wide)
    for step in range(STEPS):
        last = step == STEPS - 1
        halo_a = lax.ppermute(pack_a, "lon", lon_a)
        halo_b = lax.ppermute(pack_b, "lon", lon_b)
        new_inner = call(
            functools.partial(inner_kernel, bins, last), "inner",
            VMEM((columns - 2, rows, bins), f32) if last else inner_shape,
            (edge_a, edge_b, inner) + tables, [vmem] * 9,
            [VMEM((columns - 2, tall, padded), f32), VMEM(((columns - 2) * tall, padded), jnp.bfloat16)],
            flops=1 << 28,
        )
        fresh = []
        for second, halo, edge in ((False, halo_a, edge_a), (True, halo_b, edge_b)):
            body = functools.partial(edge_kernel, bins, second)
            if last:
                body = functools.partial(last_edge_kernel, bins, second)
            fresh.append(call(
                body, "edge", VMEM((rows, bins), f32) if last else (edge_shape, pack_shape),
                (halo, edge, inner) + tables, [vmem] * 9, [VMEM((tall, padded), f32)], flops=1 << 26,
            ))
        inner = new_inner
        if last:
            edge_a, edge_b = fresh
        else:
            (edge_a, pack_a), (edge_b, pack_b) = fresh
    return call(
        functools.partial(finish_kernel, bins), "finish",
        jax.ShapeDtypeStruct((columns, rows, bins), f32),
        (edge_a, edge_b, inner), [vmem] * 3,
        [pltpu.SemaphoreType.DMA((3,))], out_specs=anywhere,
    )


def solution(mesh):
    placed = (P("lon", "lat", None), P("lon", "lat"), P("lon", "lat"), P("lon", "lat"), P(), P())
    return jax.shard_map(
        on_device, mesh=mesh, in_specs=placed, out_specs=P("lon", "lat", None), check_vma=False
    )
```

```python
import functools
import math

import jax
import jax.numpy as jnp
import numpy as np
from jax import lax
from jax.experimental import pallas as pl
from jax.experimental.pallas import tpu as pltpu
from jax.sharding import PartitionSpec as P

DIRS = 36
STEPS = 4
LANES = 128
DEPTH = 4

time_step = 0.2
dissipation = 0.5

VMEM = pltpu.VMEM
SMEM = pltpu.SMEM


def swap_pairs(size, first, wrap):
    pairs = []
    for i in range(first, size, 2):
        j = i + 1
        if j >= size:
            if not wrap:
                continue
            j = j % size
        pairs += [(i, j), (j, i)]
    return pairs


def lane_tiles(bins):
    return pl.cdiv(bins, LANES)


def lanes_of(tile):
    return slice(tile * LANES, (tile + 1) * LANES)


def lane_index(shape):
    return lax.broadcasted_iota(jnp.int32, shape, 1)


def row_index(shape):
    return lax.broadcasted_iota(jnp.int32, shape, 0)


def eastward(bins, tile, shape):
    bin_here = lane_index(shape) + tile * LANES
    quarter = bins // 4
    return (bin_here < quarter) | (bin_here >= bins - quarter)


def northward(bins, tile, shape):
    return lane_index(shape) + tile * LANES < bins // 2


def kinds(bins, tile, test):
    low, high = tile * LANES, min((tile + 1) * LANES, bins)
    return {bool(test(b)) for b in range(low, high)}


def is_east(bins):
    return lambda b: b < bins // 4 or b >= bins - bins // 4


def is_north(bins):
    return lambda b: b < bins // 2


def upwind_lat(f, bins, tile):
    shape = f.shape
    rows = shape[0]
    found = kinds(bins, tile, is_north(bins))
    south = pltpu.roll(f, 1, 0) if True in found else None
    north = pltpu.roll(f, rows - 1, 0) if False in found else None
    if south is None:
        return north
    if north is None:
        return south
    return jnp.where(northward(bins, tile, shape), south, north)


def advect(f, across, stay, go_x, go_y, bins, tile):
    along = upwind_lat(f, bins, tile)
    return stay * f + go_x * across + go_y * along


def pack_half(tiles, west_edge, bins):
    quarter = bins // 4
    split = quarter - LANES
    shape = tiles[0].shape
    lane = lane_index(shape)
    last = jnp.where(lane < split, tiles[1], jnp.where(lane >= LANES // 2, tiles[3], pltpu.roll(tiles[5], split, 1)))
    return (
        jnp.where(west_edge, tiles[2], tiles[0]),
        jnp.where(west_edge, tiles[1], tiles[4]),
        jnp.where(west_edge, tiles[3], last),
    )


def across_edge(halo, inner, west_edge, bins):
    quarter = bins // 4
    split = quarter - LANES
    shape = inner[0].shape
    pick = [eastward(bins, tile, shape) == west_edge for tile in (1, 3)]
    return (
        jnp.where(west_edge, halo[0], inner[0]),
        jnp.where(pick[0], jnp.where(west_edge, halo[2], halo[1]), inner[1]),
        jnp.where(west_edge, inner[2], halo[0]),
        jnp.where(pick[1], halo[2], inner[3]),
        jnp.where(west_edge, halo[1], inner[4]),
        jnp.where(west_edge, pltpu.roll(halo[2], LANES - split, 1), inner[5]),
    )


def west_flag(second):
    odd = lax.rem(lax.axis_index("lon"), 2)
    return (1 - odd if second else odd) == 1


def south_flag(second):
    odd = lax.rem(lax.axis_index("lat"), 2)
    return (1 - odd if second else odd) == 1


def read_tile(ref, where, bins, tile):
    low, high = tile * LANES, min((tile + 1) * LANES, bins)
    value = ref[where + (slice(None), slice(low, high))]
    if high - low == LANES:
        return value
    return jnp.concatenate([value, jnp.zeros((value.shape[0], LANES - (high - low)), value.dtype)], axis=1)


def write_tile(ref, where, bins, tile, value):
    rows, low, high = ref.shape[-2], tile * LANES, min((tile + 1) * LANES, bins)
    ref[where + (slice(None), slice(low, high))] = value[:rows, : high - low]


def masks_kernel_part(sea_ref, ice_ref, wind_ref):
    sea = sea_ref[...].astype(jnp.float32)
    gain = 1.0 + time_step * (wind_ref[...] * (1.0 - ice_ref[...].astype(jnp.float32)))
    columns, rows = sea.shape
    sea = jnp.concatenate([sea, gain], axis=1)
    turned = jnp.transpose(sea)
    return turned[:rows], turned[rows:]


def first_kernel(bins, spectrum, sea_hbm, ice_hbm, wind_hbm, out_a, out_b, edge, sea_ref, ice_ref, wind_ref, sems):
    columns, rows = sea_ref.shape
    copies = []
    masks = [
        pltpu.make_async_copy(source, target, sems.at[2 + k])
        for k, (source, target) in enumerate(((sea_hbm, sea_ref), (ice_hbm, ice_ref), (wind_hbm, wind_ref)))
    ]
    for copy in masks:
        copy.start()
    for c in range(columns):
        for k, start in enumerate((0, rows - 8)):
            copy = pltpu.make_async_copy(
                spectrum.at[c, pl.ds(start, 8)], edge.at[k, c], sems.at[k]
            )
            copy.start()
            copies.append(copy)
    for copy in masks:
        copy.wait()
    sea, gain = masks_kernel_part(sea_ref, ice_ref, wind_ref)
    shape = (8, LANES)
    lane = lane_index(shape)
    row = row_index(shape)
    used = bins % LANES
    for copy in copies:
        copy.wait()
    tiles = lane_tiles(bins)
    for second, out in ((False, out_a), (True, out_b)):
        to_south = south_flag(second)
        for pair in range(columns // 2):
            for tile in range(tiles):
                halves = []
                for c in (2 * pair, 2 * pair + 1):
                    low, high = read_tile(edge, (0, c), bins, tile), read_tile(edge, (1, c), bins, tile)
                    here = jnp.where(to_south, low, high)
                    s = jnp.where(to_south, sea[0:8, c : c + 1], sea[rows - 8 : rows, c : c + 1])
                    s = jnp.broadcast_to(s, shape)
                    value = here * s
                    if tile == tiles - 1:
                        g = jnp.where(to_south, gain[0:8, c : c + 1], gain[rows - 8 : rows, c : c + 1])
                        g = jnp.broadcast_to(g, shape)
                        value = jnp.where(lane < used, value, jnp.where(lane == used, s, g))
                    halves.append(value)
                first, other = halves
                keep = (row < DEPTH) == to_south
                out[pair, :, lanes_of(tile)] = jnp.where(keep, first, pltpu.roll(other, DEPTH, 0))


def table_kernel(bins, rows, speed_ref, angle_ref, coupling_ref, stay, go_x, go_y, wide):
    tiles = lane_tiles(bins)
    padded = tiles * LANES
    used = bins % LANES
    shape = (rows + 2 * DEPTH, LANES)
    row = row_index(shape)
    here = jnp.where(row >= rows + DEPTH, row - rows - 2 * DEPTH, row) + lax.axis_index("lat") * rows
    total = rows * lax.axis_size("lat")
    latitude = (-60.0 + 120.0 * (here.astype(jnp.float32) + 0.5) / total) * (math.pi / 180.0)
    over = 1.0 / jnp.cos(latitude)
    count = speed_ref.shape[0]
    for tile in range(tiles):
        which = angle_ref[2:3, lanes_of(tile)]
        speed = jnp.zeros((1, LANES), jnp.float32)
        for k in range(count):
            speed = jnp.where(which == float(k), speed_ref[k], speed)
        x = (angle_ref[0:1, lanes_of(tile)] * speed) * over
        y = angle_ref[1:2, lanes_of(tile)] * speed
        go_x[:, lanes_of(tile)] = x
        go_y[:, lanes_of(tile)] = jnp.broadcast_to(y, (8, LANES))
        stay[:, lanes_of(tile)] = 1.0 - x - y
    body = bins - used
    wide[:, :body] = jnp.concatenate(
        [coupling_ref[:, :body], jnp.zeros((padded - bins, body), jnp.bfloat16)], axis=0
    )
    tail = jnp.concatenate([coupling_ref[:, body:], jnp.ones((bins, padded - bins), jnp.bfloat16)], axis=1)
    wide[:, body:] = jnp.concatenate([tail, jnp.zeros((padded - bins, LANES), jnp.bfloat16)], axis=0)


def load_kernel(bins, spectrum, sea_ref, ice_ref, wind_ref, edge_a, edge_b, inner, seas, gains):
    columns, rows = sea_ref.shape
    tiles = lane_tiles(bins)
    used = bins % LANES
    sea, gain = masks_kernel_part(sea_ref, ice_ref, wind_ref)
    for c in range(columns):
        s = jnp.broadcast_to(sea[:, c : c + 1], (rows, LANES))
        seas[c, :rows] = time_step * s
        gains[c, :rows] = s * jnp.broadcast_to(gain[:, c : c + 1], (rows, LANES))
    lane = lane_index((rows, LANES))

    def put(target, c):
        s = seas[c, :rows] != 0.0
        for tile in range(tiles):
            value = read_tile(spectrum, (c,), bins, tile)
            keep = s
            if tile == tiles - 1:
                keep = s & (lane < used)
            target[:rows, lanes_of(tile)] = jnp.where(keep, value, 0.0)

    for c in range(1, columns - 1):
        put(inner.at[c - 1], c)
    for second, target in ((False, edge_a), (True, edge_b)):
        put(target, jnp.where(west_flag(second), 0, columns - 1))


def join_kernel(
    bins, halo_a, halo_b, edge_a_in, edge_b_in, inner_in, seas_in, gains_in,
    edge_a, edge_b, inner, seas, gains, pack_a, pack_b,
):
    columns = seas.shape[0]
    rows = seas.shape[1] - 2 * DEPTH
    tiles = lane_tiles(bins)
    used = bins % LANES
    shape = (8, LANES)
    row = row_index(shape)
    lane = lane_index(shape)
    a_south = south_flag(False)
    top = row < DEPTH
    values = []
    for c in range(columns):
        tile_values = []
        for tile in range(tiles):
            from_a, from_b = halo_a[c // 2, :, lanes_of(tile)], halo_b[c // 2, :, lanes_of(tile)]
            low, high = jnp.where(a_south, from_a, from_b), jnp.where(a_south, from_b, from_a)
            if c % 2:
                low, high = pltpu.roll(low, DEPTH, 0), pltpu.roll(high, DEPTH, 0)
            tile_values.append(jnp.where(top, high, low))
        last = tile_values[-1]
        s = jnp.broadcast_to(last[:, used : used + 1], shape)
        g = jnp.broadcast_to(last[:, used + 1 : used + 2], shape)
        seas[c, rows:] = time_step * s
        gains[c, rows:] = s * g
        tile_values[-1] = jnp.where(lane < used, last, 0.0)
        values.append(tile_values)
    for tile in range(tiles):
        for c in range(1, columns - 1):
            inner[c - 1, rows:, lanes_of(tile)] = values[c][tile]
        for second, target in ((False, edge_a), (True, edge_b)):
            target[rows:, lanes_of(tile)] = jnp.where(
                west_flag(second), values[0][tile], values[columns - 1][tile]
            )
    for second, target, pack in ((False, edge_a, pack_a), (True, edge_b, pack_b)):
        packed = pack_half([target[:, lanes_of(t)] for t in range(tiles)], west_flag(second), bins)
        for k, value in enumerate(packed):
            pack[k] = value


def combine(adv, product, seas, gains, share):
    return adv * (gains - seas * share) + seas * product


def last_edge_kernel(bins, second, halo, edge, inner, seas, gains, stay, go_x, go_y, wide, whole, out, adv_ref, column, sem):
    edge_step(bins, second, halo, edge, inner, seas, gains, stay, go_x, go_y, wide, column, None, adv_ref)
    mine = jnp.where(west_flag(second), 0, out.shape[0] - 1)
    copy = pltpu.make_async_copy(column, out.at[mine], sem.at[0])
    copy.start()
    copy.wait()


def edge_kernel(bins, second, *refs):
    edge_step(bins, second, *refs)


def edge_step(bins, second, halo, edge, inner, seas, gains, stay, go_x, go_y, wide, out, pack, adv_ref):
    last = pack is None
    tiles = lane_tiles(bins)
    columns = inner.shape[0] + 2
    west = west_flag(second)
    near = jnp.where(west, 0, columns - 3)
    mine = jnp.where(west, 0, columns - 1)
    across = across_edge(
        [halo[k] for k in range(3)], [inner[near, :, lanes_of(t)] for t in range(tiles)], west, bins
    )
    for t in range(tiles):
        here = lanes_of(t)
        adv_ref[:, here] = advect(edge[:, here], across[t], stay[:, here], go_x[:, here], go_y[0:1, here], bins, t)
    product = jnp.dot(adv_ref[...].astype(jnp.bfloat16), wide[...], preferred_element_type=jnp.float32)
    share = jnp.broadcast_to(product[:, -1:], (product.shape[0], LANES)) * (dissipation / bins)
    s, g = seas[mine], gains[mine]
    fresh = []
    for t in range(tiles):
        here = lanes_of(t)
        fresh.append(combine(adv_ref[:, here], product[:, here], s, g, share))
        if last:
            write_tile(out, (), bins, t, fresh[-1])
        else:
            out[:, here] = fresh[-1]
    if not last:
        for k, value in enumerate(pack_half(fresh, west, bins)):
            pack[k] = value


def inner_kernel(bins, last, edge_a, edge_b, inner, seas, gains, stay, go_x, go_y, wide, out, adv_ref, low_ref, done=None, sems=None):
    tiles = lane_tiles(bins)
    count, rows = inner.shape[0], inner.shape[1]
    a_west = west_flag(False)
    shape = (rows, LANES)
    for t in range(tiles):
        here = lanes_of(t)
        found = kinds(bins, t, is_east(bins))
        for c in range(count):
            west = east = None
            if True in found:
                west = inner[c - 1, :, here] if c else jnp.where(a_west, edge_a[:, here], edge_b[:, here])
            if False in found:
                east = inner[c + 1, :, here] if c < count - 1 else jnp.where(a_west, edge_b[:, here], edge_a[:, here])
            if west is None:
                across = east
            elif east is None:
                across = west
            else:
                across = jnp.where(eastward(bins, t, shape), west, east)
            adv = advect(inner[c, :, here], across, stay[:, here], go_x[:, here], go_y[0:1, here], bins, t)
            adv_ref[c, :, here] = adv
            low_ref[c * rows : (c + 1) * rows, here] = adv.astype(jnp.bfloat16)
    product = jnp.dot(low_ref[...], wide[...], preferred_element_type=jnp.float32)
    for c in range(count):
        part = product[c * rows : (c + 1) * rows]
        share = jnp.broadcast_to(part[:, -1:], shape) * (dissipation / bins)
        for t in range(tiles):
            here = lanes_of(t)
            value = combine(adv_ref[c, :, here], part[:, here], seas[c + 1], gains[c + 1], share)
            if last:
                write_tile(done, (c,), bins, t, value)
            else:
                out[c, :, here] = value
        if last:
            pltpu.make_async_copy(done.at[c], out.at[c + 1], sems.at[c]).start()
    if last:
        for c in range(count):
            pltpu.make_async_copy(done.at[c], out.at[c + 1], sems.at[c]).wait()


def angle_table(bins, freqs):
    padded = lane_tiles(bins) * LANES
    table = np.zeros((8, padded), np.float32)
    theta = (np.arange(DIRS) + 0.5) * (2.0 * math.pi / DIRS)
    table[0, :bins] = np.repeat(0.225 * np.abs(np.cos(theta)), freqs)
    table[1, :bins] = np.repeat(0.45 * np.abs(np.sin(theta)), freqs)
    table[2, :] = -1.0
    table[2, :bins] = np.tile(np.arange(freqs), DIRS)
    return table


def on_device(spectrum, sea_mask, ice_flags, wind_forcing, group_speed, coupling):
    columns, rows, bins = spectrum.shape
    tiles = lane_tiles(bins)
    padded = tiles * LANES
    tall = rows + 2 * DEPTH
    f32 = jnp.float32
    lon, lat = lax.axis_size("lon"), lax.axis_size("lat")
    lon_a, lon_b = swap_pairs(lon, 0, True), swap_pairs(lon, 1, True)
    lat_a, lat_b = swap_pairs(lat, 0, False), swap_pairs(lat, 1, False)
    vmem = pl.BlockSpec(memory_space=VMEM)
    smem = pl.BlockSpec(memory_space=SMEM)
    hbm = pl.BlockSpec(memory_space=pltpu.HBM)
    edge_shape = VMEM((tall, padded), f32)
    inner_shape = VMEM((columns - 2, tall, padded), f32)
    mask_shape = VMEM((columns, tall, LANES), f32)
    pack_shape = VMEM((3, tall, LANES), f32)
    table_shape = VMEM((tall, padded), f32)

    def call(body, name, outs, ins, specs, scratch=(), aliases=None, flops=0, out_specs=None):
        return pl.pallas_call(
            body,
            name=name,
            out_shape=outs,
            in_specs=specs,
            out_specs=out_specs if out_specs is not None else jax.tree.map(lambda _: vmem, outs),
            scratch_shapes=list(scratch),
            input_output_aliases=aliases or {},
            cost_estimate=pl.CostEstimate(flops=flops, bytes_accessed=0, transcendentals=0),
            compiler_params=pltpu.CompilerParams(vmem_limit_bytes=24 * 1024 * 1024),
        )(*ins)

    send_a, send_b = call(
        functools.partial(first_kernel, bins), "first",
        (VMEM((columns // 2, 8, padded), f32),) * 2,
        [pltpu.with_memory_space_constraint(x, pltpu.HBM) for x in (spectrum, sea_mask, ice_flags, wind_forcing)],
        [hbm] * 4,
        [VMEM((2, columns, 8, bins), f32), VMEM((columns, rows), sea_mask.dtype), VMEM((columns, rows), ice_flags.dtype),
         VMEM((columns, rows), f32), pltpu.SemaphoreType.DMA((5,))],
    )
    halo_b = lax.ppermute(send_b, "lat", lat_b)
    halo_a = lax.ppermute(send_a, "lat", lat_a)
    edge_a, edge_b, inner, seas, gains = call(
        functools.partial(load_kernel, bins), "load",
        (edge_shape, edge_shape, inner_shape, mask_shape, mask_shape),
        (spectrum, sea_mask, ice_flags, wind_forcing), [vmem] * 4, flops=1 << 24,
    )
    stay, go_x, go_y, wide = call(
        functools.partial(table_kernel, bins, rows), "tables",
        (table_shape, table_shape, VMEM((8, padded), f32), VMEM((padded, padded), jnp.bfloat16)),
        (group_speed, jnp.asarray(angle_table(bins, group_speed.shape[0])), coupling),
        [smem, vmem, vmem], flops=1 << 24,
    )
    edge_a, edge_b, inner, seas, gains, pack_a, pack_b = call(
        functools.partial(join_kernel, bins), "join",
        (edge_shape, edge_shape, inner_shape, mask_shape, mask_shape, pack_shape, pack_shape),
        (halo_a, halo_b, edge_a, edge_b, inner, seas, gains),
        [vmem] * 7,
        aliases={2: 0, 3: 1, 4: 2, 5: 3, 6: 4},
    )
    tables = (seas, gains, stay, go_x, go_y, wide)
    for step in range(STEPS):
        last = step == STEPS - 1
        halo_a = lax.ppermute(pack_a, "lon", lon_a)
        halo_b = lax.ppermute(pack_b, "lon", lon_b)
        whole = pltpu.HBM((columns, rows, bins), f32)
        new_inner = call(
            functools.partial(inner_kernel, bins, last), "inner", whole if last else inner_shape,
            (edge_a, edge_b, inner) + tables, [vmem] * 9,
            [VMEM((columns - 2, tall, padded), f32), VMEM(((columns - 2) * tall, padded), jnp.bfloat16)]
            + ([VMEM((columns - 2, rows, bins), f32), pltpu.SemaphoreType.DMA((columns - 2,))] if last else []),
            flops=1 << 28, out_specs=hbm if last else vmem,
        )
        if last:
            for second, halo, edge in ((True, halo_b, edge_b), (False, halo_a, edge_a)):
                new_inner = call(
                    functools.partial(last_edge_kernel, bins, second), "edge", whole,
                    (halo, edge, inner) + tables + (new_inner,), [vmem] * 9 + [hbm],
                    [VMEM((tall, padded), f32), VMEM((rows, bins), f32), pltpu.SemaphoreType.DMA((1,))],
                    aliases={9: 0}, flops=1 << 26, out_specs=hbm,
                )
            return new_inner
        fresh = []
        for second, halo, edge in ((False, halo_a, edge_a), (True, halo_b, edge_b)):
            fresh.append(call(
                functools.partial(edge_kernel, bins, second), "edge", (edge_shape, pack_shape),
                (halo, edge, inner) + tables, [vmem] * 9, [VMEM((tall, padded), f32)], flops=1 << 26,
            ))
        inner = new_inner
        (edge_a, pack_a), (edge_b, pack_b) = fresh


def solution(mesh):
    placed = (P("lon", "lat", None), P("lon", "lat"), P("lon", "lat"), P("lon", "lat"), P(), P())
    return jax.shard_map(
        on_device, mesh=mesh, in_specs=placed, out_specs=P("lon", "lat", None), check_vma=False
    )
```

```python
import functools
import math

import jax
import jax.numpy as jnp
import numpy as np
from jax import lax
from jax.experimental import pallas as pl
from jax.experimental.pallas import tpu as pltpu
from jax.sharding import PartitionSpec as P

DIRS = 36
STEPS = 4
LANES = 128
DEPTH = 4

time_step = 0.2
dissipation = 0.5

VMEM = pltpu.VMEM
SMEM = pltpu.SMEM


def swap_pairs(size, first, wrap):
    pairs = []
    for i in range(first, size, 2):
        j = i + 1
        if j >= size:
            if not wrap:
                continue
            j = j % size
        pairs += [(i, j), (j, i)]
    return pairs


def lane_tiles(bins):
    return pl.cdiv(bins, LANES)


def lanes_of(tile):
    return slice(tile * LANES, (tile + 1) * LANES)


def lane_index(shape):
    return lax.broadcasted_iota(jnp.int32, shape, 1)


def row_index(shape):
    return lax.broadcasted_iota(jnp.int32, shape, 0)


def eastward(bins, tile, shape):
    bin_here = lane_index(shape) + tile * LANES
    quarter = bins // 4
    return (bin_here < quarter) | (bin_here >= bins - quarter)


def northward(bins, tile, shape):
    return lane_index(shape) + tile * LANES < bins // 2


def kinds(bins, tile, test):
    low, high = tile * LANES, min((tile + 1) * LANES, bins)
    return {bool(test(b)) for b in range(low, high)}


def is_east(bins):
    return lambda b: b < bins // 4 or b >= bins - bins // 4


def is_north(bins):
    return lambda b: b < bins // 2


def upwind_lat(f, bins, tile):
    shape = f.shape
    rows = shape[0]
    found = kinds(bins, tile, is_north(bins))
    south = pltpu.roll(f, 1, 0) if True in found else None
    north = pltpu.roll(f, rows - 1, 0) if False in found else None
    if south is None:
        return north
    if north is None:
        return south
    return jnp.where(northward(bins, tile, shape), south, north)


def advect(f, across, stay, go_x, go_y, bins, tile):
    along = upwind_lat(f, bins, tile)
    return stay * f + go_x * across + go_y * along


def turn(value, shift):
    shift = shift % LANES
    return pltpu.roll(value, shift, 1) if shift else value


def pack_plan(bins, west):
    split = bins // 4 - LANES
    high = bins - bins // 4 - 3 * LANES
    width = 2 * split
    return split, high, width, LANES - width, (split if west else high)


def pack_count(rows, halo):
    blocks = rows // 8
    return 2 * blocks + blocks // 2 + 1 + (2 if halo else 0)


def pack_half(tiles, west, bins, rows, halo, out):
    split, high, width, kept, start = pack_plan(bins, west)
    rest = width - kept
    blocks = rows // 8
    half = blocks // 2
    lane = lane_index((8, LANES))

    def parts(block):
        t = [tile[8 * block : 8 * block + 8] for tile in tiles]
        if west:
            return t[2], jnp.where(lane < high, t[3], t[1]), t[1]
        return t[0], t[4], jnp.where(lane < split, t[1], jnp.where(lane >= high, t[3], turn(t[5], split)))

    left = jnp.zeros((8, LANES), jnp.float32)
    held = {}
    for block in range(blocks + (1 if halo else 0)):
        full, other, part = parts(block)
        if block < blocks:
            out[block] = full
            out[blocks + block] = other
            if block < half:
                held[block] = turn(part, -start)
            else:
                k = block - half
                out[2 * blocks + k] = jnp.where(lane < width, held.pop(k), turn(part, width - start))
                low = rest * k
                left = jnp.where((lane >= low) & (lane < low + rest), turn(part, low - kept - start), left)
        else:
            left = jnp.where(lane >= half * rest, turn(part, half * rest - start), left)
            out[2 * blocks + half + 1] = full
            out[2 * blocks + half + 2] = other
    out[2 * blocks + half] = left


def across_edge(halo, inner, west, bins, rows, with_halo):
    split, high, width, kept, start = pack_plan(bins, not west)
    rest = width - kept
    blocks = rows // 8
    half = blocks // 2
    lane = lane_index((8, LANES))
    left = halo[2 * blocks + half]
    found = [[] for _ in inner]
    for block in range(blocks + 1):
        near = [tile[8 * block : 8 * block + 8] for tile in inner]
        if block == blocks and not with_halo:
            new = near
        else:
            if block == blocks:
                full, other = halo[2 * blocks + half + 1], halo[2 * blocks + half + 2]
                part = turn(left, start - half * rest)
            else:
                full, other = halo[block], halo[blocks + block]
                if block < half:
                    part = turn(halo[2 * blocks + block], start)
                else:
                    k = block - half
                    early = (lane >= high) | (lane < split) if west else lane < start + kept
                    part = jnp.where(early, turn(halo[2 * blocks + k], start - width), turn(left, start + kept - rest * k))
            if west:
                new = [
                    full, jnp.where(lane < split, part, near[1]), near[2],
                    jnp.where(lane >= high, part, near[3]), other, turn(part, -split),
                ]
            else:
                new = [
                    near[0], jnp.where(lane < split, near[1], jnp.where(lane < high, part, other)), full,
                    jnp.where(lane < high, other, near[3]), near[4], near[5],
                ]
        for k, value in enumerate(new):
            found[k].append(value)
    return [jnp.concatenate(values, axis=0) for values in found]


def on_each_side(second, body):
    west = west_flag(second)

    @pl.when(west)
    def _():
        body(True)

    @pl.when(jnp.logical_not(west))
    def _():
        body(False)


def west_flag(second):
    odd = lax.rem(lax.axis_index("lon"), 2)
    return (1 - odd if second else odd) == 1


def south_flag(second):
    odd = lax.rem(lax.axis_index("lat"), 2)
    return (1 - odd if second else odd) == 1


def read_tile(ref, where, bins, tile):
    low, high = tile * LANES, min((tile + 1) * LANES, bins)
    value = ref[where + (slice(None), slice(low, high))]
    if high - low == LANES:
        return value
    return jnp.concatenate([value, jnp.zeros((value.shape[0], LANES - (high - low)), value.dtype)], axis=1)


def write_tile(ref, where, bins, tile, value):
    rows, low, high = ref.shape[-2], tile * LANES, min((tile + 1) * LANES, bins)
    ref[where + (slice(None), slice(low, high))] = value[:rows, : high - low]


def masks_kernel_part(sea_ref, ice_ref, wind_ref):
    sea = sea_ref[...].astype(jnp.float32)
    gain = 1.0 + time_step * (wind_ref[...] * (1.0 - ice_ref[...].astype(jnp.float32)))
    columns, rows = sea.shape
    sea = jnp.concatenate([sea, gain], axis=1)
    turned = jnp.transpose(sea)
    return turned[:rows], turned[rows:]


def first_kernel(bins, spectrum, sea_hbm, ice_hbm, wind_hbm, out_a, out_b, edge, sea_ref, ice_ref, wind_ref, sems):
    columns, rows = sea_ref.shape
    copies = []
    masks = [
        pltpu.make_async_copy(source, target, sems.at[2 + k])
        for k, (source, target) in enumerate(((sea_hbm, sea_ref), (ice_hbm, ice_ref), (wind_hbm, wind_ref)))
    ]
    for copy in masks:
        copy.start()
    for c in range(columns):
        for k, start in enumerate((0, rows - 8)):
            copy = pltpu.make_async_copy(
                spectrum.at[c, pl.ds(start, 8)], edge.at[k, c], sems.at[k]
            )
            copy.start()
            copies.append(copy)
    for copy in masks:
        copy.wait()
    sea, gain = masks_kernel_part(sea_ref, ice_ref, wind_ref)
    shape = (8, LANES)
    lane = lane_index(shape)
    row = row_index(shape)
    used = bins % LANES
    for copy in copies:
        copy.wait()
    tiles = lane_tiles(bins)
    for second, out in ((False, out_a), (True, out_b)):
        to_south = south_flag(second)
        for pair in range(columns // 2):
            for tile in range(tiles):
                halves = []
                for c in (2 * pair, 2 * pair + 1):
                    low, high = read_tile(edge, (0, c), bins, tile), read_tile(edge, (1, c), bins, tile)
                    here = jnp.where(to_south, low, high)
                    s = jnp.where(to_south, sea[0:8, c : c + 1], sea[rows - 8 : rows, c : c + 1])
                    s = jnp.broadcast_to(s, shape)
                    value = here * s
                    if tile == tiles - 1:
                        g = jnp.where(to_south, gain[0:8, c : c + 1], gain[rows - 8 : rows, c : c + 1])
                        g = jnp.broadcast_to(g, shape)
                        value = jnp.where(lane < used, value, jnp.where(lane == used, s, g))
                    halves.append(value)
                first, other = halves
                keep = (row < DEPTH) == to_south
                out[pair, :, lanes_of(tile)] = jnp.where(keep, first, pltpu.roll(other, DEPTH, 0))


def table_kernel(bins, rows, speed_ref, angle_ref, coupling_ref, stay, go_x, go_y, wide):
    tiles = lane_tiles(bins)
    padded = tiles * LANES
    used = bins % LANES
    shape = (rows + 2 * DEPTH, LANES)
    row = row_index(shape)
    here = jnp.where(row >= rows + DEPTH, row - rows - 2 * DEPTH, row) + lax.axis_index("lat") * rows
    total = rows * lax.axis_size("lat")
    latitude = (-60.0 + 120.0 * (here.astype(jnp.float32) + 0.5) / total) * (math.pi / 180.0)
    over = 1.0 / jnp.cos(latitude)
    count = speed_ref.shape[0]
    for tile in range(tiles):
        which = angle_ref[2:3, lanes_of(tile)]
        speed = jnp.zeros((1, LANES), jnp.float32)
        for k in range(count):
            speed = jnp.where(which == float(k), speed_ref[k], speed)
        x = (angle_ref[0:1, lanes_of(tile)] * speed) * over
        y = angle_ref[1:2, lanes_of(tile)] * speed
        go_x[:, lanes_of(tile)] = x
        go_y[:, lanes_of(tile)] = jnp.broadcast_to(y, (8, LANES))
        stay[:, lanes_of(tile)] = 1.0 - x - y
    body = bins - used
    wide[:, :body] = jnp.concatenate(
        [coupling_ref[:, :body], jnp.zeros((padded - bins, body), jnp.bfloat16)], axis=0
    )
    tail = jnp.concatenate([coupling_ref[:, body:], jnp.ones((bins, padded - bins), jnp.bfloat16)], axis=1)
    wide[:, body:] = jnp.concatenate([tail, jnp.zeros((padded - bins, LANES), jnp.bfloat16)], axis=0)


def load_kernel(bins, spectrum, sea_ref, ice_ref, wind_ref, edge_a, edge_b, inner, seas, gains):
    columns, rows = sea_ref.shape
    tiles = lane_tiles(bins)
    used = bins % LANES
    sea, gain = masks_kernel_part(sea_ref, ice_ref, wind_ref)
    for c in range(columns):
        s = jnp.broadcast_to(sea[:, c : c + 1], (rows, LANES))
        seas[c, :rows] = time_step * s
        gains[c, :rows] = s * jnp.broadcast_to(gain[:, c : c + 1], (rows, LANES))
    lane = lane_index((rows, LANES))

    def put(target, c):
        s = seas[c, :rows] != 0.0
        for tile in range(tiles):
            value = read_tile(spectrum, (c,), bins, tile)
            keep = s
            if tile == tiles - 1:
                keep = s & (lane < used)
            target[:rows, lanes_of(tile)] = jnp.where(keep, value, 0.0)

    for c in range(1, columns - 1):
        put(inner.at[c - 1], c)
    for second, target in ((False, edge_a), (True, edge_b)):
        put(target, jnp.where(west_flag(second), 0, columns - 1))


def join_kernel(
    bins, halo_a, halo_b, edge_a_in, edge_b_in, inner_in, seas_in, gains_in,
    edge_a, edge_b, inner, seas, gains, pack_a, pack_b,
):
    columns = seas.shape[0]
    rows = seas.shape[1] - 2 * DEPTH
    tiles = lane_tiles(bins)
    used = bins % LANES
    shape = (8, LANES)
    row = row_index(shape)
    lane = lane_index(shape)
    a_south = south_flag(False)
    top = row < DEPTH
    values = []
    for c in range(columns):
        tile_values = []
        for tile in range(tiles):
            from_a, from_b = halo_a[c // 2, :, lanes_of(tile)], halo_b[c // 2, :, lanes_of(tile)]
            low, high = jnp.where(a_south, from_a, from_b), jnp.where(a_south, from_b, from_a)
            if c % 2:
                low, high = pltpu.roll(low, DEPTH, 0), pltpu.roll(high, DEPTH, 0)
            tile_values.append(jnp.where(top, high, low))
        last = tile_values[-1]
        s = jnp.broadcast_to(last[:, used : used + 1], shape)
        g = jnp.broadcast_to(last[:, used + 1 : used + 2], shape)
        seas[c, rows:] = time_step * s
        gains[c, rows:] = s * g
        tile_values[-1] = jnp.where(lane < used, last, 0.0)
        values.append(tile_values)
    for tile in range(tiles):
        for c in range(1, columns - 1):
            inner[c - 1, rows:, lanes_of(tile)] = values[c][tile]
    for second, target, pack in ((False, edge_a, pack_a), (True, edge_b, pack_b)):

        def side(west, target=target, pack=pack):
            for tile in range(tiles):
                target[rows:, lanes_of(tile)] = values[0 if west else columns - 1][tile]
            pack_half([target[:, lanes_of(t)] for t in range(tiles)], west, bins, rows, True, pack)

        on_each_side(second, side)


def combine(adv, product, seas, gains, share):
    return adv * (gains - seas * share) + seas * product


def edge_kernel(bins, second, halo, edge, inner, seas, gains, stay, go_x, go_y, wide, after, out, pack, adv_ref):
    rows = edge.shape[0] - 2 * DEPTH
    halo_next = pack.shape[0] == pack_count(rows, True)

    def side(west):
        fresh = edge_step(bins, west, halo, edge, inner, seas, gains, stay, go_x, go_y, wide, adv_ref, False)
        for t, value in enumerate(fresh):
            out[:, lanes_of(t)] = value
        pack_half(fresh, west, bins, rows, halo_next, pack)

    on_each_side(second, side)


def late_edge_kernel(bins, second, halo, edge, inner, seas, gains, stay, go_x, go_y, wide, after, out, adv_ref):
    def side(west):
        fresh = edge_step(bins, west, halo, edge, inner, seas, gains, stay, go_x, go_y, wide, adv_ref, True)
        for t, value in enumerate(fresh):
            write_tile(out, (), bins, t, value)

    on_each_side(second, side)


def last_edge_kernel(
    bins, second, halo, edge, inner, seas, gains, stay, go_x, go_y, wide, done_inner, done_edge, out, adv_ref, column, sems
):
    columns = out.shape[0]
    mine = jnp.where(west_flag(second), 0, columns - 1)
    copies = [
        pltpu.make_async_copy(done_inner, out.at[pl.ds(1, columns - 2)], sems.at[0]),
        pltpu.make_async_copy(done_edge, out.at[columns - 1 - mine], sems.at[1]),
    ]
    for copy in copies:
        copy.start()
    late_edge_kernel(bins, second, halo, edge, inner, seas, gains, stay, go_x, go_y, wide, None, column, adv_ref)
    copies.append(pltpu.make_async_copy(column, out.at[mine], sems.at[2]))
    copies[2].start()
    for copy in copies:
        copy.wait()


def edge_step(bins, west, halo, edge, inner, seas, gains, stay, go_x, go_y, wide, adv_ref, last):
    tiles = lane_tiles(bins)
    columns = inner.shape[0] + 2
    rows = edge.shape[0] - 2 * DEPTH
    used = rows if last else edge.shape[0]
    near, mine = (0, 0) if west else (columns - 3, columns - 1)
    across = across_edge(halo, [inner[near, :, lanes_of(t)] for t in range(tiles)], west, bins, rows, not last)
    for t in range(tiles):
        here = lanes_of(t)
        adv = advect(edge[:, here], across[t], stay[:, here], go_x[:, here], go_y[0:1, here], bins, t)
        adv_ref[:used, here] = adv[:used]
    product = jnp.dot(adv_ref[:used].astype(jnp.bfloat16), wide[...], preferred_element_type=jnp.float32)
    share = jnp.broadcast_to(product[:, -1:], (used, LANES)) * (dissipation / bins)
    s, g = seas[mine, :used], gains[mine, :used]
    return [combine(adv_ref[:used, lanes_of(t)], product[:, lanes_of(t)], s, g, share) for t in range(tiles)]


def inner_kernel(bins, edge_a, edge_b, inner, seas, gains, stay, go_x, go_y, wide, out, adv_ref, low_ref):
    tiles = lane_tiles(bins)
    count, tall = inner.shape[0], inner.shape[1]
    rows = adv_ref.shape[1]
    a_west = west_flag(False)
    for t in range(tiles):
        here = lanes_of(t)
        found = kinds(bins, t, is_east(bins))
        for c in range(count):
            west = east = None
            if True in found:
                west = inner[c - 1, :, here] if c else jnp.where(a_west, edge_a[:, here], edge_b[:, here])
            if False in found:
                east = inner[c + 1, :, here] if c < count - 1 else jnp.where(a_west, edge_b[:, here], edge_a[:, here])
            if west is None:
                across = east
            elif east is None:
                across = west
            else:
                across = jnp.where(eastward(bins, t, (tall, LANES)), west, east)
            adv = advect(inner[c, :, here], across, stay[:, here], go_x[:, here], go_y[0:1, here], bins, t)[:rows]
            adv_ref[c, :, here] = adv
            low_ref[c * rows : (c + 1) * rows, here] = adv.astype(jnp.bfloat16)
    product = jnp.dot(low_ref[...], wide[...], preferred_element_type=jnp.float32)
    for c in range(count):
        part = product[c * rows : (c + 1) * rows]
        share = jnp.broadcast_to(part[:, -1:], (rows, LANES)) * (dissipation / bins)
        for t in range(tiles):
            here = lanes_of(t)
            value = combine(adv_ref[c, :, here], part[:, here], seas[c + 1, :rows], gains[c + 1, :rows], share)
            if rows == tall:
                out[c, :, here] = value
            else:
                write_tile(out, (c,), bins, t, value)


def angle_table(bins, freqs):
    padded = lane_tiles(bins) * LANES
    table = np.zeros((8, padded), np.float32)
    theta = (np.arange(DIRS) + 0.5) * (2.0 * math.pi / DIRS)
    table[0, :bins] = np.repeat(0.225 * np.abs(np.cos(theta)), freqs)
    table[1, :bins] = np.repeat(0.45 * np.abs(np.sin(theta)), freqs)
    table[2, :] = -1.0
    table[2, :bins] = np.tile(np.arange(freqs), DIRS)
    return table


def on_device(spectrum, sea_mask, ice_flags, wind_forcing, group_speed, coupling):
    columns, rows, bins = spectrum.shape
    tiles = lane_tiles(bins)
    padded = tiles * LANES
    tall = rows + 2 * DEPTH
    f32 = jnp.float32
    lon, lat = lax.axis_size("lon"), lax.axis_size("lat")
    lon_a, lon_b = swap_pairs(lon, 0, True), swap_pairs(lon, 1, True)
    lat_a, lat_b = swap_pairs(lat, 0, False), swap_pairs(lat, 1, False)
    vmem = pl.BlockSpec(memory_space=VMEM)
    smem = pl.BlockSpec(memory_space=SMEM)
    hbm = pl.BlockSpec(memory_space=pltpu.HBM)
    edge_shape = VMEM((tall, padded), f32)
    inner_shape = VMEM((columns - 2, tall, padded), f32)
    mask_shape = VMEM((columns, tall, LANES), f32)
    pack_shape = VMEM((pack_count(rows, True), 8, LANES), f32)
    table_shape = VMEM((tall, padded), f32)

    def call(body, name, outs, ins, specs, scratch=(), aliases=None, flops=0, out_specs=None):
        return pl.pallas_call(
            body,
            name=name,
            out_shape=outs,
            in_specs=specs,
            out_specs=out_specs if out_specs is not None else jax.tree.map(lambda _: vmem, outs),
            scratch_shapes=list(scratch),
            input_output_aliases=aliases or {},
            cost_estimate=pl.CostEstimate(flops=flops, bytes_accessed=0, transcendentals=0),
            compiler_params=pltpu.CompilerParams(vmem_limit_bytes=24 * 1024 * 1024),
        )(*ins)

    send_a, send_b = call(
        functools.partial(first_kernel, bins), "first",
        (VMEM((columns // 2, 8, padded), f32),) * 2,
        [pltpu.with_memory_space_constraint(x, pltpu.HBM) for x in (spectrum, sea_mask, ice_flags, wind_forcing)],
        [hbm] * 4,
        [VMEM((2, columns, 8, bins), f32), VMEM((columns, rows), sea_mask.dtype), VMEM((columns, rows), ice_flags.dtype),
         VMEM((columns, rows), f32), pltpu.SemaphoreType.DMA((5,))],
    )
    halo_b = lax.ppermute(send_b, "lat", lat_b)
    halo_a = lax.ppermute(send_a, "lat", lat_a)
    edge_a, edge_b, inner, seas, gains = call(
        functools.partial(load_kernel, bins), "load",
        (edge_shape, edge_shape, inner_shape, mask_shape, mask_shape),
        (spectrum, sea_mask, ice_flags, wind_forcing), [vmem] * 4, flops=1 << 24,
    )
    stay, go_x, go_y, wide = call(
        functools.partial(table_kernel, bins, rows), "tables",
        (table_shape, table_shape, VMEM((8, padded), f32), VMEM((padded, padded), jnp.bfloat16)),
        (group_speed, jnp.asarray(angle_table(bins, group_speed.shape[0])), coupling),
        [smem, vmem, vmem], flops=1 << 24,
    )
    edge_a, edge_b, inner, seas, gains, pack_a, pack_b = call(
        functools.partial(join_kernel, bins), "join",
        (edge_shape, edge_shape, inner_shape, mask_shape, mask_shape, pack_shape, pack_shape),
        (halo_a, halo_b, edge_a, edge_b, inner, seas, gains),
        [vmem] * 7,
        aliases={2: 0, 3: 1, 4: 2, 5: 3, 6: 4},
    )
    tables = (seas, gains, stay, go_x, go_y, wide)
    for step in range(STEPS):
        last = step == STEPS - 1
        halo_a = lax.ppermute(pack_a, "lon", lon_a)
        halo_b = lax.ppermute(pack_b, "lon", lon_b)
        used = rows if last else tall
        new_inner = call(
            functools.partial(inner_kernel, bins), "inner", VMEM((columns - 2, rows, bins), f32) if last else inner_shape,
            (edge_a, edge_b, inner) + tables, [vmem] * 9,
            [VMEM((columns - 2, used, padded), f32), VMEM(((columns - 2) * used, padded), jnp.bfloat16)],
            flops=1 << 28,
        )
        if last:
            column = VMEM((rows, bins), f32)
            scratch = [VMEM((tall, padded), f32)]
            done_b = call(
                functools.partial(late_edge_kernel, bins, True), "late", column,
                (halo_b, edge_b, inner) + tables + (new_inner,), [vmem] * 10, scratch, flops=1 << 26,
            )
            return call(
                functools.partial(last_edge_kernel, bins, False), "last", pltpu.HBM((columns, rows, bins), f32),
                (halo_a, edge_a, inner) + tables + (new_inner, done_b), [vmem] * 11,
                scratch + [column, pltpu.SemaphoreType.DMA((3,))], flops=1 << 26, out_specs=hbm,
            )
        fresh = []
        pack_next = VMEM((pack_count(rows, step < STEPS - 2), 8, LANES), f32)
        for second, halo, edge in ((False, halo_a, edge_a), (True, halo_b, edge_b)):
            fresh.append(call(
                functools.partial(edge_kernel, bins, second), "edge", (edge_shape, pack_next),
                (halo, edge, inner) + tables + (new_inner,), [vmem] * 10, [VMEM((tall, padded), f32)], flops=1 << 26,
            ))
        inner = new_inner
        (edge_a, pack_a), (edge_b, pack_b) = fresh


def solution(mesh):
    placed = (P("lon", "lat", None), P("lon", "lat"), P("lon", "lat"), P("lon", "lat"), P(), P())
    return jax.shard_map(
        on_device, mesh=mesh, in_specs=placed, out_specs=P("lon", "lat", None), check_vma=False
    )
```

```python
import functools
import math

import jax
import jax.numpy as jnp
import numpy as np
from jax import lax
from jax.experimental import pallas as pl
from jax.experimental.pallas import tpu as pltpu
from jax.sharding import PartitionSpec as P


DIRS = 36
STEPS = 4
LANES = 128
DEPTH = 4

time_step = 0.2
dissipation = 0.5

VMEM = pltpu.VMEM
SMEM = pltpu.SMEM


def swap_pairs(size, first, wrap):
    pairs = []
    for i in range(first, size, 2):
        j = i + 1
        if j >= size:
            if not wrap:
                continue
            j = j % size
        pairs += [(i, j), (j, i)]
    return pairs


def lane_tiles(bins):
    return pl.cdiv(bins, LANES)


def lanes_of(tile):
    return slice(tile * LANES, (tile + 1) * LANES)


def lane_index(shape):
    return lax.broadcasted_iota(jnp.int32, shape, 1)


def row_index(shape):
    return lax.broadcasted_iota(jnp.int32, shape, 0)


def eastward(bins, tile, shape):
    bin_here = lane_index(shape) + tile * LANES
    quarter = bins // 4
    return (bin_here < quarter) | (bin_here >= bins - quarter)


def northward(bins, tile, shape):
    return lane_index(shape) + tile * LANES < bins // 2


def kinds(bins, tile, test):
    low, high = tile * LANES, min((tile + 1) * LANES, bins)
    return {bool(test(b)) for b in range(low, high)}


def is_east(bins):
    return lambda b: b < bins // 4 or b >= bins - bins // 4


def is_north(bins):
    return lambda b: b < bins // 2


def upwind_lat(f, bins, tile):
    shape = f.shape
    rows = shape[0]
    found = kinds(bins, tile, is_north(bins))
    south = pltpu.roll(f, 1, 0) if True in found else None
    north = pltpu.roll(f, rows - 1, 0) if False in found else None
    if south is None:
        return north
    if north is None:
        return south
    return jnp.where(northward(bins, tile, shape), south, north)


def advect(f, across, stay, go_x, go_y, bins, tile):
    along = upwind_lat(f, bins, tile)
    return stay * f + go_x * across + go_y * along


def turn(value, shift):
    shift = shift % LANES
    return pltpu.roll(value, shift, 1) if shift else value


def pack_plan(bins, west):
    split = bins // 4 - LANES
    high = bins - bins // 4 - 3 * LANES
    width = 2 * split
    return split, high, width, LANES - width, (split if west else high)


def pack_count(rows, halo):
    blocks = rows // 8
    return 2 * blocks + blocks // 2 + 1 + (2 if halo else 0)


def half_parts(t, west, bins):
    split, high, _, _, _ = pack_plan(bins, west)
    lane = lane_index(t[0].shape)
    if west:
        return t[2], jnp.where(lane < high, t[3], t[1]), t[1]
    return t[0], t[4], jnp.where(lane < split, t[1], jnp.where(lane >= high, t[3], turn(t[5], split)))


def pack_half(tiles, west, bins, rows, halo, out):
    _, _, width, kept, start = pack_plan(bins, west)
    rest = width - kept
    blocks = rows // 8
    half = blocks // 2
    lane = lane_index((8, LANES))

    left = jnp.zeros((8, LANES), jnp.float32)
    held = {}
    for block in range(blocks + (1 if halo else 0)):
        full, other, part = half_parts([tile[8 * block : 8 * block + 8] for tile in tiles], west, bins)
        if block < blocks:
            out[block] = full
            out[blocks + block] = other
            if block < half:
                held[block] = turn(part, -start)
            else:
                k = block - half
                out[2 * blocks + k] = jnp.where(lane < width, held.pop(k), turn(part, width - start))
                low = rest * k
                left = jnp.where((lane >= low) & (lane < low + rest), turn(part, low - kept - start), left)
        else:
            left = jnp.where(lane >= half * rest, turn(part, half * rest - start), left)
            out[2 * blocks + half + 1] = full
            out[2 * blocks + half + 2] = other
    out[2 * blocks + half] = left


def across_edge(halo, inner, west, bins, rows, with_halo, corner=None):
    split, high, width, kept, start = pack_plan(bins, not west)
    rest = width - kept
    blocks = rows // 8
    half = blocks // 2
    lane = lane_index((8, LANES))
    left = halo[2 * blocks + half]
    found = [[] for _ in inner]
    for block in range(blocks + 1):
        near = [tile[8 * block : 8 * block + 8] for tile in inner]
        if block == blocks and not with_halo:
            new = near
        else:
            if block == blocks and corner is not None:
                full, other, part = corner[0], corner[1], corner[2]
            elif block == blocks:
                full, other = halo[2 * blocks + half + 1], halo[2 * blocks + half + 2]
                part = turn(left, start - half * rest)
            else:
                full, other = halo[block], halo[blocks + block]
                if block < half:
                    part = turn(halo[2 * blocks + block], start)
                else:
                    k = block - half
                    early = (lane >= high) | (lane < split) if west else lane < start + kept
                    part = jnp.where(early, turn(halo[2 * blocks + k], start - width), turn(left, start + kept - rest * k))
            if west:
                new = [
                    full, jnp.where(lane < split, part, near[1]), near[2],
                    jnp.where(lane >= high, part, near[3]), other, turn(part, -split),
                ]
            else:
                new = [
                    near[0], jnp.where(lane < split, near[1], jnp.where(lane < high, part, other)), full,
                    jnp.where(lane < high, other, near[3]), near[4], near[5],
                ]
        for k, value in enumerate(new):
            found[k].append(value)
    return [jnp.concatenate(values, axis=0) for values in found]


def on_each_side(second, body):
    west = west_flag(second)

    @pl.when(west)
    def _():
        body(True)

    @pl.when(jnp.logical_not(west))
    def _():
        body(False)


def west_flag(second):
    odd = lax.rem(lax.axis_index("lon"), 2)
    return (1 - odd if second else odd) == 1


def south_flag(second):
    odd = lax.rem(lax.axis_index("lat"), 2)
    return (1 - odd if second else odd) == 1


def read_tile(ref, where, bins, tile):
    low, high = tile * LANES, min((tile + 1) * LANES, bins)
    value = ref[where + (slice(None), slice(low, high))]
    if high - low == LANES:
        return value
    return jnp.concatenate([value, jnp.zeros((value.shape[0], LANES - (high - low)), value.dtype)], axis=1)


def write_tile(ref, where, bins, tile, value):
    rows, low, high = ref.shape[-2], tile * LANES, min((tile + 1) * LANES, bins)
    ref[where + (slice(None), slice(low, high))] = value[:rows, : high - low]


def masks_kernel_part(sea_ref, ice_ref, wind_ref):
    sea = sea_ref[...].astype(jnp.float32)
    gain = 1.0 + time_step * (wind_ref[...] * (1.0 - ice_ref[...].astype(jnp.float32)))
    _, rows = sea.shape
    sea = jnp.concatenate([sea, gain], axis=1)
    turned = jnp.transpose(sea)
    return turned[:rows], turned[rows:]


def first_kernel(bins, spectrum, sea_hbm, ice_hbm, wind_hbm, out_a, out_b, edge, sea_ref, ice_ref, wind_ref, sems):
    columns, rows = sea_ref.shape
    copies = []
    masks = [
        pltpu.make_async_copy(source, target, sems.at[2 + k])
        for k, (source, target) in enumerate(((sea_hbm, sea_ref), (ice_hbm, ice_ref), (wind_hbm, wind_ref)))
    ]
    for copy in masks:
        copy.start()
    for c in range(columns):
        for k, start in enumerate((0, rows - 8)):
            copy = pltpu.make_async_copy(
                spectrum.at[c, pl.ds(start, 8)], edge.at[k, c], sems.at[k]
            )
            copy.start()
            copies.append(copy)
    for copy in masks:
        copy.wait()
    sea, gain = masks_kernel_part(sea_ref, ice_ref, wind_ref)
    shape = (8, LANES)
    lane = lane_index(shape)
    row = row_index(shape)
    used = bins % LANES
    for copy in copies:
        copy.wait()
    tiles = lane_tiles(bins)
    for second, out in ((False, out_a), (True, out_b)):
        to_south = south_flag(second)
        for pair in range(columns // 2):
            for tile in range(tiles):
                halves = []
                for c in (2 * pair, 2 * pair + 1):
                    low, high = read_tile(edge, (0, c), bins, tile), read_tile(edge, (1, c), bins, tile)
                    here = jnp.where(to_south, low, high)
                    s = jnp.where(to_south, sea[0:8, c : c + 1], sea[rows - 8 : rows, c : c + 1])
                    s = jnp.broadcast_to(s, shape)
                    value = here * s
                    if tile == tiles - 1:
                        g = jnp.where(to_south, gain[0:8, c : c + 1], gain[rows - 8 : rows, c : c + 1])
                        g = jnp.broadcast_to(g, shape)
                        value = jnp.where(lane < used, value, jnp.where(lane == used, s, g))
                    halves.append(value)
                first, other = halves
                keep = (row < DEPTH) == to_south
                out[pair, :, lanes_of(tile)] = jnp.where(keep, first, pltpu.roll(other, DEPTH, 0))


def table_kernel(bins, rows, speed_ref, angle_ref, coupling_ref, stay, go_x, go_y, wide):
    tiles = lane_tiles(bins)
    padded = tiles * LANES
    used = bins % LANES
    shape = (rows + 2 * DEPTH, LANES)
    row = row_index(shape)
    here = jnp.where(row >= rows + DEPTH, row - rows - 2 * DEPTH, row) + lax.axis_index("lat") * rows
    total = rows * lax.axis_size("lat")
    latitude = (-60.0 + 120.0 * (here.astype(jnp.float32) + 0.5) / total) * (math.pi / 180.0)
    over = 1.0 / jnp.cos(latitude)
    count = speed_ref.shape[0]
    for tile in range(tiles):
        which = angle_ref[2:3, lanes_of(tile)]
        speed = jnp.zeros((1, LANES), jnp.float32)
        for k in range(count):
            speed = jnp.where(which == float(k), speed_ref[k], speed)
        x = (angle_ref[0:1, lanes_of(tile)] * speed) * over
        y = angle_ref[1:2, lanes_of(tile)] * speed
        go_x[:, lanes_of(tile)] = x
        go_y[:, lanes_of(tile)] = jnp.broadcast_to(y, (8, LANES))
        stay[:, lanes_of(tile)] = 1.0 - x - y
    body = bins - used
    wide[:, :body] = jnp.concatenate(
        [coupling_ref[:, :body], jnp.zeros((padded - bins, body), jnp.bfloat16)], axis=0
    )
    tail = jnp.concatenate([coupling_ref[:, body:], jnp.ones((bins, padded - bins), jnp.bfloat16)], axis=1)
    wide[:, body:] = jnp.concatenate([tail, jnp.zeros((padded - bins, LANES), jnp.bfloat16)], axis=0)


def load_kernel(bins, spectrum, sea_ref, ice_ref, wind_ref, edge_a, edge_b, inner, seas, gains, pack_a, pack_b):
    columns, rows = sea_ref.shape
    tiles = lane_tiles(bins)
    used = bins % LANES
    sea, gain = masks_kernel_part(sea_ref, ice_ref, wind_ref)
    for c in range(columns):
        s = jnp.broadcast_to(sea[:, c : c + 1], (rows, LANES))
        seas[c, :rows] = time_step * s
        gains[c, :rows] = s * jnp.broadcast_to(gain[:, c : c + 1], (rows, LANES))
    lane = lane_index((rows, LANES))

    def put(target, c):
        s = seas[c, :rows] != 0.0
        for tile in range(tiles):
            value = read_tile(spectrum, (c,), bins, tile)
            keep = s
            if tile == tiles - 1:
                keep = s & (lane < used)
            target[:rows, lanes_of(tile)] = jnp.where(keep, value, 0.0)

    for c in range(1, columns - 1):
        put(inner.at[c - 1], c)
    for second, target, pack in ((False, edge_a, pack_a), (True, edge_b, pack_b)):

        def side(west, target=target, pack=pack):
            put(target, 0 if west else columns - 1)
            pack_half([target[:rows, lanes_of(t)] for t in range(tiles)], west, bins, rows, False, pack)

        on_each_side(second, side)


def join_kernel(
    bins, halo_a, halo_b, edge_a_in, edge_b_in, inner_in, seas_in, gains_in,
    edge_a, edge_b, inner, seas, gains, pack_a, pack_b,
):
    columns = seas.shape[0]
    rows = seas.shape[1] - 2 * DEPTH
    tiles = lane_tiles(bins)
    used = bins % LANES
    shape = (8, LANES)
    row = row_index(shape)
    lane = lane_index(shape)
    a_south = south_flag(False)
    top = row < DEPTH
    values = []
    for c in range(columns):
        tile_values = []
        for tile in range(tiles):
            from_a, from_b = halo_a[c // 2, :, lanes_of(tile)], halo_b[c // 2, :, lanes_of(tile)]
            low, high = jnp.where(a_south, from_a, from_b), jnp.where(a_south, from_b, from_a)
            if c % 2:
                low, high = pltpu.roll(low, DEPTH, 0), pltpu.roll(high, DEPTH, 0)
            tile_values.append(jnp.where(top, high, low))
        last = tile_values[-1]
        s = jnp.broadcast_to(last[:, used : used + 1], shape)
        g = jnp.broadcast_to(last[:, used + 1 : used + 2], shape)
        seas[c, rows:] = time_step * s
        gains[c, rows:] = s * g
        tile_values[-1] = jnp.where(lane < used, last, 0.0)
        values.append(tile_values)
    for tile in range(tiles):
        for c in range(1, columns - 1):
            inner[c - 1, rows:, lanes_of(tile)] = values[c][tile]
    for second, target, pack in ((False, edge_a, pack_a), (True, edge_b, pack_b)):

        def side(west, target=target, pack=pack):
            for tile in range(tiles):
                target[rows:, lanes_of(tile)] = values[0 if west else columns - 1][tile]
            for k, value in enumerate(half_parts(values[0 if west else columns - 1], west, bins)):
                pack[k] = value

        on_each_side(second, side)


def combine(adv, product, seas, gains, share):
    return adv * (gains - seas * share) + seas * product


def first_edge_kernel(bins, second, corner, *refs):
    edge_kernel(bins, second, *refs, corner=corner)


def edge_kernel(
    bins, second, halo, edge, inner, seas, gains, stay, go_x, go_y, wide, after, out, pack, adv_ref, corner=None
):
    rows = edge.shape[0] - 2 * DEPTH
    halo_next = pack.shape[0] == pack_count(rows, True)

    def side(west):
        fresh = edge_step(bins, west, halo, edge, inner, seas, gains, stay, go_x, go_y, wide, adv_ref, False, corner)
        for t, value in enumerate(fresh):
            out[:, lanes_of(t)] = value
        pack_half(fresh, west, bins, rows, halo_next, pack)

    on_each_side(second, side)


def late_edge_kernel(bins, second, halo, edge, inner, seas, gains, stay, go_x, go_y, wide, after, out, adv_ref):
    def side(west):
        fresh = edge_step(bins, west, halo, edge, inner, seas, gains, stay, go_x, go_y, wide, adv_ref, True)
        for t, value in enumerate(fresh):
            write_tile(out, (), bins, t, value)

    on_each_side(second, side)


def last_edge_kernel(
    bins, second, halo, edge, inner, seas, gains, stay, go_x, go_y, wide, done_inner, done_edge, out, adv_ref, column, sems
):
    columns = out.shape[0]
    mine = jnp.where(west_flag(second), 0, columns - 1)
    copies = [
        pltpu.make_async_copy(done_inner, out.at[pl.ds(1, columns - 2)], sems.at[0]),
        pltpu.make_async_copy(done_edge, out.at[columns - 1 - mine], sems.at[1]),
    ]
    for copy in copies:
        copy.start()
    late_edge_kernel(bins, second, halo, edge, inner, seas, gains, stay, go_x, go_y, wide, None, column, adv_ref)
    copies.append(pltpu.make_async_copy(column, out.at[mine], sems.at[2]))
    copies[2].start()
    for copy in copies:
        copy.wait()


def edge_step(bins, west, halo, edge, inner, seas, gains, stay, go_x, go_y, wide, adv_ref, last, corner=None):
    tiles = lane_tiles(bins)
    columns = inner.shape[0] + 2
    rows = edge.shape[0] - 2 * DEPTH
    used = rows if last else edge.shape[0]
    near, mine = (0, 0) if west else (columns - 3, columns - 1)
    across = across_edge(halo, [inner[near, :, lanes_of(t)] for t in range(tiles)], west, bins, rows, not last, corner)
    for t in range(tiles):
        here = lanes_of(t)
        adv = advect(edge[:, here], across[t], stay[:, here], go_x[:, here], go_y[0:1, here], bins, t)
        adv_ref[:used, here] = adv[:used]
    product = jnp.dot(adv_ref[:used].astype(jnp.bfloat16), wide[...], preferred_element_type=jnp.float32)
    share = jnp.broadcast_to(product[:, -1:], (used, LANES)) * (dissipation / bins)
    s, g = seas[mine, :used], gains[mine, :used]
    return [combine(adv_ref[:used, lanes_of(t)], product[:, lanes_of(t)], s, g, share) for t in range(tiles)]


def inner_kernel(bins, edge_a, edge_b, inner, seas, gains, stay, go_x, go_y, wide, out, adv_ref, low_ref):
    tiles = lane_tiles(bins)
    count, tall = inner.shape[0], inner.shape[1]
    rows = adv_ref.shape[1]
    a_west = west_flag(False)
    for t in range(tiles):
        here = lanes_of(t)
        found = kinds(bins, t, is_east(bins))
        for c in range(count):
            west = east = None
            if True in found:
                west = inner[c - 1, :, here] if c else jnp.where(a_west, edge_a[:, here], edge_b[:, here])
            if False in found:
                east = inner[c + 1, :, here] if c < count - 1 else jnp.where(a_west, edge_b[:, here], edge_a[:, here])
            if west is None:
                across = east
            elif east is None:
                across = west
            else:
                across = jnp.where(eastward(bins, t, (tall, LANES)), west, east)
            adv = advect(inner[c, :, here], across, stay[:, here], go_x[:, here], go_y[0:1, here], bins, t)[:rows]
            adv_ref[c, :, here] = adv
            low_ref[c * rows : (c + 1) * rows, here] = adv.astype(jnp.bfloat16)
    product = jnp.dot(low_ref[...], wide[...], preferred_element_type=jnp.float32)
    for c in range(count):
        part = product[c * rows : (c + 1) * rows]
        share = jnp.broadcast_to(part[:, -1:], (rows, LANES)) * (dissipation / bins)
        for t in range(tiles):
            here = lanes_of(t)
            value = combine(adv_ref[c, :, here], part[:, here], seas[c + 1, :rows], gains[c + 1, :rows], share)
            if rows == tall:
                out[c, :, here] = value
            else:
                write_tile(out, (c,), bins, t, value)


def angle_table(bins, freqs):
    padded = lane_tiles(bins) * LANES
    table = np.zeros((8, padded), np.float32)
    theta = (np.arange(DIRS) + 0.5) * (2.0 * math.pi / DIRS)
    table[0, :bins] = np.repeat(0.225 * np.abs(np.cos(theta)), freqs)
    table[1, :bins] = np.repeat(0.45 * np.abs(np.sin(theta)), freqs)
    table[2, :] = -1.0
    table[2, :bins] = np.tile(np.arange(freqs), DIRS)
    return table


def steps(spectrum, sea_mask, ice_flags, wind_forcing, group_speed, coupling):
    columns, rows, bins = spectrum.shape
    tiles = lane_tiles(bins)
    padded = tiles * LANES
    tall = rows + 2 * DEPTH
    f32 = jnp.float32
    lon, lat = lax.axis_size("lon"), lax.axis_size("lat")
    lon_a, lon_b = swap_pairs(lon, 0, True), swap_pairs(lon, 1, True)
    lat_a, lat_b = swap_pairs(lat, 0, False), swap_pairs(lat, 1, False)
    vmem = pl.BlockSpec(memory_space=VMEM)
    smem = pl.BlockSpec(memory_space=SMEM)
    hbm = pl.BlockSpec(memory_space=pltpu.HBM)
    edge_shape = VMEM((tall, padded), f32)
    inner_shape = VMEM((columns - 2, tall, padded), f32)
    mask_shape = VMEM((columns, tall, LANES), f32)
    table_shape = VMEM((tall, padded), f32)

    def call(body, outs, ins, specs, scratch=(), aliases=None, flops=0, out_specs=None):
        return pl.pallas_call(
            body,
            out_shape=outs,
            in_specs=specs,
            out_specs=out_specs if out_specs is not None else jax.tree.map(lambda _: vmem, outs),
            scratch_shapes=list(scratch),
            input_output_aliases=aliases or {},
            cost_estimate=pl.CostEstimate(flops=flops, bytes_accessed=0, transcendentals=0),
            compiler_params=pltpu.CompilerParams(vmem_limit_bytes=24 * 1024 * 1024),
        )(*ins)

    send_a, send_b = call(
        functools.partial(first_kernel, bins),
        (VMEM((columns // 2, 8, padded), f32),) * 2,
        [pltpu.with_memory_space_constraint(x, pltpu.HBM) for x in (spectrum, sea_mask, ice_flags, wind_forcing)],
        [hbm] * 4,
        [VMEM((2, columns, 8, bins), f32), VMEM((columns, rows), sea_mask.dtype), VMEM((columns, rows), ice_flags.dtype),
         VMEM((columns, rows), f32), pltpu.SemaphoreType.DMA((5,))],
    )
    halo_b = lax.ppermute(send_b, "lat", lat_b)
    halo_a = lax.ppermute(send_a, "lat", lat_a)
    pack_shape = VMEM((pack_count(rows, False), 8, LANES), f32)
    corner_shape = VMEM((3, 8, LANES), f32)
    edge_a, edge_b, inner, seas, gains, pack_a, pack_b = call(
        functools.partial(load_kernel, bins),
        (edge_shape, edge_shape, inner_shape, mask_shape, mask_shape, pack_shape, pack_shape),
        (spectrum, sea_mask, ice_flags, wind_forcing), [vmem] * 4, flops=1 << 24,
    )
    stay, go_x, go_y, wide = call(
        functools.partial(table_kernel, bins, rows),
        (table_shape, table_shape, VMEM((8, padded), f32), VMEM((padded, padded), jnp.bfloat16)),
        (group_speed, jnp.asarray(angle_table(bins, group_speed.shape[0])), coupling),
        [smem, vmem, vmem], flops=1 << 24,
    )
    edge_a, edge_b, inner, seas, gains, corner_a, corner_b = call(
        functools.partial(join_kernel, bins),
        (edge_shape, edge_shape, inner_shape, mask_shape, mask_shape, corner_shape, corner_shape),
        (halo_a, halo_b, edge_a, edge_b, inner, seas, gains),
        [vmem] * 7,
        aliases={2: 0, 3: 1, 4: 2, 5: 3, 6: 4},
    )
    tables = (seas, gains, stay, go_x, go_y, wide)
    for step in range(STEPS):
        last = step == STEPS - 1
        halo_b = lax.ppermute(pack_b, "lon", lon_b)
        halo_a = lax.ppermute(pack_a, "lon", lon_a)
        if step == 0:
            corners = (lax.ppermute(corner_a, "lon", lon_a), lax.ppermute(corner_b, "lon", lon_b))
        used = rows if last else tall
        new_inner = call(
            functools.partial(inner_kernel, bins), VMEM((columns - 2, rows, bins), f32) if last else inner_shape,
            (edge_a, edge_b, inner) + tables, [vmem] * 9,
            [VMEM((columns - 2, used, padded), f32), VMEM(((columns - 2) * used, padded), jnp.bfloat16)],
            flops=1 << 28,
        )
        if last:
            column = VMEM((rows, bins), f32)
            scratch = [VMEM((tall, padded), f32)]
            done_b = call(
                functools.partial(late_edge_kernel, bins, True), column,
                (halo_b, edge_b, inner) + tables + (new_inner,), [vmem] * 10, scratch, flops=1 << 26,
            )
            return call(
                functools.partial(last_edge_kernel, bins, False), pltpu.HBM((columns, rows, bins), f32),
                (halo_a, edge_a, inner) + tables + (new_inner, done_b), [vmem] * 11,
                scratch + [column, pltpu.SemaphoreType.DMA((3,))], flops=1 << 26, out_specs=hbm,
            )
        fresh = []
        pack_next = VMEM((pack_count(rows, step < STEPS - 2), 8, LANES), f32)
        for second, halo, edge in ((False, halo_a, edge_a), (True, halo_b, edge_b)):
            body, ins = edge_kernel, (halo, edge, inner) + tables + (new_inner,)
            if step == 0:
                body, ins = first_edge_kernel, (corners[second],) + ins
            fresh.append(call(
                functools.partial(body, bins, second), (edge_shape, pack_next),
                ins, [vmem] * len(ins), [VMEM((tall, padded), f32)], flops=1 << 26,
            ))
        inner = new_inner
        (edge_a, pack_a), (edge_b, pack_b) = fresh


def solution(mesh):
    placed = (P("lon", "lat", None), P("lon", "lat"), P("lon", "lat"), P("lon", "lat"), P(), P())
    return jax.shard_map(steps, mesh=mesh, in_specs=placed, out_specs=P("lon", "lat", None), check_vma=False)
```

```python
import functools
import math

import jax
import jax.numpy as jnp
import numpy as np
from jax import lax
from jax.experimental import pallas as pl
from jax.experimental.pallas import tpu as pltpu
from jax.sharding import PartitionSpec as P


DIRS = 36
STEPS = 4
LANES = 128
DEPTH = 4

time_step = 0.2
dissipation = 0.5

VMEM = pltpu.VMEM
SMEM = pltpu.SMEM


def swap_pairs(size, first, wrap):
    pairs = []
    for i in range(first, size, 2):
        j = i + 1
        if j >= size:
            if not wrap:
                continue
            j = j % size
        pairs += [(i, j), (j, i)]
    return pairs


def lane_tiles(bins):
    return pl.cdiv(bins, LANES)


def lanes_of(tile):
    return slice(tile * LANES, (tile + 1) * LANES)


def lane_index(shape):
    return lax.broadcasted_iota(jnp.int32, shape, 1)


def row_index(shape):
    return lax.broadcasted_iota(jnp.int32, shape, 0)


def eastward(bins, tile, shape):
    bin_here = lane_index(shape) + tile * LANES
    quarter = bins // 4
    return (bin_here < quarter) | (bin_here >= bins - quarter)


def northward(bins, tile, shape):
    return lane_index(shape) + tile * LANES < bins // 2


def kinds(bins, tile, test):
    low, high = tile * LANES, min((tile + 1) * LANES, bins)
    return {bool(test(b)) for b in range(low, high)}


def is_east(bins):
    return lambda b: b < bins // 4 or b >= bins - bins // 4


def is_north(bins):
    return lambda b: b < bins // 2


def upwind_lat(f, bins, tile):
    shape = f.shape
    rows = shape[0]
    found = kinds(bins, tile, is_north(bins))
    south = pltpu.roll(f, 1, 0) if True in found else None
    north = pltpu.roll(f, rows - 1, 0) if False in found else None
    if south is None:
        return north
    if north is None:
        return south
    return jnp.where(northward(bins, tile, shape), south, north)


def advect(f, across, stay, go_x, go_y, bins, tile):
    along = upwind_lat(f, bins, tile)
    return stay * f + go_x * across + go_y * along


def turn(value, shift):
    shift = shift % LANES
    return pltpu.roll(value, shift, 1) if shift else value


def pack_plan(bins, west):
    split = bins // 4 - LANES
    high = bins - bins // 4 - 3 * LANES
    width = 2 * split
    return split, high, width, LANES - width, (split if west else high)


def pack_count(rows, halo):
    blocks = rows // 8
    return 2 * blocks + blocks // 2 + 1 + (2 if halo else 0)


def half_parts(t, west, bins):
    split, high, _, _, _ = pack_plan(bins, west)
    lane = lane_index(t[0].shape)
    if west:
        return t[2], jnp.where(lane < high, t[3], t[1]), t[1]
    return t[0], t[4], jnp.where(lane < split, t[1], jnp.where(lane >= high, t[3], turn(t[5], split)))


def pack_half(tiles, west, bins, rows, halo, out):
    _, _, width, kept, start = pack_plan(bins, west)
    rest = width - kept
    blocks = rows // 8
    half = blocks // 2
    lane = lane_index((8, LANES))

    left = jnp.zeros((8, LANES), jnp.float32)
    held = {}
    for block in range(blocks + (1 if halo else 0)):
        full, other, part = half_parts([tile[8 * block : 8 * block + 8] for tile in tiles], west, bins)
        if block < blocks:
            out[block] = full
            out[blocks + block] = other
            if block < half:
                held[block] = turn(part, -start)
            else:
                k = block - half
                out[2 * blocks + k] = jnp.where(lane < width, held.pop(k), turn(part, width - start))
                low = rest * k
                left = jnp.where((lane >= low) & (lane < low + rest), turn(part, low - kept - start), left)
        else:
            left = jnp.where(lane >= half * rest, turn(part, half * rest - start), left)
            out[2 * blocks + half + 1] = full
            out[2 * blocks + half + 2] = other
    out[2 * blocks + half] = left


def pack_corner(parts, before, west, bins, rows, out):
    _, _, width, kept, start = pack_plan(bins, west)
    rest = width - kept
    half = rows // 16
    spot = 5 * half
    lane = lane_index((8, LANES))
    out[spot] = jnp.where(lane >= half * rest, turn(parts[2], half * rest - start), before[spot])
    out[spot + 1] = parts[0]
    out[spot + 2] = parts[1]


def across_edge(halo, inner, west, bins, rows, with_halo, corner=None):
    split, high, width, kept, start = pack_plan(bins, not west)
    rest = width - kept
    blocks = rows // 8
    half = blocks // 2
    lane = lane_index((8, LANES))
    left = halo[2 * blocks + half]
    found = [[] for _ in inner]
    for block in range(blocks + 1):
        near = [tile[8 * block : 8 * block + 8] for tile in inner]
        if block == blocks and not with_halo:
            new = near
        else:
            if block == blocks and corner is not None:
                full, other, part = corner[0], corner[1], corner[2]
            elif block == blocks:
                full, other = halo[2 * blocks + half + 1], halo[2 * blocks + half + 2]
                part = turn(left, start - half * rest)
            else:
                full, other = halo[block], halo[blocks + block]
                if block < half:
                    part = turn(halo[2 * blocks + block], start)
                else:
                    k = block - half
                    early = (lane >= high) | (lane < split) if west else lane < start + kept
                    part = jnp.where(early, turn(halo[2 * blocks + k], start - width), turn(left, start + kept - rest * k))
            if west:
                new = [
                    full, jnp.where(lane < split, part, near[1]), near[2],
                    jnp.where(lane >= high, part, near[3]), other, turn(part, -split),
                ]
            else:
                new = [
                    near[0], jnp.where(lane < split, near[1], jnp.where(lane < high, part, other)), full,
                    jnp.where(lane < high, other, near[3]), near[4], near[5],
                ]
        for k, value in enumerate(new):
            found[k].append(value)
    return [jnp.concatenate(values, axis=0) for values in found]


def on_each_side(second, body):
    west = west_flag(second)

    @pl.when(west)
    def _():
        body(True)

    @pl.when(jnp.logical_not(west))
    def _():
        body(False)


def west_flag(second):
    odd = lax.rem(lax.axis_index("lon"), 2)
    return (1 - odd if second else odd) == 1


def south_flag(second):
    odd = lax.rem(lax.axis_index("lat"), 2)
    return (1 - odd if second else odd) == 1


def read_tile(ref, where, bins, tile):
    low, high = tile * LANES, min((tile + 1) * LANES, bins)
    value = ref[where + (slice(None), slice(low, high))]
    if high - low == LANES:
        return value
    return jnp.concatenate([value, jnp.zeros((value.shape[0], LANES - (high - low)), value.dtype)], axis=1)


def write_tile(ref, where, bins, tile, value):
    rows, low, high = ref.shape[-2], tile * LANES, min((tile + 1) * LANES, bins)
    ref[where + (slice(None), slice(low, high))] = value[:rows, : high - low]


def masks_kernel_part(sea_ref, ice_ref, wind_ref):
    sea = sea_ref[...].astype(jnp.float32)
    gain = 1.0 + time_step * (wind_ref[...] * (1.0 - ice_ref[...].astype(jnp.float32)))
    _, rows = sea.shape
    sea = jnp.concatenate([sea, gain], axis=1)
    turned = jnp.transpose(sea)
    return turned[:rows], turned[rows:]


def first_kernel(bins, spectrum, sea_hbm, ice_hbm, wind_hbm, out_a, out_b, edge, sea_ref, ice_ref, wind_ref, sems):
    columns, rows = sea_ref.shape
    copies = []
    masks = [
        pltpu.make_async_copy(source, target, sems.at[2 + k])
        for k, (source, target) in enumerate(((sea_hbm, sea_ref), (ice_hbm, ice_ref), (wind_hbm, wind_ref)))
    ]
    for copy in masks:
        copy.start()
    for c in range(columns):
        for k, start in enumerate((0, rows - 8)):
            copy = pltpu.make_async_copy(
                spectrum.at[c, pl.ds(start, 8)], edge.at[k, c], sems.at[k]
            )
            copy.start()
            copies.append(copy)
    for copy in masks:
        copy.wait()
    sea, gain = masks_kernel_part(sea_ref, ice_ref, wind_ref)
    shape = (8, LANES)
    lane = lane_index(shape)
    row = row_index(shape)
    used = bins % LANES
    for copy in copies:
        copy.wait()
    tiles = lane_tiles(bins)
    for second, out in ((False, out_a), (True, out_b)):
        to_south = south_flag(second)
        for pair in range(columns // 2):
            for tile in range(tiles):
                halves = []
                for c in (2 * pair, 2 * pair + 1):
                    low, high = read_tile(edge, (0, c), bins, tile), read_tile(edge, (1, c), bins, tile)
                    here = jnp.where(to_south, low, high)
                    s = jnp.where(to_south, sea[0:8, c : c + 1], sea[rows - 8 : rows, c : c + 1])
                    s = jnp.broadcast_to(s, shape)
                    value = here * s
                    if tile == tiles - 1:
                        g = jnp.where(to_south, gain[0:8, c : c + 1], gain[rows - 8 : rows, c : c + 1])
                        g = jnp.broadcast_to(g, shape)
                        value = jnp.where(lane < used, value, jnp.where(lane == used, s, g))
                    halves.append(value)
                first, other = halves
                keep = (row < DEPTH) == to_south
                out[pair, :, lanes_of(tile)] = jnp.where(keep, first, pltpu.roll(other, DEPTH, 0))


def table_kernel(bins, rows, speed_ref, angle_ref, coupling_ref, stay, go_x, go_y, wide):
    tiles = lane_tiles(bins)
    padded = tiles * LANES
    used = bins % LANES
    shape = (rows + 2 * DEPTH, LANES)
    row = row_index(shape)
    here = jnp.where(row >= rows + DEPTH, row - rows - 2 * DEPTH, row) + lax.axis_index("lat") * rows
    total = rows * lax.axis_size("lat")
    latitude = (-60.0 + 120.0 * (here.astype(jnp.float32) + 0.5) / total) * (math.pi / 180.0)
    over = 1.0 / jnp.cos(latitude)
    count = speed_ref.shape[0]
    for tile in range(tiles):
        which = angle_ref[2:3, lanes_of(tile)]
        speed = jnp.zeros((1, LANES), jnp.float32)
        for k in range(count):
            speed = jnp.where(which == float(k), speed_ref[k], speed)
        x = (angle_ref[0:1, lanes_of(tile)] * speed) * over
        y = angle_ref[1:2, lanes_of(tile)] * speed
        go_x[:, lanes_of(tile)] = x
        go_y[:, lanes_of(tile)] = jnp.broadcast_to(y, (8, LANES))
        stay[:, lanes_of(tile)] = 1.0 - x - y
    body = bins - used
    wide[:, :body] = jnp.concatenate(
        [coupling_ref[:, :body], jnp.zeros((padded - bins, body), jnp.bfloat16)], axis=0
    )
    tail = jnp.concatenate([coupling_ref[:, body:], jnp.ones((bins, padded - bins), jnp.bfloat16)], axis=1)
    wide[:, body:] = jnp.concatenate([tail, jnp.zeros((padded - bins, LANES), jnp.bfloat16)], axis=0)


def load_kernel(bins, spectrum, sea_ref, ice_ref, wind_ref, edge_a, edge_b, inner, seas, gains, pack_a, pack_b):
    columns, rows = sea_ref.shape
    tiles = lane_tiles(bins)
    used = bins % LANES
    sea, gain = masks_kernel_part(sea_ref, ice_ref, wind_ref)
    for c in range(columns):
        s = jnp.broadcast_to(sea[:, c : c + 1], (rows, LANES))
        seas[c, :rows] = time_step * s
        gains[c, :rows] = s * jnp.broadcast_to(gain[:, c : c + 1], (rows, LANES))
    lane = lane_index((rows, LANES))

    def put(target, c):
        s = seas[c, :rows] != 0.0
        for tile in range(tiles):
            value = read_tile(spectrum, (c,), bins, tile)
            keep = s
            if tile == tiles - 1:
                keep = s & (lane < used)
            target[:rows, lanes_of(tile)] = jnp.where(keep, value, 0.0)

    for c in range(1, columns - 1):
        put(inner.at[c - 1], c)
    for second, target, pack in ((False, edge_a, pack_a), (True, edge_b, pack_b)):

        def side(west, target=target, pack=pack):
            put(target, 0 if west else columns - 1)
            pack_half([target[:rows, lanes_of(t)] for t in range(tiles)], west, bins, rows, False, pack)

        on_each_side(second, side)


def join_kernel(
    bins, halo_a, halo_b, edge_a_in, edge_b_in, inner_in, seas_in, gains_in, pack_in,
    edge_a, edge_b, inner, seas, gains, pack_a, corner_b,
):
    columns = seas.shape[0]
    rows = seas.shape[1] - 2 * DEPTH
    tiles = lane_tiles(bins)
    used = bins % LANES
    shape = (8, LANES)
    row = row_index(shape)
    lane = lane_index(shape)
    a_south = south_flag(False)
    top = row < DEPTH
    values = []
    for c in range(columns):
        tile_values = []
        for tile in range(tiles):
            from_a, from_b = halo_a[c // 2, :, lanes_of(tile)], halo_b[c // 2, :, lanes_of(tile)]
            low, high = jnp.where(a_south, from_a, from_b), jnp.where(a_south, from_b, from_a)
            if c % 2:
                low, high = pltpu.roll(low, DEPTH, 0), pltpu.roll(high, DEPTH, 0)
            tile_values.append(jnp.where(top, high, low))
        last = tile_values[-1]
        s = jnp.broadcast_to(last[:, used : used + 1], shape)
        g = jnp.broadcast_to(last[:, used + 1 : used + 2], shape)
        seas[c, rows:] = time_step * s
        gains[c, rows:] = s * g
        tile_values[-1] = jnp.where(lane < used, last, 0.0)
        values.append(tile_values)
    for tile in range(tiles):
        for c in range(1, columns - 1):
            inner[c - 1, rows:, lanes_of(tile)] = values[c][tile]
    for second, target in ((False, edge_a), (True, edge_b)):

        def side(west, second=second, target=target):
            mine = values[0 if west else columns - 1]
            for tile in range(tiles):
                target[rows:, lanes_of(tile)] = mine[tile]
            parts = half_parts(mine, west, bins)
            if second:
                for k, value in enumerate(parts):
                    corner_b[k] = value
            else:
                pack_corner(parts, pack_in, west, bins, rows, pack_a)

        on_each_side(second, side)


def combine(adv, product, seas, gains, share):
    return adv * (gains - seas * share) + seas * product


def first_edge_kernel(bins, second, corner, *refs):
    edge_kernel(bins, second, *refs, corner=corner)


def edge_kernel(
    bins, second, halo, edge, inner, seas, gains, stay, go_x, go_y, wide, after, out, pack, adv_ref, corner=None
):
    rows = edge.shape[0] - 2 * DEPTH
    halo_next = pack.shape[0] == pack_count(rows, True)

    def side(west):
        fresh = edge_step(bins, west, halo, edge, inner, seas, gains, stay, go_x, go_y, wide, adv_ref, False, corner)
        for t, value in enumerate(fresh):
            out[:, lanes_of(t)] = value
        pack_half(fresh, west, bins, rows, halo_next, pack)

    on_each_side(second, side)


def late_edge_kernel(bins, second, halo, edge, inner, seas, gains, stay, go_x, go_y, wide, after, out, adv_ref):
    def side(west):
        fresh = edge_step(bins, west, halo, edge, inner, seas, gains, stay, go_x, go_y, wide, adv_ref, True)
        for t, value in enumerate(fresh):
            write_tile(out, (), bins, t, value)

    on_each_side(second, side)


def last_edge_kernel(
    bins, second, halo, edge, inner, seas, gains, stay, go_x, go_y, wide, done_inner, done_edge, out, adv_ref, column, sems
):
    columns = out.shape[0]
    mine = jnp.where(west_flag(second), 0, columns - 1)
    copies = [
        pltpu.make_async_copy(done_inner, out.at[pl.ds(1, columns - 2)], sems.at[0]),
        pltpu.make_async_copy(done_edge, out.at[columns - 1 - mine], sems.at[1]),
    ]
    for copy in copies:
        copy.start()
    late_edge_kernel(bins, second, halo, edge, inner, seas, gains, stay, go_x, go_y, wide, None, column, adv_ref)
    copies.append(pltpu.make_async_copy(column, out.at[mine], sems.at[2]))
    copies[2].start()
    for copy in copies:
        copy.wait()


def edge_step(bins, west, halo, edge, inner, seas, gains, stay, go_x, go_y, wide, adv_ref, last, corner=None):
    tiles = lane_tiles(bins)
    columns = inner.shape[0] + 2
    rows = edge.shape[0] - 2 * DEPTH
    used = rows if last else edge.shape[0]
    near, mine = (0, 0) if west else (columns - 3, columns - 1)
    across = across_edge(halo, [inner[near, :, lanes_of(t)] for t in range(tiles)], west, bins, rows, not last, corner)
    for t in range(tiles):
        here = lanes_of(t)
        adv = advect(edge[:, here], across[t], stay[:, here], go_x[:, here], go_y[0:1, here], bins, t)
        adv_ref[:used, here] = adv[:used]
    product = jnp.dot(adv_ref[:used].astype(jnp.bfloat16), wide[...], preferred_element_type=jnp.float32)
    share = jnp.broadcast_to(product[:, -1:], (used, LANES)) * (dissipation / bins)
    s, g = seas[mine, :used], gains[mine, :used]
    return [combine(adv_ref[:used, lanes_of(t)], product[:, lanes_of(t)], s, g, share) for t in range(tiles)]


def inner_kernel(bins, edge_a, edge_b, inner, seas, gains, stay, go_x, go_y, wide, out, adv_ref, low_ref):
    tiles = lane_tiles(bins)
    count, tall = inner.shape[0], inner.shape[1]
    rows = adv_ref.shape[1]
    a_west = west_flag(False)
    for t in range(tiles):
        here = lanes_of(t)
        found = kinds(bins, t, is_east(bins))
        for c in range(count):
            west = east = None
            if True in found:
                west = inner[c - 1, :, here] if c else jnp.where(a_west, edge_a[:, here], edge_b[:, here])
            if False in found:
                east = inner[c + 1, :, here] if c < count - 1 else jnp.where(a_west, edge_b[:, here], edge_a[:, here])
            if west is None:
                across = east
            elif east is None:
                across = west
            else:
                across = jnp.where(eastward(bins, t, (tall, LANES)), west, east)
            adv = advect(inner[c, :, here], across, stay[:, here], go_x[:, here], go_y[0:1, here], bins, t)[:rows]
            adv_ref[c, :, here] = adv
            low_ref[c * rows : (c + 1) * rows, here] = adv.astype(jnp.bfloat16)
    product = jnp.dot(low_ref[...], wide[...], preferred_element_type=jnp.float32)
    for c in range(count):
        part = product[c * rows : (c + 1) * rows]
        share = jnp.broadcast_to(part[:, -1:], (rows, LANES)) * (dissipation / bins)
        for t in range(tiles):
            here = lanes_of(t)
            value = combine(adv_ref[c, :, here], part[:, here], seas[c + 1, :rows], gains[c + 1, :rows], share)
            if rows == tall:
                out[c, :, here] = value
            else:
                write_tile(out, (c,), bins, t, value)


def angle_table(bins, freqs):
    padded = lane_tiles(bins) * LANES
    table = np.zeros((8, padded), np.float32)
    theta = (np.arange(DIRS) + 0.5) * (2.0 * math.pi / DIRS)
    table[0, :bins] = np.repeat(0.225 * np.abs(np.cos(theta)), freqs)
    table[1, :bins] = np.repeat(0.45 * np.abs(np.sin(theta)), freqs)
    table[2, :] = -1.0
    table[2, :bins] = np.tile(np.arange(freqs), DIRS)
    return table


def steps(spectrum, sea_mask, ice_flags, wind_forcing, group_speed, coupling):
    columns, rows, bins = spectrum.shape
    tiles = lane_tiles(bins)
    padded = tiles * LANES
    tall = rows + 2 * DEPTH
    f32 = jnp.float32
    lon, lat = lax.axis_size("lon"), lax.axis_size("lat")
    lon_a, lon_b = swap_pairs(lon, 0, True), swap_pairs(lon, 1, True)
    lat_a, lat_b = swap_pairs(lat, 0, False), swap_pairs(lat, 1, False)
    vmem = pl.BlockSpec(memory_space=VMEM)
    smem = pl.BlockSpec(memory_space=SMEM)
    hbm = pl.BlockSpec(memory_space=pltpu.HBM)
    edge_shape = VMEM((tall, padded), f32)
    inner_shape = VMEM((columns - 2, tall, padded), f32)
    mask_shape = VMEM((columns, tall, LANES), f32)
    table_shape = VMEM((tall, padded), f32)

    def call(body, outs, ins, specs, scratch=(), aliases=None, flops=0, out_specs=None):
        return pl.pallas_call(
            body,
            out_shape=outs,
            in_specs=specs,
            out_specs=out_specs if out_specs is not None else jax.tree.map(lambda _: vmem, outs),
            scratch_shapes=list(scratch),
            input_output_aliases=aliases or {},
            cost_estimate=pl.CostEstimate(flops=flops, bytes_accessed=0, transcendentals=0),
            compiler_params=pltpu.CompilerParams(vmem_limit_bytes=24 * 1024 * 1024),
        )(*ins)

    send_a, send_b = call(
        functools.partial(first_kernel, bins),
        (VMEM((columns // 2, 8, padded), f32),) * 2,
        [pltpu.with_memory_space_constraint(x, pltpu.HBM) for x in (spectrum, sea_mask, ice_flags, wind_forcing)],
        [hbm] * 4,
        [VMEM((2, columns, 8, bins), f32), VMEM((columns, rows), sea_mask.dtype), VMEM((columns, rows), ice_flags.dtype),
         VMEM((columns, rows), f32), pltpu.SemaphoreType.DMA((5,))],
    )
    halo_b = lax.ppermute(send_b, "lat", lat_b)
    halo_a = lax.ppermute(send_a, "lat", lat_a)
    pack_own = VMEM((pack_count(rows, False), 8, LANES), f32)
    pack_shape = VMEM((pack_count(rows, True), 8, LANES), f32)
    corner_shape = VMEM((3, 8, LANES), f32)
    edge_a, edge_b, inner, seas, gains, pack_a, pack_b = call(
        functools.partial(load_kernel, bins),
        (edge_shape, edge_shape, inner_shape, mask_shape, mask_shape, pack_shape, pack_own),
        (spectrum, sea_mask, ice_flags, wind_forcing), [vmem] * 4, flops=1 << 24,
    )
    stay, go_x, go_y, wide = call(
        functools.partial(table_kernel, bins, rows),
        (table_shape, table_shape, VMEM((8, padded), f32), VMEM((padded, padded), jnp.bfloat16)),
        (group_speed, jnp.asarray(angle_table(bins, group_speed.shape[0])), coupling),
        [smem, vmem, vmem], flops=1 << 24,
    )
    edge_a, edge_b, inner, seas, gains, pack_a, corner_b = call(
        functools.partial(join_kernel, bins),
        (edge_shape, edge_shape, inner_shape, mask_shape, mask_shape, pack_shape, corner_shape),
        (halo_a, halo_b, edge_a, edge_b, inner, seas, gains, pack_a),
        [vmem] * 8,
        aliases={2: 0, 3: 1, 4: 2, 5: 3, 6: 4, 7: 5},
    )
    tables = (seas, gains, stay, go_x, go_y, wide)
    for step in range(STEPS):
        last = step == STEPS - 1
        halo_b = lax.ppermute(pack_b, "lon", lon_b)
        halo_a = lax.ppermute(pack_a, "lon", lon_a)
        if step == 0:
            corner = lax.ppermute(corner_b, "lon", lon_b)
        used = rows if last else tall
        new_inner = call(
            functools.partial(inner_kernel, bins), VMEM((columns - 2, rows, bins), f32) if last else inner_shape,
            (edge_a, edge_b, inner) + tables, [vmem] * 9,
            [VMEM((columns - 2, used, padded), f32), VMEM(((columns - 2) * used, padded), jnp.bfloat16)],
            flops=1 << 28,
        )
        if last:
            column = VMEM((rows, bins), f32)
            scratch = [VMEM((tall, padded), f32)]
            done_b = call(
                functools.partial(late_edge_kernel, bins, True), column,
                (halo_b, edge_b, inner) + tables + (new_inner,), [vmem] * 10, scratch, flops=1 << 26,
            )
            return call(
                functools.partial(last_edge_kernel, bins, False), pltpu.HBM((columns, rows, bins), f32),
                (halo_a, edge_a, inner) + tables + (new_inner, done_b), [vmem] * 11,
                scratch + [column, pltpu.SemaphoreType.DMA((3,))], flops=1 << 26, out_specs=hbm,
            )
        fresh = []
        pack_next = VMEM((pack_count(rows, step < STEPS - 2), 8, LANES), f32)
        for second, halo, edge in ((False, halo_a, edge_a), (True, halo_b, edge_b)):
            body, ins = edge_kernel, (halo, edge, inner) + tables + (new_inner,)
            if step == 0 and second:
                body, ins = first_edge_kernel, (corner,) + ins
            fresh.append(call(
                functools.partial(body, bins, second), (edge_shape, pack_next),
                ins, [vmem] * len(ins), [VMEM((tall, padded), f32)], flops=1 << 26,
            ))
        inner = new_inner
        (edge_a, pack_a), (edge_b, pack_b) = fresh


def solution(mesh):
    placed = (P("lon", "lat", None), P("lon", "lat"), P("lon", "lat"), P("lon", "lat"), P(), P())
    return jax.shard_map(steps, mesh=mesh, in_specs=placed, out_specs=P("lon", "lat", None), check_vma=False)
```

```python
import functools
import math

import jax
import jax.numpy as jnp
import numpy as np
from jax import lax
from jax.experimental import pallas as pl
from jax.experimental.pallas import tpu as pltpu
from jax.sharding import PartitionSpec as P


DIRS = 36
STEPS = 4
LANES = 128
DEPTH = 4

time_step = 0.2
dissipation = 0.5

VMEM = pltpu.VMEM
SMEM = pltpu.SMEM


def swap_pairs(size, first, wrap):
    pairs = []
    for i in range(first, size, 2):
        j = i + 1
        if j >= size:
            if not wrap:
                continue
            j = j % size
        pairs += [(i, j), (j, i)]
    return pairs


def lane_tiles(bins):
    return pl.cdiv(bins, LANES)


def lanes_of(tile):
    return slice(tile * LANES, (tile + 1) * LANES)


def lane_index(shape):
    return lax.broadcasted_iota(jnp.int32, shape, 1)


def row_index(shape):
    return lax.broadcasted_iota(jnp.int32, shape, 0)


def eastward(bins, tile, shape):
    bin_here = lane_index(shape) + tile * LANES
    quarter = bins // 4
    return (bin_here < quarter) | (bin_here >= bins - quarter)


def northward(bins, tile, shape):
    return lane_index(shape) + tile * LANES < bins // 2


def kinds(bins, tile, test):
    low, high = tile * LANES, min((tile + 1) * LANES, bins)
    return {bool(test(b)) for b in range(low, high)}


def is_east(bins):
    return lambda b: b < bins // 4 or b >= bins - bins // 4


def is_north(bins):
    return lambda b: b < bins // 2


def upwind_lat(f, bins, tile):
    shape = f.shape
    rows = shape[0]
    found = kinds(bins, tile, is_north(bins))
    south = pltpu.roll(f, 1, 0) if True in found else None
    north = pltpu.roll(f, rows - 1, 0) if False in found else None
    if south is None:
        return north
    if north is None:
        return south
    return jnp.where(northward(bins, tile, shape), south, north)


def advect(f, across, stay, go_x, go_y, bins, tile):
    along = upwind_lat(f, bins, tile)
    return stay * f + go_x * across + go_y * along


def turn(value, shift):
    shift = shift % LANES
    return pltpu.roll(value, shift, 1) if shift else value


def pack_plan(bins, west):
    split = bins // 4 - LANES
    high = bins - bins // 4 - 3 * LANES
    width = 2 * split
    return split, high, width, LANES - width, (split if west else high)


def pack_count(rows, halo):
    blocks = rows // 8
    return 2 * blocks + blocks // 2 + 1 + (2 if halo else 0)


def half_parts(t, west, bins):
    split, high, _, _, _ = pack_plan(bins, west)
    lane = lane_index(t[0].shape)
    if west:
        return t[2], jnp.where(lane < high, t[3], t[1]), t[1]
    return t[0], t[4], jnp.where(lane < split, t[1], jnp.where(lane >= high, t[3], turn(t[5], split)))


def pack_half(tiles, west, bins, rows, halo, out):
    _, _, width, kept, start = pack_plan(bins, west)
    rest = width - kept
    blocks = rows // 8
    half = blocks // 2
    lane = lane_index((8, LANES))

    left = jnp.zeros((8, LANES), jnp.float32)
    held = {}
    for block in range(blocks + (1 if halo else 0)):
        full, other, part = half_parts([tile[8 * block : 8 * block + 8] for tile in tiles], west, bins)
        if block < blocks:
            out[block] = full
            out[blocks + block] = other
            if block < half:
                held[block] = turn(part, -start)
            else:
                k = block - half
                out[2 * blocks + k] = jnp.where(lane < width, held.pop(k), turn(part, width - start))
                low = rest * k
                left = jnp.where((lane >= low) & (lane < low + rest), turn(part, low - kept - start), left)
        else:
            left = jnp.where(lane >= half * rest, turn(part, half * rest - start), left)
            out[2 * blocks + half + 1] = full
            out[2 * blocks + half + 2] = other
    out[2 * blocks + half] = left


def pack_corner(parts, before, west, bins, rows, out):
    _, _, width, kept, start = pack_plan(bins, west)
    rest = width - kept
    half = rows // 16
    spot = 5 * half
    lane = lane_index((8, LANES))
    out[spot] = jnp.where(lane >= half * rest, turn(parts[2], half * rest - start), before[spot])
    out[spot + 1] = parts[0]
    out[spot + 2] = parts[1]


def across_edge(halo, inner, west, bins, rows, with_halo, corner=None):
    split, high, width, kept, start = pack_plan(bins, not west)
    rest = width - kept
    blocks = rows // 8
    half = blocks // 2
    lane = lane_index((8, LANES))
    left = halo[2 * blocks + half]
    found = [[] for _ in inner]
    for block in range(blocks + 1):
        near = [tile[8 * block : 8 * block + 8] for tile in inner]
        if block == blocks and not with_halo:
            new = near
        else:
            if block == blocks and corner is not None:
                full, other, part = corner[0], corner[1], corner[2]
            elif block == blocks:
                full, other = halo[2 * blocks + half + 1], halo[2 * blocks + half + 2]
                part = turn(left, start - half * rest)
            else:
                full, other = halo[block], halo[blocks + block]
                if block < half:
                    part = turn(halo[2 * blocks + block], start)
                else:
                    k = block - half
                    early = (lane >= high) | (lane < split) if west else lane < start + kept
                    part = jnp.where(early, turn(halo[2 * blocks + k], start - width), turn(left, start + kept - rest * k))
            if west:
                new = [
                    full, jnp.where(lane < split, part, near[1]), near[2],
                    jnp.where(lane >= high, part, near[3]), other, turn(part, -split),
                ]
            else:
                new = [
                    near[0], jnp.where(lane < split, near[1], jnp.where(lane < high, part, other)), full,
                    jnp.where(lane < high, other, near[3]), near[4], near[5],
                ]
        for k, value in enumerate(new):
            found[k].append(value)
    return [jnp.concatenate(values, axis=0) for values in found]


def on_each_side(second, body):
    west = west_flag(second)

    @pl.when(west)
    def _():
        body(True)

    @pl.when(jnp.logical_not(west))
    def _():
        body(False)


def west_flag(second):
    odd = lax.rem(lax.axis_index("lon"), 2)
    return (1 - odd if second else odd) == 1


def south_flag(second):
    odd = lax.rem(lax.axis_index("lat"), 2)
    return (1 - odd if second else odd) == 1


def read_tile(ref, where, bins, tile):
    low, high = tile * LANES, min((tile + 1) * LANES, bins)
    value = ref[where + (slice(None), slice(low, high))]
    if high - low == LANES:
        return value
    return jnp.concatenate([value, jnp.zeros((value.shape[0], LANES - (high - low)), value.dtype)], axis=1)


def write_tile(ref, where, bins, tile, value):
    rows, low, high = ref.shape[-2], tile * LANES, min((tile + 1) * LANES, bins)
    ref[where + (slice(None), slice(low, high))] = value[:rows, : high - low]


def masks_kernel_part(sea_ref, ice_ref, wind_ref):
    sea = sea_ref[...].astype(jnp.float32)
    gain = 1.0 + time_step * (wind_ref[...] * (1.0 - ice_ref[...].astype(jnp.float32)))
    _, rows = sea.shape
    sea = jnp.concatenate([sea, gain], axis=1)
    turned = jnp.transpose(sea)
    return turned[:rows], turned[rows:]


def first_kernel(bins, spectrum, sea_hbm, ice_hbm, wind_hbm, out_a, out_b, edge, sea_ref, ice_ref, wind_ref, sems):
    columns, rows = sea_ref.shape
    copies = []
    masks = [
        pltpu.make_async_copy(source, target, sems.at[2 + k])
        for k, (source, target) in enumerate(((sea_hbm, sea_ref), (ice_hbm, ice_ref), (wind_hbm, wind_ref)))
    ]
    for copy in masks:
        copy.start()
    for c in range(columns):
        for k, start in enumerate((0, rows - 8)):
            copy = pltpu.make_async_copy(
                spectrum.at[c, pl.ds(start, 8)], edge.at[k, c], sems.at[k]
            )
            copy.start()
            copies.append(copy)
    for copy in masks:
        copy.wait()
    sea, gain = masks_kernel_part(sea_ref, ice_ref, wind_ref)
    shape = (8, LANES)
    lane = lane_index(shape)
    row = row_index(shape)
    used = bins % LANES
    for copy in copies:
        copy.wait()
    tiles = lane_tiles(bins)
    for second, out in ((False, out_a), (True, out_b)):
        to_south = south_flag(second)
        for pair in range(columns // 2):
            for tile in range(tiles):
                halves = []
                for c in (2 * pair, 2 * pair + 1):
                    low, high = read_tile(edge, (0, c), bins, tile), read_tile(edge, (1, c), bins, tile)
                    here = jnp.where(to_south, low, high)
                    s = jnp.where(to_south, sea[0:8, c : c + 1], sea[rows - 8 : rows, c : c + 1])
                    s = jnp.broadcast_to(s, shape)
                    value = here * s
                    if tile == tiles - 1:
                        g = jnp.where(to_south, gain[0:8, c : c + 1], gain[rows - 8 : rows, c : c + 1])
                        g = jnp.broadcast_to(g, shape)
                        value = jnp.where(lane < used, value, jnp.where(lane == used, s, g))
                    halves.append(value)
                first, other = halves
                keep = (row < DEPTH) == to_south
                out[pair, :, lanes_of(tile)] = jnp.where(keep, first, pltpu.roll(other, DEPTH, 0))


def table_kernel(bins, rows, speed_ref, angle_ref, coupling_ref, stay, go_x, go_y, wide):
    tiles = lane_tiles(bins)
    padded = tiles * LANES
    used = bins % LANES
    shape = (rows + 2 * DEPTH, LANES)
    row = row_index(shape)
    here = jnp.where(row >= rows + DEPTH, row - rows - 2 * DEPTH, row) + lax.axis_index("lat") * rows
    total = rows * lax.axis_size("lat")
    latitude = (-60.0 + 120.0 * (here.astype(jnp.float32) + 0.5) / total) * (math.pi / 180.0)
    over = 1.0 / jnp.cos(latitude)
    count = speed_ref.shape[0]
    for tile in range(tiles):
        which = angle_ref[2:3, lanes_of(tile)]
        speed = jnp.zeros((1, LANES), jnp.float32)
        for k in range(count):
            speed = jnp.where(which == float(k), speed_ref[k], speed)
        x = (angle_ref[0:1, lanes_of(tile)] * speed) * over
        y = angle_ref[1:2, lanes_of(tile)] * speed
        go_x[:, lanes_of(tile)] = x
        go_y[:, lanes_of(tile)] = jnp.broadcast_to(y, (8, LANES))
        stay[:, lanes_of(tile)] = 1.0 - x - y
    body = bins - used
    wide[:, :body] = jnp.concatenate(
        [coupling_ref[:, :body], jnp.zeros((padded - bins, body), jnp.bfloat16)], axis=0
    )
    tail = jnp.concatenate([coupling_ref[:, body:], jnp.ones((bins, padded - bins), jnp.bfloat16)], axis=1)
    wide[:, body:] = jnp.concatenate([tail, jnp.zeros((padded - bins, LANES), jnp.bfloat16)], axis=0)


def load_kernel(bins, spectrum, sea_ref, ice_ref, wind_ref, edge_a, edge_b, inner, seas, gains, pack_a, pack_b):
    columns, rows = sea_ref.shape
    tiles = lane_tiles(bins)
    used = bins % LANES
    sea, gain = masks_kernel_part(sea_ref, ice_ref, wind_ref)
    for c in range(columns):
        s = jnp.broadcast_to(sea[:, c : c + 1], (rows, LANES))
        seas[c, :rows] = time_step * s
        gains[c, :rows] = s * jnp.broadcast_to(gain[:, c : c + 1], (rows, LANES))
    lane = lane_index((rows, LANES))

    def put(target, c):
        s = seas[c, :rows] != 0.0
        for tile in range(tiles):
            value = read_tile(spectrum, (c,), bins, tile)
            keep = s
            if tile == tiles - 1:
                keep = s & (lane < used)
            target[:rows, lanes_of(tile)] = jnp.where(keep, value, 0.0)

    for c in range(1, columns - 1):
        put(inner.at[c - 1], c)
    for second, target, pack in ((False, edge_a, pack_a), (True, edge_b, pack_b)):

        def side(west, target=target, pack=pack):
            put(target, 0 if west else columns - 1)
            pack_half([target[:rows, lanes_of(t)] for t in range(tiles)], west, bins, rows, False, pack)

        on_each_side(second, side)


def join_kernel(
    bins, halo_a, halo_b, edge_a_in, edge_b_in, inner_in, seas_in, gains_in, pack_in, after,
    edge_a, edge_b, inner, seas, gains, pack_a, corner_b,
):
    columns = seas.shape[0]
    rows = seas.shape[1] - 2 * DEPTH
    tiles = lane_tiles(bins)
    used = bins % LANES
    shape = (8, LANES)
    row = row_index(shape)
    lane = lane_index(shape)
    a_south = south_flag(False)
    top = row < DEPTH
    values = []
    for c in range(columns):
        tile_values = []
        for tile in range(tiles):
            from_a, from_b = halo_a[c // 2, :, lanes_of(tile)], halo_b[c // 2, :, lanes_of(tile)]
            low, high = jnp.where(a_south, from_a, from_b), jnp.where(a_south, from_b, from_a)
            if c % 2:
                low, high = pltpu.roll(low, DEPTH, 0), pltpu.roll(high, DEPTH, 0)
            tile_values.append(jnp.where(top, high, low))
        last = tile_values[-1]
        s = jnp.broadcast_to(last[:, used : used + 1], shape)
        g = jnp.broadcast_to(last[:, used + 1 : used + 2], shape)
        seas[c, rows:] = time_step * s
        gains[c, rows:] = s * g
        tile_values[-1] = jnp.where(lane < used, last, 0.0)
        values.append(tile_values)
    for tile in range(tiles):
        for c in range(1, columns - 1):
            inner[c - 1, rows:, lanes_of(tile)] = values[c][tile]
    for second, target in ((False, edge_a), (True, edge_b)):

        def side(west, second=second, target=target):
            mine = values[0 if west else columns - 1]
            for tile in range(tiles):
                target[rows:, lanes_of(tile)] = mine[tile]
            parts = half_parts(mine, west, bins)
            if second:
                for k, value in enumerate(parts):
                    corner_b[k] = value
            else:
                pack_corner(parts, pack_in, west, bins, rows, pack_a)

        on_each_side(second, side)


def combine(adv, product, seas, gains, share):
    return adv * (gains - seas * share) + seas * product


def first_edge_kernel(bins, second, corner, *refs):
    edge_kernel(bins, second, *refs, corner=corner)


def ordered_edge_kernel(bins, second, after, *refs):
    edge_kernel(bins, second, *refs)


def edge_kernel(
    bins, second, halo, edge, inner, seas, gains, stay, go_x, go_y, wide, out, pack, adv_ref, corner=None
):
    rows = edge.shape[0] - 2 * DEPTH
    halo_next = pack.shape[0] == pack_count(rows, True)

    def side(west):
        fresh = edge_step(bins, west, halo, edge, inner, seas, gains, stay, go_x, go_y, wide, adv_ref, False, corner)
        for t, value in enumerate(fresh):
            out[:, lanes_of(t)] = value
        pack_half(fresh, west, bins, rows, halo_next, pack)

    on_each_side(second, side)


def late_edge_kernel(bins, second, halo, edge, inner, seas, gains, stay, go_x, go_y, wide, out, adv_ref):
    def side(west):
        fresh = edge_step(bins, west, halo, edge, inner, seas, gains, stay, go_x, go_y, wide, adv_ref, True)
        for t, value in enumerate(fresh):
            write_tile(out, (), bins, t, value)

    on_each_side(second, side)


def last_edge_kernel(
    bins, second, halo, edge, inner, seas, gains, stay, go_x, go_y, wide, done_inner, done_edge, out, adv_ref, column, sems
):
    columns = out.shape[0]
    mine = jnp.where(west_flag(second), 0, columns - 1)
    copies = [
        pltpu.make_async_copy(done_inner, out.at[pl.ds(1, columns - 2)], sems.at[0]),
        pltpu.make_async_copy(done_edge, out.at[columns - 1 - mine], sems.at[1]),
    ]
    for copy in copies:
        copy.start()
    late_edge_kernel(bins, second, halo, edge, inner, seas, gains, stay, go_x, go_y, wide, column, adv_ref)
    copies.append(pltpu.make_async_copy(column, out.at[mine], sems.at[2]))
    copies[2].start()
    for copy in copies:
        copy.wait()


def edge_step(bins, west, halo, edge, inner, seas, gains, stay, go_x, go_y, wide, adv_ref, last, corner=None):
    tiles = lane_tiles(bins)
    columns = inner.shape[0] + 2
    rows = edge.shape[0] - 2 * DEPTH
    used = rows if last else edge.shape[0]
    near, mine = (0, 0) if west else (columns - 3, columns - 1)
    across = across_edge(halo, [inner[near, :, lanes_of(t)] for t in range(tiles)], west, bins, rows, not last, corner)
    for t in range(tiles):
        here = lanes_of(t)
        adv = advect(edge[:, here], across[t], stay[:, here], go_x[:, here], go_y[0:1, here], bins, t)
        adv_ref[:used, here] = adv[:used]
    product = jnp.dot(adv_ref[:used].astype(jnp.bfloat16), wide[...], preferred_element_type=jnp.float32)
    share = jnp.broadcast_to(product[:, -1:], (used, LANES)) * (dissipation / bins)
    s, g = seas[mine, :used], gains[mine, :used]
    return [combine(adv_ref[:used, lanes_of(t)], product[:, lanes_of(t)], s, g, share) for t in range(tiles)]


def inner_kernel(bins, edge_a, edge_b, inner, seas, gains, stay, go_x, go_y, wide, out, adv_ref, low_ref):
    tiles = lane_tiles(bins)
    count, tall = inner.shape[0], inner.shape[1]
    rows = adv_ref.shape[1]
    a_west = west_flag(False)
    for t in range(tiles):
        here = lanes_of(t)
        found = kinds(bins, t, is_east(bins))
        for c in range(count):
            west = east = None
            if True in found:
                west = inner[c - 1, :, here] if c else jnp.where(a_west, edge_a[:, here], edge_b[:, here])
            if False in found:
                east = inner[c + 1, :, here] if c < count - 1 else jnp.where(a_west, edge_b[:, here], edge_a[:, here])
            if west is None:
                across = east
            elif east is None:
                across = west
            else:
                across = jnp.where(eastward(bins, t, (tall, LANES)), west, east)
            adv = advect(inner[c, :, here], across, stay[:, here], go_x[:, here], go_y[0:1, here], bins, t)[:rows]
            adv_ref[c, :, here] = adv
            low_ref[c * rows : (c + 1) * rows, here] = adv.astype(jnp.bfloat16)
    product = jnp.dot(low_ref[...], wide[...], preferred_element_type=jnp.float32)
    for c in range(count):
        part = product[c * rows : (c + 1) * rows]
        share = jnp.broadcast_to(part[:, -1:], (rows, LANES)) * (dissipation / bins)
        for t in range(tiles):
            here = lanes_of(t)
            value = combine(adv_ref[c, :, here], part[:, here], seas[c + 1, :rows], gains[c + 1, :rows], share)
            if rows == tall:
                out[c, :, here] = value
            else:
                write_tile(out, (c,), bins, t, value)


def angle_table(bins, freqs):
    padded = lane_tiles(bins) * LANES
    table = np.zeros((8, padded), np.float32)
    theta = (np.arange(DIRS) + 0.5) * (2.0 * math.pi / DIRS)
    table[0, :bins] = np.repeat(0.225 * np.abs(np.cos(theta)), freqs)
    table[1, :bins] = np.repeat(0.45 * np.abs(np.sin(theta)), freqs)
    table[2, :] = -1.0
    table[2, :bins] = np.tile(np.arange(freqs), DIRS)
    return table


def steps(spectrum, sea_mask, ice_flags, wind_forcing, group_speed, coupling):
    columns, rows, bins = spectrum.shape
    tiles = lane_tiles(bins)
    padded = tiles * LANES
    tall = rows + 2 * DEPTH
    f32 = jnp.float32
    lon, lat = lax.axis_size("lon"), lax.axis_size("lat")
    lon_a, lon_b = swap_pairs(lon, 0, True), swap_pairs(lon, 1, True)
    lat_a, lat_b = swap_pairs(lat, 0, False), swap_pairs(lat, 1, False)
    vmem = pl.BlockSpec(memory_space=VMEM)
    smem = pl.BlockSpec(memory_space=SMEM)
    hbm = pl.BlockSpec(memory_space=pltpu.HBM)
    edge_shape = VMEM((tall, padded), f32)
    inner_shape = VMEM((columns - 2, tall, padded), f32)
    mask_shape = VMEM((columns, tall, LANES), f32)
    table_shape = VMEM((tall, padded), f32)

    def call(body, outs, ins, specs, scratch=(), aliases=None, flops=0, out_specs=None):
        return pl.pallas_call(
            body,
            out_shape=outs,
            in_specs=specs,
            out_specs=out_specs if out_specs is not None else jax.tree.map(lambda _: vmem, outs),
            scratch_shapes=list(scratch),
            input_output_aliases=aliases or {},
            cost_estimate=pl.CostEstimate(flops=flops, bytes_accessed=0, transcendentals=0),
            compiler_params=pltpu.CompilerParams(vmem_limit_bytes=24 * 1024 * 1024),
        )(*ins)

    send_a, send_b = call(
        functools.partial(first_kernel, bins),
        (VMEM((columns // 2, 8, padded), f32),) * 2,
        [pltpu.with_memory_space_constraint(x, pltpu.HBM) for x in (spectrum, sea_mask, ice_flags, wind_forcing)],
        [hbm] * 4,
        [VMEM((2, columns, 8, bins), f32), VMEM((columns, rows), sea_mask.dtype), VMEM((columns, rows), ice_flags.dtype),
         VMEM((columns, rows), f32), pltpu.SemaphoreType.DMA((5,))],
    )
    halo_b = lax.ppermute(send_b, "lat", lat_b)
    halo_a = lax.ppermute(send_a, "lat", lat_a)
    pack_own = VMEM((pack_count(rows, False), 8, LANES), f32)
    pack_shape = VMEM((pack_count(rows, True), 8, LANES), f32)
    corner_shape = VMEM((3, 8, LANES), f32)
    edge_a, edge_b, inner, seas, gains, pack_a, pack_b = call(
        functools.partial(load_kernel, bins),
        (edge_shape, edge_shape, inner_shape, mask_shape, mask_shape, pack_shape, pack_own),
        (spectrum, sea_mask, ice_flags, wind_forcing), [vmem] * 4, flops=1 << 24,
    )
    stay, go_x, go_y, wide = call(
        functools.partial(table_kernel, bins, rows),
        (table_shape, table_shape, VMEM((8, padded), f32), VMEM((padded, padded), jnp.bfloat16)),
        (group_speed, jnp.asarray(angle_table(bins, group_speed.shape[0])), coupling),
        [smem, vmem, vmem], flops=1 << 24,
    )
    edge_a, edge_b, inner, seas, gains, pack_a, corner_b = call(
        functools.partial(join_kernel, bins),
        (edge_shape, edge_shape, inner_shape, mask_shape, mask_shape, pack_shape, corner_shape),
        (halo_a, halo_b, edge_a, edge_b, inner, seas, gains, pack_a, go_y),
        [vmem] * 9,
        aliases={2: 0, 3: 1, 4: 2, 5: 3, 6: 4, 7: 5},
    )
    tables = (seas, gains, stay, go_x, go_y, wide)
    for step in range(STEPS):
        last = step == STEPS - 1
        halo_b = lax.ppermute(pack_b, "lon", lon_b)
        halo_a = lax.ppermute(pack_a, "lon", lon_a)
        if step == 0:
            corner = lax.ppermute(corner_b, "lon", lon_b)
        used = rows if last else tall
        new_inner = call(
            functools.partial(inner_kernel, bins), VMEM((columns - 2, rows, bins), f32) if last else inner_shape,
            (edge_a, edge_b, inner) + tables, [vmem] * 9,
            [VMEM((columns - 2, used, padded), f32), VMEM(((columns - 2) * used, padded), jnp.bfloat16)],
            flops=1 << 28,
        )
        if last:
            column = VMEM((rows, bins), f32)
            scratch = [VMEM((tall, padded), f32)]
            done_b = call(
                functools.partial(late_edge_kernel, bins, True), column,
                (halo_b, edge_b, inner) + tables, [vmem] * 9, scratch, flops=1 << 26,
            )
            return call(
                functools.partial(last_edge_kernel, bins, False), pltpu.HBM((columns, rows, bins), f32),
                (halo_a, edge_a, inner) + tables + (new_inner, done_b), [vmem] * 11,
                scratch + [column, pltpu.SemaphoreType.DMA((3,))], flops=1 << 26, out_specs=hbm,
            )
        fresh = []
        pack_next = VMEM((pack_count(rows, step < STEPS - 2), 8, LANES), f32)
        for second, halo, edge in ((False, halo_a, edge_a), (True, halo_b, edge_b)):
            body, ins = edge_kernel, (halo, edge, inner) + tables
            if not second:
                body, ins = ordered_edge_kernel, (new_inner,) + ins
            elif step == 0:
                body, ins = first_edge_kernel, (corner,) + ins
            fresh.append(call(
                functools.partial(body, bins, second), (edge_shape, pack_next),
                ins, [vmem] * len(ins), [VMEM((tall, padded), f32)], flops=1 << 26,
            ))
        inner = new_inner
        (edge_a, pack_a), (edge_b, pack_b) = fresh


def solution(mesh):
    placed = (P("lon", "lat", None), P("lon", "lat"), P("lon", "lat"), P("lon", "lat"), P(), P())
    return jax.shard_map(steps, mesh=mesh, in_specs=placed, out_specs=P("lon", "lat", None), check_vma=False)
```

```python
import functools
import math

import jax
import jax.numpy as jnp
import numpy as np
from jax import lax
from jax.experimental import pallas as pl
from jax.experimental.pallas import tpu as pltpu
from jax.sharding import PartitionSpec as P


DIRS = 36
STEPS = 4
LANES = 128
DEPTH = 4

time_step = 0.2
dissipation = 0.5

VMEM = pltpu.VMEM
SMEM = pltpu.SMEM


def swap_pairs(size, first, wrap):
    pairs = []
    for i in range(first, size, 2):
        j = i + 1
        if j >= size:
            if not wrap:
                continue
            j = j % size
        pairs += [(i, j), (j, i)]
    return pairs


def lane_tiles(bins):
    return pl.cdiv(bins, LANES)


def lanes_of(tile):
    return slice(tile * LANES, (tile + 1) * LANES)


def lane_index(shape):
    return lax.broadcasted_iota(jnp.int32, shape, 1)


def row_index(shape):
    return lax.broadcasted_iota(jnp.int32, shape, 0)


def eastward(bins, tile, shape):
    bin_here = lane_index(shape) + tile * LANES
    quarter = bins // 4
    return (bin_here < quarter) | (bin_here >= bins - quarter)


def northward(bins, tile, shape):
    return lane_index(shape) + tile * LANES < bins // 2


def kinds(bins, tile, test):
    low, high = tile * LANES, min((tile + 1) * LANES, bins)
    return {bool(test(b)) for b in range(low, high)}


def is_east(bins):
    return lambda b: b < bins // 4 or b >= bins - bins // 4


def is_north(bins):
    return lambda b: b < bins // 2


def upwind_lat(f, bins, tile):
    shape = f.shape
    rows = shape[0]
    found = kinds(bins, tile, is_north(bins))
    south = pltpu.roll(f, 1, 0) if True in found else None
    north = pltpu.roll(f, rows - 1, 0) if False in found else None
    if south is None:
        return north
    if north is None:
        return south
    return jnp.where(northward(bins, tile, shape), south, north)


def advect(f, across, stay, go_x, go_y, bins, tile):
    along = upwind_lat(f, bins, tile)
    return stay * f + go_x * across + go_y * along


def turn(value, shift):
    shift = shift % LANES
    return pltpu.roll(value, shift, 1) if shift else value


def pack_plan(bins, west):
    split = bins // 4 - LANES
    high = bins - bins // 4 - 3 * LANES
    width = 2 * split
    return split, high, width, LANES - width, (split if west else high)


def pack_count(rows, halo):
    blocks = rows // 8
    return 2 * blocks + blocks // 2 + 1 + (2 if halo else 0)


def half_parts(t, west, bins):
    split, high, _, _, _ = pack_plan(bins, west)
    lane = lane_index(t[0].shape)
    if west:
        return t[2], jnp.where(lane < high, t[3], t[1]), t[1]
    return t[0], t[4], jnp.where(lane < split, t[1], jnp.where(lane >= high, t[3], turn(t[5], split)))


def pack_half(tiles, west, bins, rows, halo, out):
    _, _, width, kept, start = pack_plan(bins, west)
    rest = width - kept
    blocks = rows // 8
    half = blocks // 2
    lane = lane_index((8, LANES))

    left = jnp.zeros((8, LANES), jnp.float32)
    held = {}
    for block in range(blocks + (1 if halo else 0)):
        full, other, part = half_parts([tile[8 * block : 8 * block + 8] for tile in tiles], west, bins)
        if block < blocks:
            out[block] = full
            out[blocks + block] = other
            if block < half:
                held[block] = turn(part, -start)
            else:
                k = block - half
                out[2 * blocks + k] = jnp.where(lane < width, held.pop(k), turn(part, width - start))
                low = rest * k
                left = jnp.where((lane >= low) & (lane < low + rest), turn(part, low - kept - start), left)
        else:
            left = jnp.where(lane >= half * rest, turn(part, half * rest - start), left)
            out[2 * blocks + half + 1] = full
            out[2 * blocks + half + 2] = other
    out[2 * blocks + half] = left


def pack_corner(parts, before, west, bins, rows, out):
    _, _, width, kept, start = pack_plan(bins, west)
    rest = width - kept
    half = rows // 16
    spot = 5 * half
    lane = lane_index((8, LANES))
    out[spot] = jnp.where(lane >= half * rest, turn(parts[2], half * rest - start), before[spot])
    out[spot + 1] = parts[0]
    out[spot + 2] = parts[1]


def across_edge(halo, inner, west, bins, rows, with_halo, corner=None):
    split, high, width, kept, start = pack_plan(bins, not west)
    rest = width - kept
    blocks = rows // 8
    half = blocks // 2
    lane = lane_index((8, LANES))
    left = halo[2 * blocks + half]
    found = [[] for _ in inner]
    for block in range(blocks + 1):
        near = [tile[8 * block : 8 * block + 8] for tile in inner]
        if block == blocks and not with_halo:
            new = near
        else:
            if block == blocks and corner is not None:
                full, other, part = corner[0], corner[1], corner[2]
            elif block == blocks:
                full, other = halo[2 * blocks + half + 1], halo[2 * blocks + half + 2]
                part = turn(left, start - half * rest)
            else:
                full, other = halo[block], halo[blocks + block]
                if block < half:
                    part = turn(halo[2 * blocks + block], start)
                else:
                    k = block - half
                    early = (lane >= high) | (lane < split) if west else lane < start + kept
                    part = jnp.where(early, turn(halo[2 * blocks + k], start - width), turn(left, start + kept - rest * k))
            if west:
                new = [
                    full, jnp.where(lane < split, part, near[1]), near[2],
                    jnp.where(lane >= high, part, near[3]), other, turn(part, -split),
                ]
            else:
                new = [
                    near[0], jnp.where(lane < split, near[1], jnp.where(lane < high, part, other)), full,
                    jnp.where(lane < high, other, near[3]), near[4], near[5],
                ]
        for k, value in enumerate(new):
            found[k].append(value)
    return [jnp.concatenate(values, axis=0) for values in found]


def on_each_side(second, body):
    west = west_flag(second)

    @pl.when(west)
    def _():
        body(True)

    @pl.when(jnp.logical_not(west))
    def _():
        body(False)


def west_flag(second):
    odd = lax.rem(lax.axis_index("lon"), 2)
    return (1 - odd if second else odd) == 1


def south_flag(second):
    odd = lax.rem(lax.axis_index("lat"), 2)
    return (1 - odd if second else odd) == 1


def read_tile(ref, where, bins, tile):
    low, high = tile * LANES, min((tile + 1) * LANES, bins)
    value = ref[where + (slice(None), slice(low, high))]
    if high - low == LANES:
        return value
    return jnp.concatenate([value, jnp.zeros((value.shape[0], LANES - (high - low)), value.dtype)], axis=1)


def write_tile(ref, where, bins, tile, value):
    rows, low, high = ref.shape[-2], tile * LANES, min((tile + 1) * LANES, bins)
    ref[where + (slice(None), slice(low, high))] = value[:rows, : high - low]


def masks_kernel_part(sea_ref, ice_ref, wind_ref):
    sea = sea_ref[...].astype(jnp.float32)
    gain = 1.0 + time_step * (wind_ref[...] * (1.0 - ice_ref[...].astype(jnp.float32)))
    _, rows = sea.shape
    sea = jnp.concatenate([sea, gain], axis=1)
    turned = jnp.transpose(sea)
    return turned[:rows], turned[rows:]


def first_kernel(bins, spectrum, sea_hbm, ice_hbm, wind_hbm, out_a, out_b, edge, sea_ref, ice_ref, wind_ref, sems):
    columns, rows = sea_ref.shape
    copies = []
    masks = [
        pltpu.make_async_copy(source, target, sems.at[2 + k])
        for k, (source, target) in enumerate(((sea_hbm, sea_ref), (ice_hbm, ice_ref), (wind_hbm, wind_ref)))
    ]
    for copy in masks:
        copy.start()
    for c in range(columns):
        for k, start in enumerate((0, rows - 8)):
            copy = pltpu.make_async_copy(
                spectrum.at[c, pl.ds(start, 8)], edge.at[k, c], sems.at[k]
            )
            copy.start()
            copies.append(copy)
    for copy in masks:
        copy.wait()
    sea, gain = masks_kernel_part(sea_ref, ice_ref, wind_ref)
    shape = (8, LANES)
    lane = lane_index(shape)
    row = row_index(shape)
    used = bins % LANES
    for copy in copies:
        copy.wait()
    tiles = lane_tiles(bins)
    space = LANES // (columns // 2)
    for second, out in ((False, out_a), (True, out_b)):
        to_south = south_flag(second)
        ends = jnp.zeros(shape, jnp.float32)
        for pair in range(columns // 2):
            for tile in range(tiles):
                halves = []
                for c in (2 * pair, 2 * pair + 1):
                    low, high = read_tile(edge, (0, c), bins, tile), read_tile(edge, (1, c), bins, tile)
                    here = jnp.where(to_south, low, high)
                    s = jnp.where(to_south, sea[0:8, c : c + 1], sea[rows - 8 : rows, c : c + 1])
                    s = jnp.broadcast_to(s, shape)
                    value = here * s
                    if tile == tiles - 1:
                        g = jnp.where(to_south, gain[0:8, c : c + 1], gain[rows - 8 : rows, c : c + 1])
                        g = jnp.broadcast_to(g, shape)
                        value = jnp.where(lane < used, value, jnp.where(lane == used, s, g))
                    halves.append(value)
                first, other = halves
                keep = (row < DEPTH) == to_south
                value = jnp.where(keep, first, pltpu.roll(other, DEPTH, 0))
                if tile < tiles - 1:
                    out[pair * (tiles - 1) + tile] = value
                else:
                    here = (lane >= pair * space) & (lane < (pair + 1) * space)
                    ends = jnp.where(here, turn(value, pair * space), ends)
        out[columns // 2 * (tiles - 1)] = ends


def table_kernel(bins, rows, speed_ref, angle_ref, coupling_ref, stay, go_x, go_y, wide):
    tiles = lane_tiles(bins)
    padded = tiles * LANES
    used = bins % LANES
    shape = (rows + 2 * DEPTH, LANES)
    row = row_index(shape)
    here = jnp.where(row >= rows + DEPTH, row - rows - 2 * DEPTH, row) + lax.axis_index("lat") * rows
    total = rows * lax.axis_size("lat")
    latitude = (-60.0 + 120.0 * (here.astype(jnp.float32) + 0.5) / total) * (math.pi / 180.0)
    over = 1.0 / jnp.cos(latitude)
    count = speed_ref.shape[0]
    for tile in range(tiles):
        which = angle_ref[2:3, lanes_of(tile)]
        speed = jnp.zeros((1, LANES), jnp.float32)
        for k in range(count):
            speed = jnp.where(which == float(k), speed_ref[k], speed)
        x = (angle_ref[0:1, lanes_of(tile)] * speed) * over
        y = angle_ref[1:2, lanes_of(tile)] * speed
        go_x[:, lanes_of(tile)] = x
        go_y[:, lanes_of(tile)] = jnp.broadcast_to(y, (8, LANES))
        stay[:, lanes_of(tile)] = 1.0 - x - y
    body = bins - used
    wide[:, :body] = jnp.concatenate(
        [coupling_ref[:, :body], jnp.zeros((padded - bins, body), jnp.bfloat16)], axis=0
    )
    tail = jnp.concatenate([coupling_ref[:, body:], jnp.ones((bins, padded - bins), jnp.bfloat16)], axis=1)
    wide[:, body:] = jnp.concatenate([tail, jnp.zeros((padded - bins, LANES), jnp.bfloat16)], axis=0)


def load_kernel(bins, spectrum, sea_ref, ice_ref, wind_ref, edge_a, edge_b, inner, seas, gains, pack_a, pack_b):
    columns, rows = sea_ref.shape
    tiles = lane_tiles(bins)
    used = bins % LANES
    sea, gain = masks_kernel_part(sea_ref, ice_ref, wind_ref)
    for c in range(columns):
        s = jnp.broadcast_to(sea[:, c : c + 1], (rows, LANES))
        seas[c, :rows] = time_step * s
        gains[c, :rows] = s * jnp.broadcast_to(gain[:, c : c + 1], (rows, LANES))
    lane = lane_index((rows, LANES))

    def put(target, c):
        s = seas[c, :rows] != 0.0
        for tile in range(tiles):
            value = read_tile(spectrum, (c,), bins, tile)
            keep = s
            if tile == tiles - 1:
                keep = s & (lane < used)
            target[:rows, lanes_of(tile)] = jnp.where(keep, value, 0.0)

    for c in range(1, columns - 1):
        put(inner.at[c - 1], c)
    for second, target, pack in ((False, edge_a, pack_a), (True, edge_b, pack_b)):

        def side(west, target=target, pack=pack):
            put(target, 0 if west else columns - 1)
            pack_half([target[:rows, lanes_of(t)] for t in range(tiles)], west, bins, rows, False, pack)

        on_each_side(second, side)


def join_kernel(
    bins, halo_a, halo_b, edge_a_in, edge_b_in, inner_in, seas_in, gains_in, pack_in,
    edge_a, edge_b, inner, seas, gains, pack_a, corner_b,
):
    columns = seas.shape[0]
    rows = seas.shape[1] - 2 * DEPTH
    tiles = lane_tiles(bins)
    used = bins % LANES
    shape = (8, LANES)
    row = row_index(shape)
    lane = lane_index(shape)
    a_south = south_flag(False)
    top = row < DEPTH
    values = []
    for c in range(columns):
        tile_values = []
        for tile in range(tiles):
            spot = columns // 2 * (tiles - 1) if tile == tiles - 1 else c // 2 * (tiles - 1) + tile
            from_a, from_b = halo_a[spot], halo_b[spot]
            if tile == tiles - 1:
                back = -(c // 2) * (LANES // (columns // 2))
                from_a, from_b = turn(from_a, back), turn(from_b, back)
            low, high = jnp.where(a_south, from_a, from_b), jnp.where(a_south, from_b, from_a)
            if c % 2:
                low, high = pltpu.roll(low, DEPTH, 0), pltpu.roll(high, DEPTH, 0)
            tile_values.append(jnp.where(top, high, low))
        last = tile_values[-1]
        s = jnp.broadcast_to(last[:, used : used + 1], shape)
        g = jnp.broadcast_to(last[:, used + 1 : used + 2], shape)
        seas[c, rows:] = time_step * s
        gains[c, rows:] = s * g
        tile_values[-1] = jnp.where(lane < used, last, 0.0)
        values.append(tile_values)
    for tile in range(tiles):
        for c in range(1, columns - 1):
            inner[c - 1, rows:, lanes_of(tile)] = values[c][tile]
    for second, target in ((False, edge_a), (True, edge_b)):

        def side(west, second=second, target=target):
            mine = values[0 if west else columns - 1]
            for tile in range(tiles):
                target[rows:, lanes_of(tile)] = mine[tile]
            parts = half_parts(mine, west, bins)
            if second:
                for k, value in enumerate(parts):
                    corner_b[k] = value
            else:
                pack_corner(parts, pack_in, west, bins, rows, pack_a)

        on_each_side(second, side)


def combine(adv, product, seas, gains, share):
    return adv * (gains - seas * share) + seas * product


def first_edge_kernel(bins, second, corner, *refs):
    edge_kernel(bins, second, *refs, corner=corner)


def ordered_edge_kernel(bins, second, after, *refs):
    edge_kernel(bins, second, *refs)


def edge_kernel(
    bins, second, halo, edge, inner, seas, gains, stay, go_x, go_y, wide, out, pack, adv_ref, corner=None
):
    rows = edge.shape[0] - 2 * DEPTH
    halo_next = pack.shape[0] == pack_count(rows, True)

    def side(west):
        fresh = edge_step(bins, west, halo, edge, inner, seas, gains, stay, go_x, go_y, wide, adv_ref, False, corner)
        for t, value in enumerate(fresh):
            out[:, lanes_of(t)] = value
        pack_half(fresh, west, bins, rows, halo_next, pack)

    on_each_side(second, side)


def ordered_late_kernel(bins, second, after, *refs):
    late_edge_kernel(bins, second, *refs)


def late_edge_kernel(bins, second, halo, edge, inner, seas, gains, stay, go_x, go_y, wide, out, adv_ref):
    def side(west):
        fresh = edge_step(bins, west, halo, edge, inner, seas, gains, stay, go_x, go_y, wide, adv_ref, True)
        for t, value in enumerate(fresh):
            write_tile(out, (), bins, t, value)

    on_each_side(second, side)


def last_edge_kernel(
    bins, second, halo, edge, inner, seas, gains, stay, go_x, go_y, wide, done_inner, done_edge, out, adv_ref, column, sems
):
    columns = out.shape[0]
    mine = jnp.where(west_flag(second), 0, columns - 1)
    copies = [
        pltpu.make_async_copy(done_inner, out.at[pl.ds(1, columns - 2)], sems.at[0]),
        pltpu.make_async_copy(done_edge, out.at[columns - 1 - mine], sems.at[1]),
    ]
    for copy in copies:
        copy.start()
    late_edge_kernel(bins, second, halo, edge, inner, seas, gains, stay, go_x, go_y, wide, column, adv_ref)
    copies.append(pltpu.make_async_copy(column, out.at[mine], sems.at[2]))
    copies[2].start()
    for copy in copies:
        copy.wait()


def edge_step(bins, west, halo, edge, inner, seas, gains, stay, go_x, go_y, wide, adv_ref, last, corner=None):
    tiles = lane_tiles(bins)
    columns = inner.shape[0] + 2
    rows = edge.shape[0] - 2 * DEPTH
    used = rows if last else edge.shape[0]
    near, mine = (0, 0) if west else (columns - 3, columns - 1)
    across = across_edge(halo, [inner[near, :, lanes_of(t)] for t in range(tiles)], west, bins, rows, not last, corner)
    for t in range(tiles):
        here = lanes_of(t)
        adv = advect(edge[:, here], across[t], stay[:, here], go_x[:, here], go_y[0:1, here], bins, t)
        adv_ref[:used, here] = adv[:used]
    product = jnp.dot(adv_ref[:used].astype(jnp.bfloat16), wide[...], preferred_element_type=jnp.float32)
    share = jnp.broadcast_to(product[:, -1:], (used, LANES)) * (dissipation / bins)
    s, g = seas[mine, :used], gains[mine, :used]
    return [combine(adv_ref[:used, lanes_of(t)], product[:, lanes_of(t)], s, g, share) for t in range(tiles)]


def inner_kernel(bins, edge_a, edge_b, inner, seas, gains, stay, go_x, go_y, wide, out, adv_ref, low_ref):
    tiles = lane_tiles(bins)
    count, tall = inner.shape[0], inner.shape[1]
    rows = adv_ref.shape[1]
    a_west = west_flag(False)
    for t in range(tiles):
        here = lanes_of(t)
        found = kinds(bins, t, is_east(bins))
        for c in range(count):
            west = east = None
            if True in found:
                west = inner[c - 1, :, here] if c else jnp.where(a_west, edge_a[:, here], edge_b[:, here])
            if False in found:
                east = inner[c + 1, :, here] if c < count - 1 else jnp.where(a_west, edge_b[:, here], edge_a[:, here])
            if west is None:
                across = east
            elif east is None:
                across = west
            else:
                across = jnp.where(eastward(bins, t, (tall, LANES)), west, east)
            adv = advect(inner[c, :, here], across, stay[:, here], go_x[:, here], go_y[0:1, here], bins, t)[:rows]
            adv_ref[c, :, here] = adv
            low_ref[c * rows : (c + 1) * rows, here] = adv.astype(jnp.bfloat16)
    product = jnp.dot(low_ref[...], wide[...], preferred_element_type=jnp.float32)
    for c in range(count):
        part = product[c * rows : (c + 1) * rows]
        share = jnp.broadcast_to(part[:, -1:], (rows, LANES)) * (dissipation / bins)
        for t in range(tiles):
            here = lanes_of(t)
            value = combine(adv_ref[c, :, here], part[:, here], seas[c + 1, :rows], gains[c + 1, :rows], share)
            if rows == tall:
                out[c, :, here] = value
            else:
                write_tile(out, (c,), bins, t, value)


def angle_table(bins, freqs):
    padded = lane_tiles(bins) * LANES
    table = np.zeros((8, padded), np.float32)
    theta = (np.arange(DIRS) + 0.5) * (2.0 * math.pi / DIRS)
    table[0, :bins] = np.repeat(0.225 * np.abs(np.cos(theta)), freqs)
    table[1, :bins] = np.repeat(0.45 * np.abs(np.sin(theta)), freqs)
    table[2, :] = -1.0
    table[2, :bins] = np.tile(np.arange(freqs), DIRS)
    return table


def steps(spectrum, sea_mask, ice_flags, wind_forcing, group_speed, coupling):
    columns, rows, bins = spectrum.shape
    tiles = lane_tiles(bins)
    padded = tiles * LANES
    tall = rows + 2 * DEPTH
    f32 = jnp.float32
    lon, lat = lax.axis_size("lon"), lax.axis_size("lat")
    lon_a, lon_b = swap_pairs(lon, 0, True), swap_pairs(lon, 1, True)
    lat_a, lat_b = swap_pairs(lat, 0, False), swap_pairs(lat, 1, False)
    vmem = pl.BlockSpec(memory_space=VMEM)
    smem = pl.BlockSpec(memory_space=SMEM)
    hbm = pl.BlockSpec(memory_space=pltpu.HBM)
    edge_shape = VMEM((tall, padded), f32)
    inner_shape = VMEM((columns - 2, tall, padded), f32)
    mask_shape = VMEM((columns, tall, LANES), f32)
    table_shape = VMEM((tall, padded), f32)

    def call(body, outs, ins, specs, scratch=(), aliases=None, flops=0, out_specs=None):
        return pl.pallas_call(
            body,
            out_shape=outs,
            in_specs=specs,
            out_specs=out_specs if out_specs is not None else jax.tree.map(lambda _: vmem, outs),
            scratch_shapes=list(scratch),
            input_output_aliases=aliases or {},
            cost_estimate=pl.CostEstimate(flops=flops, bytes_accessed=0, transcendentals=0),
            compiler_params=pltpu.CompilerParams(vmem_limit_bytes=24 * 1024 * 1024),
        )(*ins)

    send_a, send_b = call(
        functools.partial(first_kernel, bins),
        (VMEM((columns // 2 * (tiles - 1) + 1, 8, LANES), f32),) * 2,
        [pltpu.with_memory_space_constraint(x, pltpu.HBM) for x in (spectrum, sea_mask, ice_flags, wind_forcing)],
        [hbm] * 4,
        [VMEM((2, columns, 8, bins), f32), VMEM((columns, rows), sea_mask.dtype), VMEM((columns, rows), ice_flags.dtype),
         VMEM((columns, rows), f32), pltpu.SemaphoreType.DMA((5,))],
    )
    halo_b = lax.ppermute(send_b, "lat", lat_b)
    halo_a = lax.ppermute(send_a, "lat", lat_a)
    pack_own = VMEM((pack_count(rows, False), 8, LANES), f32)
    pack_shape = VMEM((pack_count(rows, True), 8, LANES), f32)
    corner_shape = VMEM((3, 8, LANES), f32)
    edge_a, edge_b, inner, seas, gains, pack_a, pack_b = call(
        functools.partial(load_kernel, bins),
        (edge_shape, edge_shape, inner_shape, mask_shape, mask_shape, pack_shape, pack_own),
        (spectrum, sea_mask, ice_flags, wind_forcing), [vmem] * 4, flops=1 << 24,
    )
    stay, go_x, go_y, wide = call(
        functools.partial(table_kernel, bins, rows),
        (table_shape, table_shape, VMEM((8, padded), f32), VMEM((padded, padded), jnp.bfloat16)),
        (group_speed, jnp.asarray(angle_table(bins, group_speed.shape[0])), coupling),
        [smem, vmem, vmem], flops=1 << 24,
    )
    edge_a, edge_b, inner, seas, gains, pack_a, corner_b = call(
        functools.partial(join_kernel, bins),
        (edge_shape, edge_shape, inner_shape, mask_shape, mask_shape, pack_shape, corner_shape),
        (halo_a, halo_b, edge_a, edge_b, inner, seas, gains, pack_a),
        [vmem] * 8,
        aliases={2: 0, 3: 1, 4: 2, 5: 3, 6: 4, 7: 5},
    )
    tables = (seas, gains, stay, go_x, go_y, wide)
    for step in range(STEPS):
        last = step == STEPS - 1
        halo_b = lax.ppermute(pack_b, "lon", lon_b)
        halo_a = lax.ppermute(pack_a, "lon", lon_a)
        if step == 0:
            corner = lax.ppermute(corner_b, "lon", lon_b)
        used = rows if last else tall
        new_inner = call(
            functools.partial(inner_kernel, bins), VMEM((columns - 2, rows, bins), f32) if last else inner_shape,
            (edge_a, edge_b, inner) + tables, [vmem] * 9,
            [VMEM((columns - 2, used, padded), f32), VMEM(((columns - 2) * used, padded), jnp.bfloat16)],
            flops=1 << 28,
        )
        if last:
            column = VMEM((rows, bins), f32)
            scratch = [VMEM((tall, padded), f32)]
            done_b = call(
                functools.partial(ordered_late_kernel, bins, True), column,
                (new_inner, halo_b, edge_b, inner) + tables, [vmem] * 10, scratch, flops=1 << 26,
            )
            return call(
                functools.partial(last_edge_kernel, bins, False), pltpu.HBM((columns, rows, bins), f32),
                (halo_a, edge_a, inner) + tables + (new_inner, done_b), [vmem] * 11,
                scratch + [column, pltpu.SemaphoreType.DMA((3,))], flops=1 << 26, out_specs=hbm,
            )
        fresh = []
        pack_next = VMEM((pack_count(rows, step < STEPS - 2), 8, LANES), f32)
        for second, halo, edge in ((False, halo_a, edge_a), (True, halo_b, edge_b)):
            body, ins = edge_kernel, (halo, edge, inner) + tables
            if step > 0:
                body, ins = ordered_edge_kernel, (new_inner,) + ins
            elif second:
                body, ins = first_edge_kernel, (corner,) + ins
            fresh.append(call(
                functools.partial(body, bins, second), (edge_shape, pack_next),
                ins, [vmem] * len(ins), [VMEM((tall, padded), f32)], flops=1 << 26,
            ))
        inner = new_inner
        (edge_a, pack_a), (edge_b, pack_b) = fresh


def solution(mesh):
    placed = (P("lon", "lat", None), P("lon", "lat"), P("lon", "lat"), P("lon", "lat"), P(), P())
    return jax.shard_map(steps, mesh=mesh, in_specs=placed, out_specs=P("lon", "lat", None), check_vma=False)
```

```python
import functools
import math

import jax
import jax.numpy as jnp
import numpy as np
from jax import lax
from jax.experimental import pallas as pl
from jax.experimental.pallas import tpu as pltpu
from jax.sharding import PartitionSpec as P


DIRS = 36
STEPS = 4
LANES = 128
DEPTH = 4

time_step = 0.2
dissipation = 0.5

VMEM = pltpu.VMEM
SMEM = pltpu.SMEM


def swap_pairs(size, first, wrap):
    pairs = []
    for i in range(first, size, 2):
        j = i + 1
        if j >= size:
            if not wrap:
                continue
            j = j % size
        pairs += [(i, j), (j, i)]
    return pairs


def lane_tiles(bins):
    return pl.cdiv(bins, LANES)


def lanes_of(tile):
    return slice(tile * LANES, (tile + 1) * LANES)


def lane_index(shape):
    return lax.broadcasted_iota(jnp.int32, shape, 1)


def row_index(shape):
    return lax.broadcasted_iota(jnp.int32, shape, 0)


def eastward(bins, tile, shape):
    bin_here = lane_index(shape) + tile * LANES
    quarter = bins // 4
    return (bin_here < quarter) | (bin_here >= bins - quarter)


def northward(bins, tile, shape):
    return lane_index(shape) + tile * LANES < bins // 2


def kinds(bins, tile, test):
    low, high = tile * LANES, min((tile + 1) * LANES, bins)
    return {bool(test(b)) for b in range(low, high)}


def is_east(bins):
    return lambda b: b < bins // 4 or b >= bins - bins // 4


def is_north(bins):
    return lambda b: b < bins // 2


def upwind_lat(f, bins, tile):
    shape = f.shape
    rows = shape[0]
    found = kinds(bins, tile, is_north(bins))
    south = pltpu.roll(f, 1, 0) if True in found else None
    north = pltpu.roll(f, rows - 1, 0) if False in found else None
    if south is None:
        return north
    if north is None:
        return south
    return jnp.where(northward(bins, tile, shape), south, north)


def advect(f, across, stay, go_x, go_y, bins, tile):
    along = upwind_lat(f, bins, tile)
    return stay * f + go_x * across + go_y * along


def turn(value, shift):
    shift = shift % LANES
    return pltpu.roll(value, shift, 1) if shift else value


def pack_plan(bins, west):
    split = bins // 4 - LANES
    high = bins - bins // 4 - 3 * LANES
    width = 2 * split
    return split, high, width, LANES - width, (split if west else high)


def pack_count(rows, halo):
    blocks = rows // 8
    return 2 * blocks + blocks // 2 + 1 + (2 if halo else 0)


def half_parts(t, west, bins):
    split, high, _, _, _ = pack_plan(bins, west)
    lane = lane_index(t[0].shape)
    if west:
        return t[2], jnp.where(lane < high, t[3], t[1]), t[1]
    return t[0], t[4], jnp.where(lane < split, t[1], jnp.where(lane >= high, t[3], turn(t[5], split)))


def pack_half(tiles, west, bins, rows, halo, out):
    _, _, width, kept, start = pack_plan(bins, west)
    rest = width - kept
    blocks = rows // 8
    half = blocks // 2
    lane = lane_index((8, LANES))

    left = jnp.zeros((8, LANES), jnp.float32)
    held = {}
    for block in range(blocks + (1 if halo else 0)):
        full, other, part = half_parts([tile[8 * block : 8 * block + 8] for tile in tiles], west, bins)
        if block < blocks:
            out[block] = full
            out[blocks + block] = other
            if block < half:
                held[block] = turn(part, -start)
            else:
                k = block - half
                out[2 * blocks + k] = jnp.where(lane < width, held.pop(k), turn(part, width - start))
                low = rest * k
                left = jnp.where((lane >= low) & (lane < low + rest), turn(part, low - kept - start), left)
        else:
            left = jnp.where(lane >= half * rest, turn(part, half * rest - start), left)
            out[2 * blocks + half + 1] = full
            out[2 * blocks + half + 2] = other
    out[2 * blocks + half] = left


def pack_corner(parts, before, west, bins, rows, out):
    _, _, width, kept, start = pack_plan(bins, west)
    rest = width - kept
    half = rows // 16
    spot = 5 * half
    lane = lane_index((8, LANES))
    out[spot] = jnp.where(lane >= half * rest, turn(parts[2], half * rest - start), before[spot])
    out[spot + 1] = parts[0]
    out[spot + 2] = parts[1]


def across_edge(halo, inner, west, bins, rows, with_halo, corner=None):
    split, high, width, kept, start = pack_plan(bins, not west)
    rest = width - kept
    blocks = rows // 8
    half = blocks // 2
    lane = lane_index((8, LANES))
    left = halo[2 * blocks + half]
    found = [[] for _ in inner]
    for block in range(blocks + 1):
        near = [tile[8 * block : 8 * block + 8] for tile in inner]
        if block == blocks and not with_halo:
            new = near
        else:
            if block == blocks and corner is not None:
                full, other, part = corner[0], corner[1], corner[2]
            elif block == blocks:
                full, other = halo[2 * blocks + half + 1], halo[2 * blocks + half + 2]
                part = turn(left, start - half * rest)
            else:
                full, other = halo[block], halo[blocks + block]
                if block < half:
                    part = turn(halo[2 * blocks + block], start)
                else:
                    k = block - half
                    early = (lane >= high) | (lane < split) if west else lane < start + kept
                    part = jnp.where(early, turn(halo[2 * blocks + k], start - width), turn(left, start + kept - rest * k))
            if west:
                new = [
                    full, jnp.where(lane < split, part, near[1]), near[2],
                    jnp.where(lane >= high, part, near[3]), other, turn(part, -split),
                ]
            else:
                new = [
                    near[0], jnp.where(lane < split, near[1], jnp.where(lane < high, part, other)), full,
                    jnp.where(lane < high, other, near[3]), near[4], near[5],
                ]
        for k, value in enumerate(new):
            found[k].append(value)
    return [jnp.concatenate(values, axis=0) for values in found]


def on_each_side(second, body):
    west = west_flag(second)

    @pl.when(west)
    def _():
        body(True)

    @pl.when(jnp.logical_not(west))
    def _():
        body(False)


def west_flag(second):
    odd = lax.rem(lax.axis_index("lon"), 2)
    return (1 - odd if second else odd) == 1


def south_flag(second):
    odd = lax.rem(lax.axis_index("lat"), 2)
    return (1 - odd if second else odd) == 1


def read_tile(ref, where, bins, tile):
    low, high = tile * LANES, min((tile + 1) * LANES, bins)
    value = ref[where + (slice(None), slice(low, high))]
    if high - low == LANES:
        return value
    return jnp.concatenate([value, jnp.zeros((value.shape[0], LANES - (high - low)), value.dtype)], axis=1)


def write_tile(ref, where, bins, tile, value):
    rows, low, high = ref.shape[-2], tile * LANES, min((tile + 1) * LANES, bins)
    ref[where + (slice(None), slice(low, high))] = value[:rows, : high - low]


def masks_kernel_part(sea_ref, ice_ref, wind_ref):
    sea = sea_ref[...].astype(jnp.float32)
    gain = 1.0 + time_step * (wind_ref[...] * (1.0 - ice_ref[...].astype(jnp.float32)))
    _, rows = sea.shape
    sea = jnp.concatenate([sea, gain], axis=1)
    turned = jnp.transpose(sea)
    return turned[:rows], turned[rows:]


def first_kernel(bins, spectrum, sea_hbm, ice_hbm, wind_hbm, out_a, out_b, edge, sea_ref, ice_ref, wind_ref, sems):
    columns, rows = sea_ref.shape
    copies = []
    masks = [
        pltpu.make_async_copy(source, target, sems.at[2 + k])
        for k, (source, target) in enumerate(((sea_hbm, sea_ref), (ice_hbm, ice_ref), (wind_hbm, wind_ref)))
    ]
    for copy in masks:
        copy.start()
    for c in range(columns):
        for k, start in enumerate((0, rows - 8)):
            copy = pltpu.make_async_copy(
                spectrum.at[c, pl.ds(start, 8)], edge.at[k, c], sems.at[k]
            )
            copy.start()
            copies.append(copy)
    for copy in masks:
        copy.wait()
    sea, gain = masks_kernel_part(sea_ref, ice_ref, wind_ref)
    shape = (8, LANES)
    lane = lane_index(shape)
    row = row_index(shape)
    used = bins % LANES
    for copy in copies:
        copy.wait()
    tiles = lane_tiles(bins)
    space = LANES // (columns // 2)
    for second, out in ((False, out_a), (True, out_b)):
        to_south = south_flag(second)
        ends = jnp.zeros(shape, jnp.float32)
        for pair in range(columns // 2):
            for tile in range(tiles):
                halves = []
                for c in (2 * pair, 2 * pair + 1):
                    low, high = read_tile(edge, (0, c), bins, tile), read_tile(edge, (1, c), bins, tile)
                    here = jnp.where(to_south, low, high)
                    s = jnp.where(to_south, sea[0:8, c : c + 1], sea[rows - 8 : rows, c : c + 1])
                    s = jnp.broadcast_to(s, shape)
                    value = here * s
                    if tile == tiles - 1:
                        g = jnp.where(to_south, gain[0:8, c : c + 1], gain[rows - 8 : rows, c : c + 1])
                        g = jnp.broadcast_to(g, shape)
                        value = jnp.where(lane < used, value, jnp.where(lane == used, s, g))
                    halves.append(value)
                first, other = halves
                keep = (row < DEPTH) == to_south
                value = jnp.where(keep, first, pltpu.roll(other, DEPTH, 0))
                if tile < tiles - 1:
                    out[pair * (tiles - 1) + tile] = value
                else:
                    here = (lane >= pair * space) & (lane < (pair + 1) * space)
                    ends = jnp.where(here, turn(value, pair * space), ends)
        out[columns // 2 * (tiles - 1)] = ends


def table_kernel(bins, rows, speed_ref, angle_ref, coupling_ref, stay, go_x, go_y, wide):
    tiles = lane_tiles(bins)
    padded = tiles * LANES
    used = bins % LANES
    shape = (rows + 2 * DEPTH, LANES)
    row = row_index(shape)
    here = jnp.where(row >= rows + DEPTH, row - rows - 2 * DEPTH, row) + lax.axis_index("lat") * rows
    total = rows * lax.axis_size("lat")
    latitude = (-60.0 + 120.0 * (here.astype(jnp.float32) + 0.5) / total) * (math.pi / 180.0)
    over = 1.0 / jnp.cos(latitude)
    count = speed_ref.shape[0]
    for tile in range(tiles):
        which = angle_ref[2:3, lanes_of(tile)]
        speed = jnp.zeros((1, LANES), jnp.float32)
        for k in range(count):
            speed = jnp.where(which == float(k), speed_ref[k], speed)
        x = (angle_ref[0:1, lanes_of(tile)] * speed) * over
        y = angle_ref[1:2, lanes_of(tile)] * speed
        go_x[:, lanes_of(tile)] = x
        go_y[:, lanes_of(tile)] = jnp.broadcast_to(y, (8, LANES))
        stay[:, lanes_of(tile)] = 1.0 - x - y
    body = bins - used
    wide[:, :body] = jnp.concatenate(
        [coupling_ref[:, :body], jnp.zeros((padded - bins, body), jnp.bfloat16)], axis=0
    )
    tail = jnp.concatenate([coupling_ref[:, body:], jnp.ones((bins, padded - bins), jnp.bfloat16)], axis=1)
    wide[:, body:] = jnp.concatenate([tail, jnp.zeros((padded - bins, LANES), jnp.bfloat16)], axis=0)


def load_kernel(bins, spectrum, sea_ref, ice_ref, wind_ref, edge_a, edge_b, inner, seas, gains, pack_a, pack_b):
    columns, rows = sea_ref.shape
    tiles = lane_tiles(bins)
    used = bins % LANES
    sea, gain = masks_kernel_part(sea_ref, ice_ref, wind_ref)
    for c in range(columns):
        s = jnp.broadcast_to(sea[:, c : c + 1], (rows, LANES))
        seas[c, :rows] = time_step * s
        gains[c, :rows] = s * jnp.broadcast_to(gain[:, c : c + 1], (rows, LANES))
    lane = lane_index((rows, LANES))

    def put(target, c):
        s = seas[c, :rows] != 0.0
        for tile in range(tiles):
            value = read_tile(spectrum, (c,), bins, tile)
            keep = s
            if tile == tiles - 1:
                keep = s & (lane < used)
            target[:rows, lanes_of(tile)] = jnp.where(keep, value, 0.0)

    for c in range(1, columns - 1):
        put(inner.at[c - 1], c)
    for second, target, pack in ((False, edge_a, pack_a), (True, edge_b, pack_b)):

        def side(west, target=target, pack=pack):
            put(target, 0 if west else columns - 1)
            pack_half([target[:rows, lanes_of(t)] for t in range(tiles)], west, bins, rows, False, pack)

        on_each_side(second, side)


def join_kernel(
    bins, halo_a, halo_b, edge_a_in, edge_b_in, inner_in, seas_in, gains_in, pack_in,
    edge_a, edge_b, inner, seas, gains, pack_a, corner_b,
):
    columns = seas.shape[0]
    rows = seas.shape[1] - 2 * DEPTH
    tiles = lane_tiles(bins)
    used = bins % LANES
    shape = (8, LANES)
    row = row_index(shape)
    lane = lane_index(shape)
    a_south = south_flag(False)
    top = row < DEPTH
    values = []
    for c in range(columns):
        tile_values = []
        for tile in range(tiles):
            spot = columns // 2 * (tiles - 1) if tile == tiles - 1 else c // 2 * (tiles - 1) + tile
            from_a, from_b = halo_a[spot], halo_b[spot]
            if tile == tiles - 1:
                back = -(c // 2) * (LANES // (columns // 2))
                from_a, from_b = turn(from_a, back), turn(from_b, back)
            low, high = jnp.where(a_south, from_a, from_b), jnp.where(a_south, from_b, from_a)
            if c % 2:
                low, high = pltpu.roll(low, DEPTH, 0), pltpu.roll(high, DEPTH, 0)
            tile_values.append(jnp.where(top, high, low))
        last = tile_values[-1]
        s = jnp.broadcast_to(last[:, used : used + 1], shape)
        g = jnp.broadcast_to(last[:, used + 1 : used + 2], shape)
        seas[c, rows:] = time_step * s
        gains[c, rows:] = s * g
        tile_values[-1] = jnp.where(lane < used, last, 0.0)
        values.append(tile_values)
    for tile in range(tiles):
        for c in range(1, columns - 1):
            inner[c - 1, rows:, lanes_of(tile)] = values[c][tile]
    for second, target in ((False, edge_a), (True, edge_b)):

        def side(west, second=second, target=target):
            mine = values[0 if west else columns - 1]
            for tile in range(tiles):
                target[rows:, lanes_of(tile)] = mine[tile]
            parts = half_parts(mine, west, bins)
            if second:
                for k, value in enumerate(parts):
                    corner_b[k] = value
            else:
                pack_corner(parts, pack_in, west, bins, rows, pack_a)

        on_each_side(second, side)


def ordered_first_kernel(bins, second, after, corner, *refs):
    edge_kernel(bins, second, *refs, corner=corner)


def ordered_edge_kernel(bins, second, after, *refs):
    edge_kernel(bins, second, *refs)


def edge_kernel(
    bins, second, halo, edge, inner, seas, gains, stay, go_x, go_y, wide, out, pack, adv_ref, corner=None
):
    rows = edge.shape[0] - 2 * DEPTH
    halo_next = pack.shape[0] == pack_count(rows, True)

    def side(west):
        fresh = edge_step(bins, west, halo, edge, inner, seas, gains, stay, go_x, go_y, wide, adv_ref, False, corner)
        for t, value in enumerate(fresh):
            out[:, lanes_of(t)] = value
        pack_half(fresh, west, bins, rows, halo_next, pack)

    on_each_side(second, side)


def ordered_late_kernel(bins, second, after, *refs):
    late_edge_kernel(bins, second, *refs)


def late_edge_kernel(bins, second, halo, edge, inner, seas, gains, stay, go_x, go_y, wide, out, adv_ref):
    def side(west):
        fresh = edge_step(bins, west, halo, edge, inner, seas, gains, stay, go_x, go_y, wide, adv_ref, True)
        for t, value in enumerate(fresh):
            write_tile(out, (), bins, t, value)

    on_each_side(second, side)


def last_edge_kernel(
    bins, second, halo, edge, inner, seas, gains, stay, go_x, go_y, wide, done_inner, done_edge, out, adv_ref, column, sems
):
    columns = out.shape[0]
    mine = jnp.where(west_flag(second), 0, columns - 1)
    copies = [
        pltpu.make_async_copy(done_inner, out.at[pl.ds(1, columns - 2)], sems.at[0]),
        pltpu.make_async_copy(done_edge, out.at[columns - 1 - mine], sems.at[1]),
    ]
    for copy in copies:
        copy.start()
    late_edge_kernel(bins, second, halo, edge, inner, seas, gains, stay, go_x, go_y, wide, column, adv_ref)
    copies.append(pltpu.make_async_copy(column, out.at[mine], sems.at[2]))
    copies[2].start()
    for copy in copies:
        copy.wait()


def edge_step(bins, west, halo, edge, inner, seas, gains, stay, go_x, go_y, wide, adv_ref, last, corner=None):
    tiles = lane_tiles(bins)
    columns = inner.shape[0] + 2
    rows = edge.shape[0] - 2 * DEPTH
    used = rows if last else edge.shape[0]
    near, mine = (0, 0) if west else (columns - 3, columns - 1)
    across = across_edge(halo, [inner[near, :, lanes_of(t)] for t in range(tiles)], west, bins, rows, not last, corner)
    for t in range(tiles):
        here = lanes_of(t)
        adv = advect(edge[:, here], across[t], stay[:, here], go_x[:, here], go_y[0:1, here], bins, t)
        adv_ref[:used, here] = adv[:used]
    low = adv_ref[:used].astype(jnp.bfloat16)
    s, g = seas[mine, :used], gains[mine, :used]
    fresh = [None] * tiles
    keep = None
    for block in lane_blocks(tiles):
        product = jnp.dot(low, wide[:, block[0] * LANES : (block[-1] + 1) * LANES], preferred_element_type=jnp.float32)
        if keep is None:
            share = jnp.broadcast_to(product[:, -1:], (used, LANES)) * (dissipation / bins)
            keep = g - s * share
        for k, t in enumerate(block):
            fresh[t] = adv_ref[:used, lanes_of(t)] * keep + s * product[:, lanes_of(k)]
    return fresh


def lane_blocks(tiles):
    return [(t - 1, t) for t in range(tiles - 1, 0, -2)]


def inner_kernel(bins, edge_a, edge_b, inner, seas, gains, stay, go_x, go_y, wide, out, adv_ref, low_ref, keep_ref):
    tiles = lane_tiles(bins)
    count, tall = inner.shape[0], inner.shape[1]
    rows = adv_ref.shape[0] // count
    a_west = west_flag(False)
    parts = 2
    if count % parts:
        parts = 1
    for part in range(parts):
        group = range(part * count // parts, (part + 1) * count // parts)
        whole = slice(group[0] * rows, (group[-1] + 1) * rows)
        for t in range(tiles):
            here = lanes_of(t)
            found = kinds(bins, t, is_east(bins))
            for c in group:
                west = east = None
                if True in found:
                    west = inner[c - 1, :, here] if c else jnp.where(a_west, edge_a[:, here], edge_b[:, here])
                if False in found:
                    east = inner[c + 1, :, here] if c < count - 1 else jnp.where(a_west, edge_b[:, here], edge_a[:, here])
                if west is None:
                    across = east
                elif east is None:
                    across = west
                else:
                    across = jnp.where(eastward(bins, t, (tall, LANES)), west, east)
                adv = advect(inner[c, :, here], across, stay[:, here], go_x[:, here], go_y[0:1, here], bins, t)[:rows]
                adv_ref[c * rows : (c + 1) * rows, here] = adv
        low_ref[whole] = adv_ref[whole].astype(jnp.bfloat16)
        for block in lane_blocks(tiles):
            product = jnp.dot(
                low_ref[whole], wide[:, block[0] * LANES : (block[-1] + 1) * LANES], preferred_element_type=jnp.float32
            )
            for c in group:
                span = slice(c * rows, (c + 1) * rows)
                mine = slice((c - group[0]) * rows, (c - group[0] + 1) * rows)
                s = seas[c + 1, :rows]
                if block[-1] == tiles - 1:
                    share = jnp.broadcast_to(product[mine, -1:], (rows, LANES)) * (dissipation / bins)
                    keep_ref[span] = gains[c + 1, :rows] - s * share
                for k, t in enumerate(block):
                    value = adv_ref[span, lanes_of(t)] * keep_ref[span] + s * product[mine, lanes_of(k)]
                    if rows == tall:
                        out[c, :, lanes_of(t)] = value
                    else:
                        write_tile(out, (c,), bins, t, value)


def angle_table(bins, freqs):
    padded = lane_tiles(bins) * LANES
    table = np.zeros((8, padded), np.float32)
    theta = (np.arange(DIRS) + 0.5) * (2.0 * math.pi / DIRS)
    table[0, :bins] = np.repeat(0.225 * np.abs(np.cos(theta)), freqs)
    table[1, :bins] = np.repeat(0.45 * np.abs(np.sin(theta)), freqs)
    table[2, :] = -1.0
    table[2, :bins] = np.tile(np.arange(freqs), DIRS)
    return table


def steps(spectrum, sea_mask, ice_flags, wind_forcing, group_speed, coupling):
    columns, rows, bins = spectrum.shape
    tiles = lane_tiles(bins)
    padded = tiles * LANES
    tall = rows + 2 * DEPTH
    f32 = jnp.float32
    lon, lat = lax.axis_size("lon"), lax.axis_size("lat")
    lon_a, lon_b = swap_pairs(lon, 0, True), swap_pairs(lon, 1, True)
    lat_a, lat_b = swap_pairs(lat, 0, False), swap_pairs(lat, 1, False)
    vmem = pl.BlockSpec(memory_space=VMEM)
    smem = pl.BlockSpec(memory_space=SMEM)
    hbm = pl.BlockSpec(memory_space=pltpu.HBM)
    edge_shape = VMEM((tall, padded), f32)
    inner_shape = VMEM((columns - 2, tall, padded), f32)
    mask_shape = VMEM((columns, tall, LANES), f32)
    table_shape = VMEM((tall, padded), f32)

    def call(body, outs, ins, specs, scratch=(), aliases=None, flops=0, out_specs=None):
        return pl.pallas_call(
            body,
            out_shape=outs,
            in_specs=specs,
            out_specs=out_specs if out_specs is not None else jax.tree.map(lambda _: vmem, outs),
            scratch_shapes=list(scratch),
            input_output_aliases=aliases or {},
            cost_estimate=pl.CostEstimate(flops=flops, bytes_accessed=0, transcendentals=0),
            compiler_params=pltpu.CompilerParams(vmem_limit_bytes=24 * 1024 * 1024),
        )(*ins)

    send_a, send_b = call(
        functools.partial(first_kernel, bins),
        (VMEM((columns // 2 * (tiles - 1) + 1, 8, LANES), f32),) * 2,
        [pltpu.with_memory_space_constraint(x, pltpu.HBM) for x in (spectrum, sea_mask, ice_flags, wind_forcing)],
        [hbm] * 4,
        [VMEM((2, columns, 8, bins), f32), VMEM((columns, rows), sea_mask.dtype), VMEM((columns, rows), ice_flags.dtype),
         VMEM((columns, rows), f32), pltpu.SemaphoreType.DMA((5,))],
    )
    halo_b = lax.ppermute(send_b, "lat", lat_b)
    halo_a = lax.ppermute(send_a, "lat", lat_a)
    pack_own = VMEM((pack_count(rows, False), 8, LANES), f32)
    pack_shape = VMEM((pack_count(rows, True), 8, LANES), f32)
    corner_shape = VMEM((3, 8, LANES), f32)
    edge_a, edge_b, inner, seas, gains, pack_a, pack_b = call(
        functools.partial(load_kernel, bins),
        (edge_shape, edge_shape, inner_shape, mask_shape, mask_shape, pack_shape, pack_own),
        (spectrum, sea_mask, ice_flags, wind_forcing), [vmem] * 4, flops=1 << 24,
    )
    stay, go_x, go_y, wide = call(
        functools.partial(table_kernel, bins, rows),
        (table_shape, table_shape, VMEM((8, padded), f32), VMEM((padded, padded), jnp.bfloat16)),
        (group_speed, jnp.asarray(angle_table(bins, group_speed.shape[0])), coupling),
        [smem, vmem, vmem], flops=1 << 24,
    )
    edge_a, edge_b, inner, seas, gains, pack_a, corner_b = call(
        functools.partial(join_kernel, bins),
        (edge_shape, edge_shape, inner_shape, mask_shape, mask_shape, pack_shape, corner_shape),
        (halo_a, halo_b, edge_a, edge_b, inner, seas, gains, pack_a),
        [vmem] * 8,
        aliases={2: 0, 3: 1, 4: 2, 5: 3, 6: 4, 7: 5},
    )
    tables = (seas, gains, stay, go_x, go_y, wide)
    for step in range(STEPS):
        last = step == STEPS - 1
        halo_b = lax.ppermute(pack_b, "lon", lon_b)
        halo_a = lax.ppermute(pack_a, "lon", lon_a)
        if step == 0:
            corner = lax.ppermute(corner_b, "lon", lon_b)
        used = rows if last else tall
        new_inner = call(
            functools.partial(inner_kernel, bins), VMEM((columns - 2, rows, bins), f32) if last else inner_shape,
            (edge_a, edge_b, inner) + tables, [vmem] * 9,
            [VMEM(((columns - 2) * used, padded), f32), VMEM(((columns - 2) * used, padded), jnp.bfloat16),
             VMEM(((columns - 2) * used, LANES), f32)],
            flops=1 << 28,
        )
        if last:
            column = VMEM((rows, bins), f32)
            scratch = [VMEM((tall, padded), f32)]
            done_b = call(
                functools.partial(ordered_late_kernel, bins, True), column,
                (new_inner, halo_b, edge_b, inner) + tables, [vmem] * 10, scratch, flops=1 << 26,
            )
            return call(
                functools.partial(last_edge_kernel, bins, False), pltpu.HBM((columns, rows, bins), f32),
                (halo_a, edge_a, inner) + tables + (new_inner, done_b), [vmem] * 11,
                scratch + [column, pltpu.SemaphoreType.DMA((3,))], flops=1 << 26, out_specs=hbm,
            )
        fresh = []
        pack_next = VMEM((pack_count(rows, step < STEPS - 2), 8, LANES), f32)
        for second, halo, edge in ((False, halo_a, edge_a), (True, halo_b, edge_b)):
            body, ins = edge_kernel, (halo, edge, inner) + tables
            if step > 0:
                body, ins = ordered_edge_kernel, (new_inner,) + ins
            elif second:
                body, ins = ordered_first_kernel, (new_inner, corner) + ins
            fresh.append(call(
                functools.partial(body, bins, second), (edge_shape, pack_next),
                ins, [vmem] * len(ins), [VMEM((tall, padded), f32)], flops=1 << 26,
            ))
        inner = new_inner
        (edge_a, pack_a), (edge_b, pack_b) = fresh


def solution(mesh):
    placed = (P("lon", "lat", None), P("lon", "lat"), P("lon", "lat"), P("lon", "lat"), P(), P())
    return jax.shard_map(steps, mesh=mesh, in_specs=placed, out_specs=P("lon", "lat", None), check_vma=False)
```

```python
import functools
import math

import jax
import jax.numpy as jnp
import numpy as np
from jax import lax
from jax.experimental import pallas as pl
from jax.experimental.pallas import tpu as pltpu
from jax.sharding import PartitionSpec as P


DIRS = 36
STEPS = 4
LANES = 128
DEPTH = 4

time_step = 0.2
dissipation = 0.5

VMEM = pltpu.VMEM
SMEM = pltpu.SMEM


def swap_pairs(size, first, wrap):
    pairs = []
    for i in range(first, size, 2):
        j = i + 1
        if j >= size:
            if not wrap:
                continue
            j = j % size
        pairs += [(i, j), (j, i)]
    return pairs


def lane_tiles(bins):
    return pl.cdiv(bins, LANES)


def lanes_of(tile):
    return slice(tile * LANES, (tile + 1) * LANES)


def lane_index(shape):
    return lax.broadcasted_iota(jnp.int32, shape, 1)


def row_index(shape):
    return lax.broadcasted_iota(jnp.int32, shape, 0)


def eastward(bins, tile, shape):
    bin_here = lane_index(shape) + tile * LANES
    quarter = bins // 4
    return (bin_here < quarter) | (bin_here >= bins - quarter)


def northward(bins, tile, shape):
    return lane_index(shape) + tile * LANES < bins // 2


def kinds(bins, tile, test):
    low, high = tile * LANES, min((tile + 1) * LANES, bins)
    return {bool(test(b)) for b in range(low, high)}


def is_east(bins):
    return lambda b: b < bins // 4 or b >= bins - bins // 4


def is_north(bins):
    return lambda b: b < bins // 2


def upwind_lat(f, bins, tile):
    shape = f.shape
    rows = shape[0]
    found = kinds(bins, tile, is_north(bins))
    south = pltpu.roll(f, 1, 0) if True in found else None
    north = pltpu.roll(f, rows - 1, 0) if False in found else None
    if south is None:
        return north
    if north is None:
        return south
    return jnp.where(northward(bins, tile, shape), south, north)


def advect(f, across, stay, go_x, go_y, bins, tile):
    along = upwind_lat(f, bins, tile)
    return stay * f + go_x * across + go_y * along


def turn(value, shift):
    shift = shift % LANES
    return pltpu.roll(value, shift, 1) if shift else value


def pack_plan(bins, west):
    split = bins // 4 - LANES
    high = bins - bins // 4 - 3 * LANES
    width = 2 * split
    return split, high, width, LANES - width, (split if west else high)


def pack_count(rows, halo):
    blocks = rows // 8
    return 2 * blocks + blocks // 2 + 1 + (2 if halo else 0)


def half_parts(t, west, bins):
    split, high, _, _, _ = pack_plan(bins, west)
    lane = lane_index(t[0].shape)
    if west:
        return t[2], jnp.where(lane < high, t[3], t[1]), t[1]
    return t[0], t[4], jnp.where(lane < split, t[1], jnp.where(lane >= high, t[3], turn(t[5], split)))


def pack_half(tiles, west, bins, rows, halo, out):
    _, _, width, kept, start = pack_plan(bins, west)
    rest = width - kept
    blocks = rows // 8
    half = blocks // 2
    lane = lane_index((8, LANES))

    left = jnp.zeros((8, LANES), jnp.float32)
    held = {}
    for block in range(blocks + (1 if halo else 0)):
        full, other, part = half_parts([tile[8 * block : 8 * block + 8] for tile in tiles], west, bins)
        if block < blocks:
            out[block] = full
            out[blocks + block] = other
            if block < half:
                held[block] = turn(part, -start)
            else:
                k = block - half
                out[2 * blocks + k] = jnp.where(lane < width, held.pop(k), turn(part, width - start))
                low = rest * k
                left = jnp.where((lane >= low) & (lane < low + rest), turn(part, low - kept - start), left)
        else:
            left = jnp.where(lane >= half * rest, turn(part, half * rest - start), left)
            out[2 * blocks + half + 1] = full
            out[2 * blocks + half + 2] = other
    out[2 * blocks + half] = left


def pack_corner(parts, before, west, bins, rows, out):
    _, _, width, kept, start = pack_plan(bins, west)
    rest = width - kept
    half = rows // 16
    spot = 5 * half
    lane = lane_index((8, LANES))
    out[spot] = jnp.where(lane >= half * rest, turn(parts[2], half * rest - start), before[spot])
    out[spot + 1] = parts[0]
    out[spot + 2] = parts[1]


def across_edge(halo, inner, west, bins, rows, with_halo):
    split, high, width, kept, start = pack_plan(bins, not west)
    rest = width - kept
    blocks = rows // 8
    half = blocks // 2
    lane = lane_index((8, LANES))
    left = halo[2 * blocks + half]
    found = [[] for _ in inner]
    for block in range(blocks + 1):
        near = [tile[8 * block : 8 * block + 8] for tile in inner]
        if block == blocks and not with_halo:
            new = near
        else:
            if block == blocks:
                full, other = halo[2 * blocks + half + 1], halo[2 * blocks + half + 2]
                part = turn(left, start - half * rest)
            else:
                full, other = halo[block], halo[blocks + block]
                if block < half:
                    part = turn(halo[2 * blocks + block], start)
                else:
                    k = block - half
                    early = (lane >= high) | (lane < split) if west else lane < start + kept
                    part = jnp.where(early, turn(halo[2 * blocks + k], start - width), turn(left, start + kept - rest * k))
            if west:
                new = [
                    full, jnp.where(lane < split, part, near[1]), near[2],
                    jnp.where(lane >= high, part, near[3]), other, turn(part, -split),
                ]
            else:
                new = [
                    near[0], jnp.where(lane < split, near[1], jnp.where(lane < high, part, other)), full,
                    jnp.where(lane < high, other, near[3]), near[4], near[5],
                ]
        for k, value in enumerate(new):
            found[k].append(value)
    return [jnp.concatenate(values, axis=0) for values in found]


def on_each_side(second, body):
    west = west_flag(second)

    @pl.when(west)
    def _():
        body(True)

    @pl.when(jnp.logical_not(west))
    def _():
        body(False)


def west_flag(second):
    odd = lax.rem(lax.axis_index("lon"), 2)
    return (1 - odd if second else odd) == 1


def south_flag(second):
    odd = lax.rem(lax.axis_index("lat"), 2)
    return (1 - odd if second else odd) == 1


def read_tile(ref, where, bins, tile):
    low, high = tile * LANES, min((tile + 1) * LANES, bins)
    value = ref[where + (slice(None), slice(low, high))]
    if high - low == LANES:
        return value
    return jnp.concatenate([value, jnp.zeros((value.shape[0], LANES - (high - low)), value.dtype)], axis=1)


def write_tile(ref, where, bins, tile, value):
    rows, low, high = ref.shape[-2], tile * LANES, min((tile + 1) * LANES, bins)
    ref[where + (slice(None), slice(low, high))] = value[:rows, : high - low]


def masks_kernel_part(sea_ref, ice_ref, wind_ref):
    sea = sea_ref[...].astype(jnp.float32)
    gain = 1.0 + time_step * (wind_ref[...] * (1.0 - ice_ref[...].astype(jnp.float32)))
    _, rows = sea.shape
    sea = jnp.concatenate([sea, gain], axis=1)
    turned = jnp.transpose(sea)
    return turned[:rows], turned[rows:]


def column_pairs(columns):
    return [(0, columns - 1)] + [(c, c + 1) for c in range(1, columns - 1, 2)]


def halo_tiles(pairs, tiles):
    return pairs * (tiles - 1) + 1


def first_kernel(
    bins, spectrum, sea_hbm, ice_hbm, wind_hbm, out_a, out_b, out_c, edge, sea_ref, ice_ref, wind_ref, sems
):
    columns, rows = sea_ref.shape
    copies = []
    masks = [
        pltpu.make_async_copy(source, target, sems.at[2 + k])
        for k, (source, target) in enumerate(((sea_hbm, sea_ref), (ice_hbm, ice_ref), (wind_hbm, wind_ref)))
    ]
    for copy in masks:
        copy.start()
    for c in range(columns):
        for k, start in enumerate((0, rows - 8)):
            copy = pltpu.make_async_copy(
                spectrum.at[c, pl.ds(start, 8)], edge.at[k, c], sems.at[k]
            )
            copy.start()
            copies.append(copy)
    for copy in masks:
        copy.wait()
    sea, gain = masks_kernel_part(sea_ref, ice_ref, wind_ref)
    shape = (8, LANES)
    lane = lane_index(shape)
    row = row_index(shape)
    used = bins % LANES
    for copy in copies:
        copy.wait()
    tiles = lane_tiles(bins)
    pairs = column_pairs(columns)
    for second, group, out in ((False, pairs, out_a), (True, pairs[:1], out_b), (True, pairs[1:], out_c)):
        to_south = south_flag(second)
        space = LANES // len(group)
        ends = jnp.zeros(shape, jnp.float32)
        for index, pair in enumerate(group):
            for tile in range(tiles):
                halves = []
                for c in pair:
                    low, high = read_tile(edge, (0, c), bins, tile), read_tile(edge, (1, c), bins, tile)
                    here = jnp.where(to_south, low, high)
                    s = jnp.where(to_south, sea[0:8, c : c + 1], sea[rows - 8 : rows, c : c + 1])
                    s = jnp.broadcast_to(s, shape)
                    value = here * s
                    if tile == tiles - 1:
                        g = jnp.where(to_south, gain[0:8, c : c + 1], gain[rows - 8 : rows, c : c + 1])
                        g = jnp.broadcast_to(g, shape)
                        value = jnp.where(lane < used, value, jnp.where(lane == used, s, g))
                    halves.append(value)
                first, other = halves
                keep = (row < DEPTH) == to_south
                value = jnp.where(keep, first, pltpu.roll(other, DEPTH, 0))
                if tile < tiles - 1:
                    out[index * (tiles - 1) + tile] = value
                else:
                    here = (lane >= index * space) & (lane < (index + 1) * space)
                    ends = jnp.where(here, turn(value, index * space), ends)
        out[len(group) * (tiles - 1)] = ends


def table_kernel(bins, rows, speed_ref, angle_ref, coupling_ref, stay, go_x, go_y, wide):
    tiles = lane_tiles(bins)
    padded = tiles * LANES
    used = bins % LANES
    shape = (rows + 2 * DEPTH, LANES)
    row = row_index(shape)
    here = jnp.where(row >= rows + DEPTH, row - rows - 2 * DEPTH, row) + lax.axis_index("lat") * rows
    total = rows * lax.axis_size("lat")
    latitude = (-60.0 + 120.0 * (here.astype(jnp.float32) + 0.5) / total) * (math.pi / 180.0)
    over = 1.0 / jnp.cos(latitude)
    count = speed_ref.shape[0]
    for tile in range(tiles):
        which = angle_ref[2:3, lanes_of(tile)]
        speed = jnp.zeros((1, LANES), jnp.float32)
        for k in range(count):
            speed = jnp.where(which == float(k), speed_ref[k], speed)
        x = (angle_ref[0:1, lanes_of(tile)] * speed) * over
        y = angle_ref[1:2, lanes_of(tile)] * speed
        go_x[:, lanes_of(tile)] = x
        go_y[:, lanes_of(tile)] = jnp.broadcast_to(y, (8, LANES))
        stay[:, lanes_of(tile)] = 1.0 - x - y
    body = bins - used
    wide[:, :body] = jnp.concatenate(
        [coupling_ref[:, :body], jnp.zeros((padded - bins, body), jnp.bfloat16)], axis=0
    )
    tail = jnp.concatenate([coupling_ref[:, body:], jnp.ones((bins, padded - bins), jnp.bfloat16)], axis=1)
    wide[:, body:] = jnp.concatenate([tail, jnp.zeros((padded - bins, LANES), jnp.bfloat16)], axis=0)


def load_kernel(bins, spectrum, sea_ref, ice_ref, wind_ref, edge_a, edge_b, inner, seas, gains, pack_a, pack_b):
    columns, rows = sea_ref.shape
    tiles = lane_tiles(bins)
    used = bins % LANES
    sea, gain = masks_kernel_part(sea_ref, ice_ref, wind_ref)
    for c in range(columns):
        s = jnp.broadcast_to(sea[:, c : c + 1], (rows, LANES))
        seas[c, :rows] = time_step * s
        gains[c, :rows] = s * jnp.broadcast_to(gain[:, c : c + 1], (rows, LANES))
    lane = lane_index((rows, LANES))

    def put(target, c):
        s = seas[c, :rows] != 0.0
        for tile in range(tiles):
            value = read_tile(spectrum, (c,), bins, tile)
            keep = s
            if tile == tiles - 1:
                keep = s & (lane < used)
            target[:rows, lanes_of(tile)] = jnp.where(keep, value, 0.0)

    for c in range(1, columns - 1):
        put(inner.at[c - 1], c)
    for second, target, pack in ((False, edge_a, pack_a), (True, edge_b, pack_b)):

        def side(west, target=target, pack=pack):
            put(target, 0 if west else columns - 1)
            pack_half([target[:rows, lanes_of(t)] for t in range(tiles)], west, bins, rows, False, pack)

        on_each_side(second, side)


def halo_rows(bins, from_a, from_b, slot, seas, gains, column):
    tiles = lane_tiles(bins)
    rows = seas.shape[1] - 2 * DEPTH
    used = bins % LANES
    shape = (8, LANES)
    top = row_index(shape) < DEPTH
    a_south = south_flag(False)
    values = []
    for tile in range(tiles):
        here = []
        for ref, pairs, index in (from_a, from_b):
            if tile < tiles - 1:
                here.append(ref[index * (tiles - 1) + tile])
            else:
                here.append(turn(ref[pairs * (tiles - 1)], -index * (LANES // pairs)))
        low, high = jnp.where(a_south, here[0], here[1]), jnp.where(a_south, here[1], here[0])
        if slot:
            low, high = pltpu.roll(low, DEPTH, 0), pltpu.roll(high, DEPTH, 0)
        values.append(jnp.where(top, high, low))
    last = values[-1]
    s = jnp.broadcast_to(last[:, used : used + 1], shape)
    g = jnp.broadcast_to(last[:, used + 1 : used + 2], shape)
    seas[column, rows:] = time_step * s
    gains[column, rows:] = s * g
    values[-1] = jnp.where(lane_index(shape) < used, last, 0.0)
    return values


def join_edges_kernel(
    bins, halo_a, halo_b, edge_a_in, edge_b_in, seas_in, gains_in, pack_a_in, pack_b_in,
    edge_a, edge_b, seas, gains, pack_a, pack_b,
):
    columns = seas.shape[0]
    rows = seas.shape[1] - 2 * DEPTH
    count = columns // 2
    values = [
        halo_rows(bins, (halo_a, count, 0), (halo_b, 1, 0), slot, seas, gains, c)
        for slot, c in enumerate((0, columns - 1))
    ]
    for second, target, before, pack in ((False, edge_a, pack_a_in, pack_a), (True, edge_b, pack_b_in, pack_b)):

        def side(west, target=target, before=before, pack=pack):
            mine = values[0 if west else 1]
            for tile, value in enumerate(mine):
                target[rows:, lanes_of(tile)] = value
            pack_corner(half_parts(mine, west, bins), before, west, bins, rows, pack)

        on_each_side(second, side)


def join_inner_kernel(bins, halo_a, halo_b, inner_in, seas_in, gains_in, inner, seas, gains):
    columns = seas.shape[0]
    rows = seas.shape[1] - 2 * DEPTH
    count = columns // 2
    for index in range(1, count):
        for slot in range(2):
            c = 2 * index - 1 + slot
            values = halo_rows(bins, (halo_a, count, index), (halo_b, count - 1, index - 1), slot, seas, gains, c)
            for tile, value in enumerate(values):
                inner[c - 1, rows:, lanes_of(tile)] = value


def ordered_edge_kernel(bins, second, after, *refs):
    edge_kernel(bins, second, *refs)


def edge_kernel(
    bins, second, halo, edge, inner, seas, gains, stay, go_x, go_y, wide, out, pack, adv_ref
):
    rows = edge.shape[0] - 2 * DEPTH
    halo_next = pack.shape[0] == pack_count(rows, True)

    def side(west):
        fresh = edge_step(bins, west, halo, edge, inner, seas, gains, stay, go_x, go_y, wide, adv_ref, False)
        for t, value in enumerate(fresh):
            out[:, lanes_of(t)] = value
        pack_half(fresh, west, bins, rows, halo_next, pack)

    on_each_side(second, side)


def ordered_late_kernel(bins, second, after, *refs):
    late_edge_kernel(bins, second, *refs)


def late_edge_kernel(bins, second, halo, edge, inner, seas, gains, stay, go_x, go_y, wide, out, adv_ref):
    def side(west):
        fresh = edge_step(bins, west, halo, edge, inner, seas, gains, stay, go_x, go_y, wide, adv_ref, True)
        for t, value in enumerate(fresh):
            write_tile(out, (), bins, t, value)

    on_each_side(second, side)


def last_edge_kernel(
    bins, second, halo, edge, inner, seas, gains, stay, go_x, go_y, wide, done_inner, done_edge, out, adv_ref, column, sems
):
    columns = out.shape[0]
    mine = jnp.where(west_flag(second), 0, columns - 1)
    copies = [
        pltpu.make_async_copy(done_inner, out.at[pl.ds(1, columns - 2)], sems.at[0]),
        pltpu.make_async_copy(done_edge, out.at[columns - 1 - mine], sems.at[1]),
    ]
    for copy in copies:
        copy.start()
    late_edge_kernel(bins, second, halo, edge, inner, seas, gains, stay, go_x, go_y, wide, column, adv_ref)
    copies.append(pltpu.make_async_copy(column, out.at[mine], sems.at[2]))
    copies[2].start()
    for copy in copies:
        copy.wait()


def edge_step(bins, west, halo, edge, inner, seas, gains, stay, go_x, go_y, wide, adv_ref, last):
    tiles = lane_tiles(bins)
    columns = inner.shape[0] + 2
    rows = edge.shape[0] - 2 * DEPTH
    used = rows if last else edge.shape[0]
    near, mine = (0, 0) if west else (columns - 3, columns - 1)
    across = across_edge(halo, [inner[near, :, lanes_of(t)] for t in range(tiles)], west, bins, rows, not last)
    for t in range(tiles):
        here = lanes_of(t)
        adv = advect(edge[:, here], across[t], stay[:, here], go_x[:, here], go_y[0:1, here], bins, t)
        adv_ref[:used, here] = adv[:used]
    low = adv_ref[:used].astype(jnp.bfloat16)
    s, g = seas[mine, :used], gains[mine, :used]
    fresh = [None] * tiles
    keep = None
    for block in lane_blocks(tiles):
        product = jnp.dot(low, wide[:, block[0] * LANES : (block[-1] + 1) * LANES], preferred_element_type=jnp.float32)
        if keep is None:
            share = jnp.broadcast_to(product[:, -1:], (used, LANES)) * (dissipation / bins)
            keep = g - s * share
        for k, t in enumerate(block):
            fresh[t] = adv_ref[:used, lanes_of(t)] * keep + s * product[:, lanes_of(k)]
    return fresh


def lane_blocks(tiles):
    return [(t - 1, t) for t in range(tiles - 1, 0, -2)]


def inner_kernel(bins, edge_a, edge_b, inner, seas, gains, stay, go_x, go_y, wide, out, adv_ref, low_ref, keep_ref):
    tiles = lane_tiles(bins)
    count, tall = inner.shape[0], inner.shape[1]
    rows = adv_ref.shape[0] // count
    a_west = west_flag(False)
    parts = 2
    if count % parts:
        parts = 1
    for part in range(parts):
        group = range(part * count // parts, (part + 1) * count // parts)
        whole = slice(group[0] * rows, (group[-1] + 1) * rows)
        for t in range(tiles):
            here = lanes_of(t)
            found = kinds(bins, t, is_east(bins))
            for c in group:
                west = east = None
                if True in found:
                    west = inner[c - 1, :, here] if c else jnp.where(a_west, edge_a[:, here], edge_b[:, here])
                if False in found:
                    east = inner[c + 1, :, here] if c < count - 1 else jnp.where(a_west, edge_b[:, here], edge_a[:, here])
                if west is None:
                    across = east
                elif east is None:
                    across = west
                else:
                    across = jnp.where(eastward(bins, t, (tall, LANES)), west, east)
                adv = advect(inner[c, :, here], across, stay[:, here], go_x[:, here], go_y[0:1, here], bins, t)[:rows]
                adv_ref[c * rows : (c + 1) * rows, here] = adv
        low_ref[whole] = adv_ref[whole].astype(jnp.bfloat16)
        for block in lane_blocks(tiles):
            product = jnp.dot(
                low_ref[whole], wide[:, block[0] * LANES : (block[-1] + 1) * LANES], preferred_element_type=jnp.float32
            )
            for c in group:
                span = slice(c * rows, (c + 1) * rows)
                mine = slice((c - group[0]) * rows, (c - group[0] + 1) * rows)
                s = seas[c + 1, :rows]
                if block[-1] == tiles - 1:
                    share = jnp.broadcast_to(product[mine, -1:], (rows, LANES)) * (dissipation / bins)
                    keep_ref[span] = gains[c + 1, :rows] - s * share
                for k, t in enumerate(block):
                    value = adv_ref[span, lanes_of(t)] * keep_ref[span] + s * product[mine, lanes_of(k)]
                    if rows == tall:
                        out[c, :, lanes_of(t)] = value
                    else:
                        write_tile(out, (c,), bins, t, value)


def angle_table(bins, freqs):
    padded = lane_tiles(bins) * LANES
    table = np.zeros((8, padded), np.float32)
    theta = (np.arange(DIRS) + 0.5) * (2.0 * math.pi / DIRS)
    table[0, :bins] = np.repeat(0.225 * np.abs(np.cos(theta)), freqs)
    table[1, :bins] = np.repeat(0.45 * np.abs(np.sin(theta)), freqs)
    table[2, :] = -1.0
    table[2, :bins] = np.tile(np.arange(freqs), DIRS)
    return table


def steps(spectrum, sea_mask, ice_flags, wind_forcing, group_speed, coupling):
    columns, rows, bins = spectrum.shape
    tiles = lane_tiles(bins)
    padded = tiles * LANES
    tall = rows + 2 * DEPTH
    f32 = jnp.float32
    lon, lat = lax.axis_size("lon"), lax.axis_size("lat")
    lon_a, lon_b = swap_pairs(lon, 0, True), swap_pairs(lon, 1, True)
    lat_a, lat_b = swap_pairs(lat, 0, False), swap_pairs(lat, 1, False)
    vmem = pl.BlockSpec(memory_space=VMEM)
    smem = pl.BlockSpec(memory_space=SMEM)
    hbm = pl.BlockSpec(memory_space=pltpu.HBM)
    edge_shape = VMEM((tall, padded), f32)
    inner_shape = VMEM((columns - 2, tall, padded), f32)
    mask_shape = VMEM((columns, tall, LANES), f32)
    table_shape = VMEM((tall, padded), f32)

    def call(body, outs, ins, specs, scratch=(), aliases=None, flops=0, out_specs=None):
        return pl.pallas_call(
            body,
            out_shape=outs,
            in_specs=specs,
            out_specs=out_specs if out_specs is not None else jax.tree.map(lambda _: vmem, outs),
            scratch_shapes=list(scratch),
            input_output_aliases=aliases or {},
            cost_estimate=pl.CostEstimate(flops=flops, bytes_accessed=0, transcendentals=0),
            compiler_params=pltpu.CompilerParams(vmem_limit_bytes=24 * 1024 * 1024),
        )(*ins)

    pairs = columns // 2
    send_a, send_b, send_c = call(
        functools.partial(first_kernel, bins),
        tuple(VMEM((halo_tiles(n, tiles), 8, LANES), f32) for n in (pairs, 1, pairs - 1)),
        [pltpu.with_memory_space_constraint(x, pltpu.HBM) for x in (spectrum, sea_mask, ice_flags, wind_forcing)],
        [hbm] * 4,
        [VMEM((2, columns, 8, bins), f32), VMEM((columns, rows), sea_mask.dtype), VMEM((columns, rows), ice_flags.dtype),
         VMEM((columns, rows), f32), pltpu.SemaphoreType.DMA((5,))],
    )
    halo_a = lax.ppermute(send_a, "lat", lat_a)
    halo_b = lax.ppermute(send_b, "lat", lat_b)
    halo_c = lax.ppermute(send_c, "lat", lat_b)
    pack_shape = VMEM((pack_count(rows, True), 8, LANES), f32)
    edge_a, edge_b, inner, seas, gains, pack_a, pack_b = call(
        functools.partial(load_kernel, bins),
        (edge_shape, edge_shape, inner_shape, mask_shape, mask_shape, pack_shape, pack_shape),
        (spectrum, sea_mask, ice_flags, wind_forcing), [vmem] * 4, flops=1 << 24,
    )
    stay, go_x, go_y, wide = call(
        functools.partial(table_kernel, bins, rows),
        (table_shape, table_shape, VMEM((8, padded), f32), VMEM((padded, padded), jnp.bfloat16)),
        (group_speed, jnp.asarray(angle_table(bins, group_speed.shape[0])), coupling),
        [smem, vmem, vmem], flops=1 << 24,
    )
    edge_a, edge_b, seas, gains, pack_a, pack_b = call(
        functools.partial(join_edges_kernel, bins),
        (edge_shape, edge_shape, mask_shape, mask_shape, pack_shape, pack_shape),
        (halo_a, halo_b, edge_a, edge_b, seas, gains, pack_a, pack_b), [vmem] * 8,
        aliases={2: 0, 3: 1, 4: 2, 5: 3, 6: 4, 7: 5},
    )
    inner, seas, gains = call(
        functools.partial(join_inner_kernel, bins), (inner_shape, mask_shape, mask_shape),
        (halo_a, halo_c, inner, seas, gains), [vmem] * 5, aliases={2: 0, 3: 1, 4: 2},
    )
    tables = (seas, gains, stay, go_x, go_y, wide)
    for step in range(STEPS):
        last = step == STEPS - 1
        halo_b = lax.ppermute(pack_b, "lon", lon_b)
        halo_a = lax.ppermute(pack_a, "lon", lon_a)
        used = rows if last else tall
        new_inner = call(
            functools.partial(inner_kernel, bins), VMEM((columns - 2, rows, bins), f32) if last else inner_shape,
            (edge_a, edge_b, inner) + tables, [vmem] * 9,
            [VMEM(((columns - 2) * used, padded), f32), VMEM(((columns - 2) * used, padded), jnp.bfloat16),
             VMEM(((columns - 2) * used, LANES), f32)],
            flops=1 << 28,
        )
        if last:
            column = VMEM((rows, bins), f32)
            scratch = [VMEM((tall, padded), f32)]
            done_b = call(
                functools.partial(ordered_late_kernel, bins, True), column,
                (new_inner, halo_b, edge_b, inner) + tables, [vmem] * 10, scratch, flops=1 << 26,
            )
            return call(
                functools.partial(last_edge_kernel, bins, False), pltpu.HBM((columns, rows, bins), f32),
                (halo_a, edge_a, inner) + tables + (new_inner, done_b), [vmem] * 11,
                scratch + [column, pltpu.SemaphoreType.DMA((3,))], flops=1 << 26, out_specs=hbm,
            )
        fresh = []
        pack_next = VMEM((pack_count(rows, step < STEPS - 2), 8, LANES), f32)
        for second, halo, edge in ((False, halo_a, edge_a), (True, halo_b, edge_b)):
            ins = (new_inner, halo, edge, inner) + tables
            fresh.append(call(
                functools.partial(ordered_edge_kernel, bins, second), (edge_shape, pack_next),
                ins, [vmem] * len(ins), [VMEM((tall, padded), f32)], flops=1 << 26,
            ))
        inner = new_inner
        (edge_a, pack_a), (edge_b, pack_b) = fresh


def solution(mesh):
    placed = (P("lon", "lat", None), P("lon", "lat"), P("lon", "lat"), P("lon", "lat"), P(), P())
    return jax.shard_map(steps, mesh=mesh, in_specs=placed, out_specs=P("lon", "lat", None), check_vma=False)
```

```python
import functools
import math

import jax
import jax.numpy as jnp
import numpy as np
from jax import lax
from jax.experimental import pallas as pl
from jax.experimental.pallas import tpu as pltpu
from jax.sharding import PartitionSpec as P


DIRS = 36
STEPS = 4
LANES = 128
DEPTH = 4

time_step = 0.2
dissipation = 0.5

VMEM = pltpu.VMEM
SMEM = pltpu.SMEM


def swap_pairs(size, first, wrap):
    pairs = []
    for i in range(first, size, 2):
        j = i + 1
        if j >= size:
            if not wrap:
                continue
            j = j % size
        pairs += [(i, j), (j, i)]
    return pairs


def lane_tiles(bins):
    return pl.cdiv(bins, LANES)


def lanes_of(tile):
    return slice(tile * LANES, (tile + 1) * LANES)


def lane_index(shape):
    return lax.broadcasted_iota(jnp.int32, shape, 1)


def row_index(shape):
    return lax.broadcasted_iota(jnp.int32, shape, 0)


def eastward(bins, tile, shape):
    bin_here = lane_index(shape) + tile * LANES
    quarter = bins // 4
    return (bin_here < quarter) | (bin_here >= bins - quarter)


def northward(bins, tile, shape):
    return lane_index(shape) + tile * LANES < bins // 2


def kinds(bins, tile, test):
    low, high = tile * LANES, min((tile + 1) * LANES, bins)
    return {bool(test(b)) for b in range(low, high)}


def is_east(bins):
    return lambda b: b < bins // 4 or b >= bins - bins // 4


def is_north(bins):
    return lambda b: b < bins // 2


def upwind_lat(f, bins, tile):
    shape = f.shape
    rows = shape[0]
    found = kinds(bins, tile, is_north(bins))
    south = pltpu.roll(f, 1, 0) if True in found else None
    north = pltpu.roll(f, rows - 1, 0) if False in found else None
    if south is None:
        return north
    if north is None:
        return south
    return jnp.where(northward(bins, tile, shape), south, north)


def advect(f, across, stay, go_x, go_y, bins, tile):
    along = upwind_lat(f, bins, tile)
    return stay * f + go_x * across + go_y * along


def turn(value, shift):
    shift = shift % LANES
    return pltpu.roll(value, shift, 1) if shift else value


def pack_plan(bins, west):
    split = bins // 4 - LANES
    high = bins - bins // 4 - 3 * LANES
    width = 2 * split
    return split, high, width, LANES - width, (split if west else high)


def pack_count(rows, halo):
    blocks = rows // 8
    return 2 * blocks + blocks // 2 + 1 + (2 if halo else 0)


def half_parts(t, west, bins):
    split, high, _, _, _ = pack_plan(bins, west)
    lane = lane_index(t[0].shape)
    if west:
        return t[2], jnp.where(lane < high, t[3], t[1]), t[1]
    return t[0], t[4], jnp.where(lane < split, t[1], jnp.where(lane >= high, t[3], turn(t[5], split)))


def pack_half(tiles, west, bins, rows, halo, out):
    _, _, width, kept, start = pack_plan(bins, west)
    rest = width - kept
    blocks = rows // 8
    half = blocks // 2
    lane = lane_index((8, LANES))

    left = jnp.zeros((8, LANES), jnp.float32)
    held = {}
    for block in range(blocks + (1 if halo else 0)):
        full, other, part = half_parts([tile[8 * block : 8 * block + 8] for tile in tiles], west, bins)
        if block < blocks:
            out[block] = full
            out[blocks + block] = other
            if block < half:
                held[block] = turn(part, -start)
            else:
                k = block - half
                out[2 * blocks + k] = jnp.where(lane < width, held.pop(k), turn(part, width - start))
                low = rest * k
                left = jnp.where((lane >= low) & (lane < low + rest), turn(part, low - kept - start), left)
        else:
            left = jnp.where(lane >= half * rest, turn(part, half * rest - start), left)
            out[2 * blocks + half + 1] = full
            out[2 * blocks + half + 2] = other
    out[2 * blocks + half] = left


def pack_corner(parts, before, west, bins, rows, out):
    _, _, width, kept, start = pack_plan(bins, west)
    rest = width - kept
    half = rows // 16
    spot = 5 * half
    lane = lane_index((8, LANES))
    out[spot] = jnp.where(lane >= half * rest, turn(parts[2], half * rest - start), before[spot])
    out[spot + 1] = parts[0]
    out[spot + 2] = parts[1]


def across_edge(halo, inner, west, bins, rows, with_halo, corner=None):
    split, high, width, kept, start = pack_plan(bins, not west)
    rest = width - kept
    blocks = rows // 8
    half = blocks // 2
    lane = lane_index((8, LANES))
    left = halo[2 * blocks + half]
    found = [[] for _ in inner]
    for block in range(blocks + 1):
        near = [tile[8 * block : 8 * block + 8] for tile in inner]
        if block == blocks and not with_halo:
            new = near
        else:
            if block == blocks and corner is not None:
                full, other, part = corner[0], corner[1], corner[2]
            elif block == blocks:
                full, other = halo[2 * blocks + half + 1], halo[2 * blocks + half + 2]
                part = turn(left, start - half * rest)
            else:
                full, other = halo[block], halo[blocks + block]
                if block < half:
                    part = turn(halo[2 * blocks + block], start)
                else:
                    k = block - half
                    early = (lane >= high) | (lane < split) if west else lane < start + kept
                    part = jnp.where(early, turn(halo[2 * blocks + k], start - width), turn(left, start + kept - rest * k))
            if west:
                new = [
                    full, jnp.where(lane < split, part, near[1]), near[2],
                    jnp.where(lane >= high, part, near[3]), other, turn(part, -split),
                ]
            else:
                new = [
                    near[0], jnp.where(lane < split, near[1], jnp.where(lane < high, part, other)), full,
                    jnp.where(lane < high, other, near[3]), near[4], near[5],
                ]
        for k, value in enumerate(new):
            found[k].append(value)
    return [jnp.concatenate(values, axis=0) for values in found]


def on_each_side(second, body):
    west = west_flag(second)

    @pl.when(west)
    def _():
        body(True)

    @pl.when(jnp.logical_not(west))
    def _():
        body(False)


def west_flag(second):
    odd = lax.rem(lax.axis_index("lon"), 2)
    return (1 - odd if second else odd) == 1


def south_flag(second):
    odd = lax.rem(lax.axis_index("lat"), 2)
    return (1 - odd if second else odd) == 1


def read_tile(ref, where, bins, tile):
    low, high = tile * LANES, min((tile + 1) * LANES, bins)
    value = ref[where + (slice(None), slice(low, high))]
    if high - low == LANES:
        return value
    return jnp.concatenate([value, jnp.zeros((value.shape[0], LANES - (high - low)), value.dtype)], axis=1)


def write_tile(ref, where, bins, tile, value):
    rows, low, high = ref.shape[-2], tile * LANES, min((tile + 1) * LANES, bins)
    ref[where + (slice(None), slice(low, high))] = value[:rows, : high - low]


def masks_kernel_part(sea_ref, ice_ref, wind_ref):
    sea = sea_ref[...].astype(jnp.float32)
    gain = 1.0 + time_step * (wind_ref[...] * (1.0 - ice_ref[...].astype(jnp.float32)))
    _, rows = sea.shape
    sea = jnp.concatenate([sea, gain], axis=1)
    turned = jnp.transpose(sea)
    return turned[:rows], turned[rows:]


def first_kernel(bins, spectrum, sea_hbm, ice_hbm, wind_hbm, out_a, out_b, edge, sea_ref, ice_ref, wind_ref, sems):
    columns, rows = sea_ref.shape
    copies = []
    masks = [
        pltpu.make_async_copy(source, target, sems.at[2 + k])
        for k, (source, target) in enumerate(((sea_hbm, sea_ref), (ice_hbm, ice_ref), (wind_hbm, wind_ref)))
    ]
    for copy in masks:
        copy.start()
    for c in range(columns):
        for k, start in enumerate((0, rows - 8)):
            copy = pltpu.make_async_copy(spectrum.at[c, pl.ds(start, 8)], edge.at[k, c], sems.at[k])
            copy.start()
            copies.append(copy)
    for copy in masks:
        copy.wait()
    sea, gain = masks_kernel_part(sea_ref, ice_ref, wind_ref)
    shape = (8, LANES)
    lane = lane_index(shape)
    row = row_index(shape)
    used = bins % LANES
    for copy in copies:
        copy.wait()
    tiles = lane_tiles(bins)
    space = LANES // (columns // 2)
    for second, out in ((False, out_a), (True, out_b)):
        to_south = south_flag(second)
        ends = jnp.zeros(shape, jnp.float32)
        for pair in range(columns // 2):
            for tile in range(tiles):
                halves = []
                for c in (2 * pair, 2 * pair + 1):
                    low, high = read_tile(edge, (0, c), bins, tile), read_tile(edge, (1, c), bins, tile)
                    here = jnp.where(to_south, low, high)
                    s = jnp.where(to_south, sea[0:8, c : c + 1], sea[rows - 8 : rows, c : c + 1])
                    s = jnp.broadcast_to(s, shape)
                    value = here * s
                    if tile == tiles - 1:
                        g = jnp.where(to_south, gain[0:8, c : c + 1], gain[rows - 8 : rows, c : c + 1])
                        g = jnp.broadcast_to(g, shape)
                        value = jnp.where(lane < used, value, jnp.where(lane == used, s, g))
                    halves.append(value)
                first, other = halves
                keep = (row < DEPTH) == to_south
                value = jnp.where(keep, first, pltpu.roll(other, DEPTH, 0))
                if tile < tiles - 1:
                    out[pair * (tiles - 1) + tile] = value
                else:
                    here = (lane >= pair * space) & (lane < (pair + 1) * space)
                    ends = jnp.where(here, turn(value, pair * space), ends)
        out[columns // 2 * (tiles - 1)] = ends


def table_kernel(bins, rows, speed_ref, angle_ref, coupling_ref, stay, go_x, go_y, wide):
    tiles = lane_tiles(bins)
    padded = tiles * LANES
    used = bins % LANES
    shape = (rows + 2 * DEPTH, LANES)
    row = row_index(shape)
    here = jnp.where(row >= rows + DEPTH, row - rows - 2 * DEPTH, row) + lax.axis_index("lat") * rows
    total = rows * lax.axis_size("lat")
    latitude = (-60.0 + 120.0 * (here.astype(jnp.float32) + 0.5) / total) * (math.pi / 180.0)
    over = 1.0 / jnp.cos(latitude)
    count = speed_ref.shape[0]
    for tile in range(tiles):
        which = angle_ref[2:3, lanes_of(tile)]
        speed = jnp.zeros((1, LANES), jnp.float32)
        for k in range(count):
            speed = jnp.where(which == float(k), speed_ref[k], speed)
        x = (angle_ref[0:1, lanes_of(tile)] * speed) * over
        y = angle_ref[1:2, lanes_of(tile)] * speed
        go_x[:, lanes_of(tile)] = x
        go_y[:, lanes_of(tile)] = jnp.broadcast_to(y, (8, LANES))
        stay[:, lanes_of(tile)] = 1.0 - x - y
    body = bins - used
    wide[:, :body] = jnp.concatenate(
        [coupling_ref[:, :body], jnp.zeros((padded - bins, body), jnp.bfloat16)], axis=0
    )
    tail = jnp.concatenate([coupling_ref[:, body:], jnp.ones((bins, padded - bins), jnp.bfloat16)], axis=1)
    wide[:, body:] = jnp.concatenate([tail, jnp.zeros((padded - bins, LANES), jnp.bfloat16)], axis=0)


def load_kernel(bins, spectrum, sea_ref, ice_ref, wind_ref, edge_a, edge_b, inner, seas, gains, pack_a, pack_b):
    columns, rows = sea_ref.shape
    tiles = lane_tiles(bins)
    used = bins % LANES
    sea, gain = masks_kernel_part(sea_ref, ice_ref, wind_ref)
    for c in range(columns):
        s = jnp.broadcast_to(sea[:, c : c + 1], (rows, LANES))
        seas[c, :rows] = time_step * s
        gains[c, :rows] = s * jnp.broadcast_to(gain[:, c : c + 1], (rows, LANES))
    lane = lane_index((rows, LANES))

    def put(target, c):
        s = seas[c, :rows] != 0.0
        for tile in range(tiles):
            value = read_tile(spectrum, (c,), bins, tile)
            keep = s
            if tile == tiles - 1:
                keep = s & (lane < used)
            target[:rows, lanes_of(tile)] = jnp.where(keep, value, 0.0)

    for c in range(1, columns - 1):
        put(inner.at[c - 1], c)
    for second, target, pack in ((False, edge_a, pack_a), (True, edge_b, pack_b)):

        def side(west, target=target, pack=pack):
            put(target, 0 if west else columns - 1)
            pack_half([target[:rows, lanes_of(t)] for t in range(tiles)], west, bins, rows, False, pack)

        on_each_side(second, side)


def halo_rows(bins, from_a, from_b, slot, seas, gains, column):
    tiles = lane_tiles(bins)
    rows = seas.shape[1] - 2 * DEPTH
    used = bins % LANES
    shape = (8, LANES)
    top = row_index(shape) < DEPTH
    a_south = south_flag(False)
    values = []
    for tile in range(tiles):
        here = []
        for ref, pairs, index in (from_a, from_b):
            if tile < tiles - 1:
                here.append(ref[index * (tiles - 1) + tile])
            else:
                here.append(turn(ref[pairs * (tiles - 1)], -index * (LANES // pairs)))
        low, high = jnp.where(a_south, here[0], here[1]), jnp.where(a_south, here[1], here[0])
        if slot:
            low, high = pltpu.roll(low, DEPTH, 0), pltpu.roll(high, DEPTH, 0)
        values.append(jnp.where(top, high, low))
    last = values[-1]
    s = jnp.broadcast_to(last[:, used : used + 1], shape)
    g = jnp.broadcast_to(last[:, used + 1 : used + 2], shape)
    seas[column, rows:] = time_step * s
    gains[column, rows:] = s * g
    values[-1] = jnp.where(lane_index(shape) < used, last, 0.0)
    return values


def corner_kernel(bins, after, halo_a, halo_b, edge_in, seas_in, gains_in, edge, seas, gains, corner):
    columns = seas.shape[0]
    rows = seas.shape[1] - 2 * DEPTH

    def side(west):
        c = 0 if west else columns - 1
        at = (columns // 2, c // 2)
        mine = halo_rows(bins, (halo_a,) + at, (halo_b,) + at, c % 2, seas, gains, c)
        for tile, value in enumerate(mine):
            edge[rows:, lanes_of(tile)] = value
        for k, value in enumerate(half_parts(mine, west, bins)):
            corner[k] = value

    on_each_side(True, side)


def join_kernel(
    bins, halo_a, halo_b, edge_in, inner_in, seas_in, gains_in, pack_in, edge, inner, seas, gains, pack
):
    columns = seas.shape[0]
    rows = seas.shape[1] - 2 * DEPTH

    def column(c):
        at = (columns // 2, c // 2)
        return halo_rows(bins, (halo_a,) + at, (halo_b,) + at, c % 2, seas, gains, c)

    def side(west):
        mine = column(0 if west else columns - 1)
        for tile, value in enumerate(mine):
            edge[rows:, lanes_of(tile)] = value
        pack_corner(half_parts(mine, west, bins), pack_in, west, bins, rows, pack)

    on_each_side(False, side)
    for c in range(1, columns - 1):
        for tile, value in enumerate(column(c)):
            inner[c - 1, rows:, lanes_of(tile)] = value


def ordered_first_kernel(bins, second, after, corner, *refs):
    edge_kernel(bins, second, *refs, corner=corner)


def ordered_edge_kernel(bins, second, after, *refs):
    edge_kernel(bins, second, *refs)


def edge_kernel(
    bins, second, halo, edge, inner, seas, gains, stay, go_x, go_y, wide, out, pack, adv_ref, corner=None
):
    rows = edge.shape[0] - 2 * DEPTH
    halo_next = pack.shape[0] == pack_count(rows, True)

    def side(west):
        fresh = edge_step(bins, west, halo, edge, inner, seas, gains, stay, go_x, go_y, wide, adv_ref, False, corner)
        for t, value in enumerate(fresh):
            out[:, lanes_of(t)] = value
        pack_half(fresh, west, bins, rows, halo_next, pack)

    on_each_side(second, side)


def ordered_late_kernel(bins, second, after, *refs):
    late_edge_kernel(bins, second, *refs)


def late_edge_kernel(bins, second, halo, edge, inner, seas, gains, stay, go_x, go_y, wide, out, adv_ref):
    def side(west):
        fresh = edge_step(bins, west, halo, edge, inner, seas, gains, stay, go_x, go_y, wide, adv_ref, True)
        for t, value in enumerate(fresh):
            write_tile(out, (), bins, t, value)

    on_each_side(second, side)


def last_edge_kernel(
    bins, second, halo, edge, inner, seas, gains, stay, go_x, go_y, wide, done_inner, done_edge, out, adv_ref, column, sems
):
    columns = out.shape[0]
    mine = jnp.where(west_flag(second), 0, columns - 1)
    copies = [
        pltpu.make_async_copy(done_inner, out.at[pl.ds(1, columns - 2)], sems.at[0]),
        pltpu.make_async_copy(done_edge, out.at[columns - 1 - mine], sems.at[1]),
    ]
    for copy in copies:
        copy.start()
    late_edge_kernel(bins, second, halo, edge, inner, seas, gains, stay, go_x, go_y, wide, column, adv_ref)
    copies.append(pltpu.make_async_copy(column, out.at[mine], sems.at[2]))
    copies[2].start()
    for copy in copies:
        copy.wait()


def edge_step(bins, west, halo, edge, inner, seas, gains, stay, go_x, go_y, wide, adv_ref, last, corner=None):
    tiles = lane_tiles(bins)
    columns = inner.shape[0] + 2
    rows = edge.shape[0] - 2 * DEPTH
    used = rows if last else edge.shape[0]
    near, mine = (0, 0) if west else (columns - 3, columns - 1)
    across = across_edge(halo, [inner[near, :, lanes_of(t)] for t in range(tiles)], west, bins, rows, not last, corner)
    for t in range(tiles):
        here = lanes_of(t)
        adv = advect(edge[:, here], across[t], stay[:, here], go_x[:, here], go_y[0:1, here], bins, t)
        adv_ref[:used, here] = adv[:used]
    low = adv_ref[:used].astype(jnp.bfloat16)
    s, g = seas[mine, :used], gains[mine, :used]
    fresh = [None] * tiles
    keep = None
    for block in lane_blocks(tiles):
        product = jnp.dot(low, wide[:, block[0] * LANES : (block[-1] + 1) * LANES], preferred_element_type=jnp.float32)
        if keep is None:
            share = jnp.broadcast_to(product[:, -1:], (used, LANES)) * (dissipation / bins)
            keep = g - s * share
        for k, t in enumerate(block):
            fresh[t] = adv_ref[:used, lanes_of(t)] * keep + s * product[:, lanes_of(k)]
    return fresh


def lane_blocks(tiles):
    return [(t - 1, t) for t in range(tiles - 1, 0, -2)]


def inner_kernel(bins, edge_a, edge_b, inner, seas, gains, stay, go_x, go_y, wide, out, adv_ref, low_ref, keep_ref):
    tiles = lane_tiles(bins)
    count, tall = inner.shape[0], inner.shape[1]
    rows = adv_ref.shape[0] // count
    a_west = west_flag(False)
    parts = 2
    if count % parts:
        parts = 1
    for part in range(parts):
        group = range(part * count // parts, (part + 1) * count // parts)
        whole = slice(group[0] * rows, (group[-1] + 1) * rows)
        for t in range(tiles):
            here = lanes_of(t)
            found = kinds(bins, t, is_east(bins))
            for c in group:
                west = east = None
                if True in found:
                    west = inner[c - 1, :, here] if c else jnp.where(a_west, edge_a[:, here], edge_b[:, here])
                if False in found:
                    east = inner[c + 1, :, here] if c < count - 1 else jnp.where(a_west, edge_b[:, here], edge_a[:, here])
                if west is None:
                    across = east
                elif east is None:
                    across = west
                else:
                    across = jnp.where(eastward(bins, t, (tall, LANES)), west, east)
                adv = advect(inner[c, :, here], across, stay[:, here], go_x[:, here], go_y[0:1, here], bins, t)[:rows]
                adv_ref[c * rows : (c + 1) * rows, here] = adv
        low_ref[whole] = adv_ref[whole].astype(jnp.bfloat16)
        for block in lane_blocks(tiles):
            product = jnp.dot(
                low_ref[whole], wide[:, block[0] * LANES : (block[-1] + 1) * LANES], preferred_element_type=jnp.float32
            )
            for c in group:
                span = slice(c * rows, (c + 1) * rows)
                mine = slice((c - group[0]) * rows, (c - group[0] + 1) * rows)
                s = seas[c + 1, :rows]
                if block[-1] == tiles - 1:
                    share = jnp.broadcast_to(product[mine, -1:], (rows, LANES)) * (dissipation / bins)
                    keep_ref[span] = gains[c + 1, :rows] - s * share
                for k, t in enumerate(block):
                    value = adv_ref[span, lanes_of(t)] * keep_ref[span] + s * product[mine, lanes_of(k)]
                    if rows == tall:
                        out[c, :, lanes_of(t)] = value
                    else:
                        write_tile(out, (c,), bins, t, value)


def angle_table(bins, freqs):
    padded = lane_tiles(bins) * LANES
    table = np.zeros((8, padded), np.float32)
    theta = (np.arange(DIRS) + 0.5) * (2.0 * math.pi / DIRS)
    table[0, :bins] = np.repeat(0.225 * np.abs(np.cos(theta)), freqs)
    table[1, :bins] = np.repeat(0.45 * np.abs(np.sin(theta)), freqs)
    table[2, :] = -1.0
    table[2, :bins] = np.tile(np.arange(freqs), DIRS)
    return table


def steps(spectrum, sea_mask, ice_flags, wind_forcing, group_speed, coupling):
    columns, rows, bins = spectrum.shape
    tiles = lane_tiles(bins)
    padded = tiles * LANES
    tall = rows + 2 * DEPTH
    f32 = jnp.float32
    lon, lat = lax.axis_size("lon"), lax.axis_size("lat")
    lon_a, lon_b = swap_pairs(lon, 0, True), swap_pairs(lon, 1, True)
    lat_a, lat_b = swap_pairs(lat, 0, False), swap_pairs(lat, 1, False)
    vmem = pl.BlockSpec(memory_space=VMEM)
    smem = pl.BlockSpec(memory_space=SMEM)
    hbm = pl.BlockSpec(memory_space=pltpu.HBM)
    edge_shape = VMEM((tall, padded), f32)
    inner_shape = VMEM((columns - 2, tall, padded), f32)
    mask_shape = VMEM((columns, tall, LANES), f32)
    table_shape = VMEM((tall, padded), f32)

    def call(body, outs, ins, specs, scratch=(), aliases=None, flops=0, out_specs=None):
        return pl.pallas_call(
            body,
            out_shape=outs,
            in_specs=specs,
            out_specs=out_specs if out_specs is not None else jax.tree.map(lambda _: vmem, outs),
            scratch_shapes=list(scratch),
            input_output_aliases=aliases or {},
            cost_estimate=pl.CostEstimate(flops=flops, bytes_accessed=0, transcendentals=0),
            compiler_params=pltpu.CompilerParams(vmem_limit_bytes=24 * 1024 * 1024),
        )(*ins)

    send_a, send_b = call(
        functools.partial(first_kernel, bins),
        (VMEM((columns // 2 * (tiles - 1) + 1, 8, LANES), f32),) * 2,
        [pltpu.with_memory_space_constraint(x, pltpu.HBM) for x in (spectrum, sea_mask, ice_flags, wind_forcing)],
        [hbm] * 4,
        [VMEM((2, columns, 8, bins), f32), VMEM((columns, rows), sea_mask.dtype), VMEM((columns, rows), ice_flags.dtype),
         VMEM((columns, rows), f32), pltpu.SemaphoreType.DMA((5,))],
    )
    halo_b = lax.ppermute(send_b, "lat", lat_b)
    halo_a = lax.ppermute(send_a, "lat", lat_a)
    pack_own = VMEM((pack_count(rows, False), 8, LANES), f32)
    pack_shape = VMEM((pack_count(rows, True), 8, LANES), f32)
    corner_shape = VMEM((3, 8, LANES), f32)
    edge_a, edge_b, inner, seas, gains, pack_a, pack_b = call(
        functools.partial(load_kernel, bins),
        (edge_shape, edge_shape, inner_shape, mask_shape, mask_shape, pack_shape, pack_own),
        (spectrum, sea_mask, ice_flags, wind_forcing), [vmem] * 4, flops=1 << 24,
    )
    stay, go_x, go_y, wide = call(
        functools.partial(table_kernel, bins, rows),
        (table_shape, table_shape, VMEM((8, padded), f32), VMEM((padded, padded), jnp.bfloat16)),
        (group_speed, jnp.asarray(angle_table(bins, group_speed.shape[0])), coupling),
        [smem, vmem, vmem], flops=1 << 24,
    )
    edge_b, seas, gains, corner_b = call(
        functools.partial(corner_kernel, bins), (edge_shape, mask_shape, mask_shape, corner_shape),
        (go_y, halo_a, halo_b, edge_b, seas, gains), [vmem] * 6, aliases={3: 0, 4: 1, 5: 2},
    )
    edge_a, inner, seas, gains, pack_a = call(
        functools.partial(join_kernel, bins), (edge_shape, inner_shape, mask_shape, mask_shape, pack_shape),
        (halo_a, halo_b, edge_a, inner, seas, gains, pack_a), [vmem] * 7,
        aliases={2: 0, 3: 1, 4: 2, 5: 3, 6: 4},
    )
    tables = (seas, gains, stay, go_x, go_y, wide)
    for step in range(STEPS):
        last = step == STEPS - 1
        halo_b = lax.ppermute(pack_b, "lon", lon_b)
        halo_a = lax.ppermute(pack_a, "lon", lon_a)
        if step == 0:
            corner = lax.ppermute(corner_b, "lon", lon_b)
        used = rows if last else tall
        new_inner = call(
            functools.partial(inner_kernel, bins), VMEM((columns - 2, rows, bins), f32) if last else inner_shape,
            (edge_a, edge_b, inner) + tables, [vmem] * 9,
            [VMEM(((columns - 2) * used, padded), f32), VMEM(((columns - 2) * used, padded), jnp.bfloat16),
             VMEM(((columns - 2) * used, LANES), f32)],
            flops=1 << 28,
        )
        if last:
            column = VMEM((rows, bins), f32)
            scratch = [VMEM((tall, padded), f32)]
            done_b = call(
                functools.partial(ordered_late_kernel, bins, True), column,
                (new_inner, halo_b, edge_b, inner) + tables, [vmem] * 10, scratch, flops=1 << 26,
            )
            return call(
                functools.partial(last_edge_kernel, bins, False), pltpu.HBM((columns, rows, bins), f32),
                (halo_a, edge_a, inner) + tables + (new_inner, done_b), [vmem] * 11,
                scratch + [column, pltpu.SemaphoreType.DMA((3,))], flops=1 << 26, out_specs=hbm,
            )
        fresh = []
        pack_next = VMEM((pack_count(rows, step < STEPS - 2), 8, LANES), f32)
        for second, halo, edge in ((False, halo_a, edge_a), (True, halo_b, edge_b)):
            body, ins = edge_kernel, (halo, edge, inner) + tables
            if step > 0:
                body, ins = ordered_edge_kernel, (new_inner,) + ins
            elif second:
                body, ins = ordered_first_kernel, (new_inner, corner) + ins
            fresh.append(call(
                functools.partial(body, bins, second), (edge_shape, pack_next),
                ins, [vmem] * len(ins), [VMEM((tall, padded), f32)], flops=1 << 26,
            ))
        inner = new_inner
        (edge_a, pack_a), (edge_b, pack_b) = fresh


def solution(mesh):
    placed = (P("lon", "lat", None), P("lon", "lat"), P("lon", "lat"), P("lon", "lat"), P(), P())
    return jax.shard_map(steps, mesh=mesh, in_specs=placed, out_specs=P("lon", "lat", None), check_vma=False)
```

```python
import functools
import math

import jax
import jax.numpy as jnp
import numpy as np
from jax import lax
from jax.experimental import pallas as pl
from jax.experimental.pallas import tpu as pltpu
from jax.sharding import PartitionSpec as P


DIRS = 36
STEPS = 4
LANES = 128
DEPTH = 4

time_step = 0.2
dissipation = 0.5

VMEM = pltpu.VMEM
SMEM = pltpu.SMEM


def swap_pairs(size, first, wrap):
    pairs = []
    for i in range(first, size, 2):
        j = i + 1
        if j >= size:
            if not wrap:
                continue
            j = j % size
        pairs += [(i, j), (j, i)]
    return pairs


def lane_tiles(bins):
    return pl.cdiv(bins, LANES)


def lanes_of(tile):
    return slice(tile * LANES, (tile + 1) * LANES)


def lane_index(shape):
    return lax.broadcasted_iota(jnp.int32, shape, 1)


def row_index(shape):
    return lax.broadcasted_iota(jnp.int32, shape, 0)


def eastward(bins, tile, shape):
    bin_here = lane_index(shape) + tile * LANES
    quarter = bins // 4
    return (bin_here < quarter) | (bin_here >= bins - quarter)


def northward(bins, tile, shape):
    return lane_index(shape) + tile * LANES < bins // 2


def kinds(bins, tile, test):
    low, high = tile * LANES, min((tile + 1) * LANES, bins)
    return {bool(test(b)) for b in range(low, high)}


def is_east(bins):
    return lambda b: b < bins // 4 or b >= bins - bins // 4


def is_north(bins):
    return lambda b: b < bins // 2


def upwind_lat(f, bins, tile):
    shape = f.shape
    rows = shape[0]
    found = kinds(bins, tile, is_north(bins))
    south = pltpu.roll(f, 1, 0) if True in found else None
    north = pltpu.roll(f, rows - 1, 0) if False in found else None
    if south is None:
        return north
    if north is None:
        return south
    return jnp.where(northward(bins, tile, shape), south, north)


def advect(f, across, stay, go_x, go_y, bins, tile):
    along = upwind_lat(f, bins, tile)
    return stay * f + go_x * across + go_y * along


def turn(value, shift):
    shift = shift % LANES
    return pltpu.roll(value, shift, 1) if shift else value


def pack_plan(bins, west):
    split = bins // 4 - LANES
    high = bins - bins // 4 - 3 * LANES
    width = 2 * split
    return split, high, width, LANES - width, (split if west else high)


def pack_count(rows, halo):
    blocks = rows // 8
    return 2 * blocks + blocks // 2 + 1 + (2 if halo else 0)


def half_parts(t, west, bins):
    split, high, _, _, _ = pack_plan(bins, west)
    lane = lane_index(t[0].shape)
    if west:
        return t[2], jnp.where(lane < high, t[3], t[1]), t[1]
    return t[0], t[4], jnp.where(lane < split, t[1], jnp.where(lane >= high, t[3], turn(t[5], split)))


def pack_half(tiles, west, bins, rows, halo, out):
    _, _, width, kept, start = pack_plan(bins, west)
    rest = width - kept
    blocks = rows // 8
    half = blocks // 2
    lane = lane_index((8, LANES))

    left = jnp.zeros((8, LANES), jnp.float32)
    held = {}
    for block in range(blocks + (1 if halo else 0)):
        full, other, part = half_parts([tile[8 * block : 8 * block + 8] for tile in tiles], west, bins)
        if block < blocks:
            out[block] = full
            out[blocks + block] = other
            if block < half:
                held[block] = turn(part, -start)
            else:
                k = block - half
                out[2 * blocks + k] = jnp.where(lane < width, held.pop(k), turn(part, width - start))
                low = rest * k
                left = jnp.where((lane >= low) & (lane < low + rest), turn(part, low - kept - start), left)
        else:
            left = jnp.where(lane >= half * rest, turn(part, half * rest - start), left)
            row = row_index((8, LANES))
            near = (row < 2) | (row >= 6)
            out[2 * blocks + half + 1] = jnp.where(near, full, pltpu.roll(other, 4, 0))
    out[2 * blocks + half] = left


def pack_corner(parts, before, west, bins, rows, out):
    _, _, width, kept, start = pack_plan(bins, west)
    rest = width - kept
    half = rows // 16
    spot = 5 * half
    lane = lane_index((8, LANES))
    out[spot] = jnp.where(lane >= half * rest, turn(parts[2], half * rest - start), before[spot])
    out[spot + 1] = parts[0]
    out[spot + 2] = parts[1]


def across_edge(halo, inner, west, bins, rows, with_halo, corner=None):
    split, high, width, kept, start = pack_plan(bins, not west)
    rest = width - kept
    blocks = rows // 8
    half = blocks // 2
    lane = lane_index((8, LANES))
    left = halo[2 * blocks + half]
    found = [[] for _ in inner]
    for block in range(blocks + 1):
        near = [tile[8 * block : 8 * block + 8] for tile in inner]
        if block == blocks and not with_halo:
            new = near
        else:
            if block == blocks and corner is not None:
                full, other, part = corner[0], corner[1], corner[2]
            elif block == blocks:
                full = halo[2 * blocks + half + 1]
                if halo.shape[0] > 2 * blocks + half + 2:
                    other = halo[2 * blocks + half + 2]
                else:
                    other = pltpu.roll(full, 4, 0)
                part = turn(left, start - half * rest)
            else:
                full, other = halo[block], halo[blocks + block]
                if block < half:
                    part = turn(halo[2 * blocks + block], start)
                else:
                    k = block - half
                    early = (lane >= high) | (lane < split) if west else lane < start + kept
                    part = jnp.where(early, turn(halo[2 * blocks + k], start - width), turn(left, start + kept - rest * k))
            if west:
                new = [
                    full, jnp.where(lane < split, part, near[1]), near[2],
                    jnp.where(lane >= high, part, near[3]), other, turn(part, -split),
                ]
            else:
                new = [
                    near[0], jnp.where(lane < split, near[1], jnp.where(lane < high, part, other)), full,
                    jnp.where(lane < high, other, near[3]), near[4], near[5],
                ]
        for k, value in enumerate(new):
            found[k].append(value)
    return [jnp.concatenate(values, axis=0) for values in found]


def on_each_side(second, body):
    west = west_flag(second)

    @pl.when(west)
    def _():
        body(True)

    @pl.when(jnp.logical_not(west))
    def _():
        body(False)


def west_flag(second):
    odd = lax.rem(lax.axis_index("lon"), 2)
    return (1 - odd if second else odd) == 1


def south_flag(second):
    odd = lax.rem(lax.axis_index("lat"), 2)
    return (1 - odd if second else odd) == 1


def read_tile(ref, where, bins, tile):
    low, high = tile * LANES, min((tile + 1) * LANES, bins)
    value = ref[where + (slice(None), slice(low, high))]
    if high - low == LANES:
        return value
    return jnp.concatenate([value, jnp.zeros((value.shape[0], LANES - (high - low)), value.dtype)], axis=1)


def write_tile(ref, where, bins, tile, value):
    rows, low, high = ref.shape[-2], tile * LANES, min((tile + 1) * LANES, bins)
    ref[where + (slice(None), slice(low, high))] = value[:rows, : high - low]


def masks_kernel_part(sea_ref, ice_ref, wind_ref):
    sea = sea_ref[...].astype(jnp.float32)
    gain = 1.0 + time_step * (wind_ref[...] * (1.0 - ice_ref[...].astype(jnp.float32)))
    _, rows = sea.shape
    sea = jnp.concatenate([sea, gain], axis=1)
    turned = jnp.transpose(sea)
    return turned[:rows], turned[rows:]


def first_kernel(bins, spectrum, sea_hbm, ice_hbm, wind_hbm, out_a, out_b, edge, sea_ref, ice_ref, wind_ref, sems):
    columns, rows = sea_ref.shape
    copies = []
    masks = [
        pltpu.make_async_copy(source, target, sems.at[2 + k])
        for k, (source, target) in enumerate(((sea_hbm, sea_ref), (ice_hbm, ice_ref), (wind_hbm, wind_ref)))
    ]
    for copy in masks:
        copy.start()
    for c in range(columns):
        for k, start in enumerate((0, rows - 8)):
            copy = pltpu.make_async_copy(spectrum.at[c, pl.ds(start, 8)], edge.at[k, c], sems.at[k])
            copy.start()
            copies.append(copy)
    for copy in masks:
        copy.wait()
    sea, gain = masks_kernel_part(sea_ref, ice_ref, wind_ref)
    shape = (8, LANES)
    lane = lane_index(shape)
    row = row_index(shape)
    used = bins % LANES
    for copy in copies:
        copy.wait()
    tiles = lane_tiles(bins)
    space = LANES // (columns // 2)
    for second, out in ((False, out_a), (True, out_b)):
        to_south = south_flag(second)
        ends = jnp.zeros(shape, jnp.float32)
        for pair in range(columns // 2):
            for tile in range(tiles):
                halves = []
                for c in (2 * pair, 2 * pair + 1):
                    low, high = read_tile(edge, (0, c), bins, tile), read_tile(edge, (1, c), bins, tile)
                    here = jnp.where(to_south, low, high)
                    s = jnp.where(to_south, sea[0:8, c : c + 1], sea[rows - 8 : rows, c : c + 1])
                    s = jnp.broadcast_to(s, shape)
                    value = here * s
                    if tile == tiles - 1:
                        g = jnp.where(to_south, gain[0:8, c : c + 1], gain[rows - 8 : rows, c : c + 1])
                        g = jnp.broadcast_to(g, shape)
                        value = jnp.where(lane < used, value, jnp.where(lane == used, s, g))
                    halves.append(value)
                first, other = halves
                keep = (row < DEPTH) == to_south
                value = jnp.where(keep, first, pltpu.roll(other, DEPTH, 0))
                if tile < tiles - 1:
                    out[pair * (tiles - 1) + tile] = value
                else:
                    here = (lane >= pair * space) & (lane < (pair + 1) * space)
                    ends = jnp.where(here, turn(value, pair * space), ends)
        out[columns // 2 * (tiles - 1)] = ends


def table_kernel(bins, rows, speed_ref, angle_ref, coupling_ref, stay, go_x, go_y, wide):
    tiles = lane_tiles(bins)
    padded = tiles * LANES
    used = bins % LANES
    shape = (rows + 2 * DEPTH, LANES)
    row = row_index(shape)
    here = jnp.where(row >= rows + DEPTH, row - rows - 2 * DEPTH, row) + lax.axis_index("lat") * rows
    total = rows * lax.axis_size("lat")
    latitude = (-60.0 + 120.0 * (here.astype(jnp.float32) + 0.5) / total) * (math.pi / 180.0)
    over = 1.0 / jnp.cos(latitude)
    count = speed_ref.shape[0]
    for tile in range(tiles):
        which = angle_ref[2:3, lanes_of(tile)]
        speed = jnp.zeros((1, LANES), jnp.float32)
        for k in range(count):
            speed = jnp.where(which == float(k), speed_ref[k], speed)
        x = (angle_ref[0:1, lanes_of(tile)] * speed) * over
        y = angle_ref[1:2, lanes_of(tile)] * speed
        go_x[:, lanes_of(tile)] = x
        go_y[:, lanes_of(tile)] = jnp.broadcast_to(y, (8, LANES))
        stay[:, lanes_of(tile)] = 1.0 - x - y
    body = bins - used
    wide[:, :body] = jnp.concatenate(
        [coupling_ref[:, :body], jnp.zeros((padded - bins, body), jnp.bfloat16)], axis=0
    )
    tail = jnp.concatenate([coupling_ref[:, body:], jnp.ones((bins, padded - bins), jnp.bfloat16)], axis=1)
    wide[:, body:] = jnp.concatenate([tail, jnp.zeros((padded - bins, LANES), jnp.bfloat16)], axis=0)


def load_kernel(bins, spectrum, sea_ref, ice_ref, wind_ref, edge_a, edge_b, inner, seas, gains, pack_a, pack_b):
    columns, rows = sea_ref.shape
    tiles = lane_tiles(bins)
    used = bins % LANES
    sea, gain = masks_kernel_part(sea_ref, ice_ref, wind_ref)
    for c in range(columns):
        s = jnp.broadcast_to(sea[:, c : c + 1], (rows, LANES))
        seas[c, :rows] = time_step * s
        gains[c, :rows] = s * jnp.broadcast_to(gain[:, c : c + 1], (rows, LANES))
    lane = lane_index((rows, LANES))

    def put(target, c):
        s = seas[c, :rows] != 0.0
        for tile in range(tiles):
            value = read_tile(spectrum, (c,), bins, tile)
            keep = s
            if tile == tiles - 1:
                keep = s & (lane < used)
            target[:rows, lanes_of(tile)] = jnp.where(keep, value, 0.0)

    for c in range(1, columns - 1):
        put(inner.at[c - 1], c)
    for second, target, pack in ((False, edge_a, pack_a), (True, edge_b, pack_b)):

        def side(west, target=target, pack=pack):
            put(target, 0 if west else columns - 1)
            pack_half([target[:rows, lanes_of(t)] for t in range(tiles)], west, bins, rows, False, pack)

        on_each_side(second, side)


def halo_rows(bins, from_a, from_b, slot, seas, gains, column):
    tiles = lane_tiles(bins)
    rows = seas.shape[1] - 2 * DEPTH
    used = bins % LANES
    shape = (8, LANES)
    top = row_index(shape) < DEPTH
    a_south = south_flag(False)
    values = []
    for tile in range(tiles):
        here = []
        for ref, pairs, index in (from_a, from_b):
            if tile < tiles - 1:
                here.append(ref[index * (tiles - 1) + tile])
            else:
                here.append(turn(ref[pairs * (tiles - 1)], -index * (LANES // pairs)))
        low, high = jnp.where(a_south, here[0], here[1]), jnp.where(a_south, here[1], here[0])
        if slot:
            low, high = pltpu.roll(low, DEPTH, 0), pltpu.roll(high, DEPTH, 0)
        values.append(jnp.where(top, high, low))
    last = values[-1]
    s = jnp.broadcast_to(last[:, used : used + 1], shape)
    g = jnp.broadcast_to(last[:, used + 1 : used + 2], shape)
    seas[column, rows:] = time_step * s
    gains[column, rows:] = s * g
    values[-1] = jnp.where(lane_index(shape) < used, last, 0.0)
    return values


def corner_kernel(bins, after, halo_a, halo_b, edge_in, seas_in, gains_in, edge, seas, gains, corner):
    columns = seas.shape[0]
    rows = seas.shape[1] - 2 * DEPTH

    def side(west):
        c = 0 if west else columns - 1
        at = (columns // 2, c // 2)
        mine = halo_rows(bins, (halo_a,) + at, (halo_b,) + at, c % 2, seas, gains, c)
        for tile, value in enumerate(mine):
            edge[rows:, lanes_of(tile)] = value
        for k, value in enumerate(half_parts(mine, west, bins)):
            corner[k] = value

    on_each_side(True, side)


def join_kernel(
    bins, halo_a, halo_b, edge_in, inner_in, seas_in, gains_in, pack_in, edge, inner, seas, gains, pack
):
    columns = seas.shape[0]
    rows = seas.shape[1] - 2 * DEPTH

    def column(c):
        at = (columns // 2, c // 2)
        return halo_rows(bins, (halo_a,) + at, (halo_b,) + at, c % 2, seas, gains, c)

    def side(west):
        mine = column(0 if west else columns - 1)
        for tile, value in enumerate(mine):
            edge[rows:, lanes_of(tile)] = value
        pack_corner(half_parts(mine, west, bins), pack_in, west, bins, rows, pack)

    on_each_side(False, side)
    for c in range(1, columns - 1):
        for tile, value in enumerate(column(c)):
            inner[c - 1, rows:, lanes_of(tile)] = value


def ordered_first_kernel(bins, second, after, corner, *refs):
    edge_kernel(bins, second, *refs, corner=corner)


def ordered_edge_kernel(bins, second, after, *refs):
    edge_kernel(bins, second, *refs)


def edge_kernel(
    bins, second, halo, edge, inner, seas, gains, stay, go_x, go_y, wide, out, pack, adv_ref, corner=None
):
    rows = edge.shape[0] - 2 * DEPTH
    halo_next = pack.shape[0] > pack_count(rows, False)

    def side(west):
        fresh = edge_step(bins, west, halo, edge, inner, seas, gains, stay, go_x, go_y, wide, adv_ref, False, corner)
        for t, value in enumerate(fresh):
            out[:, lanes_of(t)] = value
        pack_half(fresh, west, bins, rows, halo_next, pack)

    on_each_side(second, side)


def ordered_late_kernel(bins, second, after, *refs):
    late_edge_kernel(bins, second, *refs)


def late_edge_kernel(bins, second, halo, edge, inner, seas, gains, stay, go_x, go_y, wide, out, adv_ref):
    def side(west):
        fresh = edge_step(bins, west, halo, edge, inner, seas, gains, stay, go_x, go_y, wide, adv_ref, True)
        for t, value in enumerate(fresh):
            write_tile(out, (), bins, t, value)

    on_each_side(second, side)


def last_edge_kernel(
    bins, second, halo, edge, inner, seas, gains, stay, go_x, go_y, wide, done_inner, done_edge, out, adv_ref, column, sems
):
    columns = out.shape[0]
    mine = jnp.where(west_flag(second), 0, columns - 1)
    copies = [
        pltpu.make_async_copy(done_inner, out.at[pl.ds(1, columns - 2)], sems.at[0]),
        pltpu.make_async_copy(done_edge, out.at[columns - 1 - mine], sems.at[1]),
    ]
    for copy in copies:
        copy.start()
    late_edge_kernel(bins, second, halo, edge, inner, seas, gains, stay, go_x, go_y, wide, column, adv_ref)
    copies.append(pltpu.make_async_copy(column, out.at[mine], sems.at[2]))
    copies[2].start()
    for copy in copies:
        copy.wait()


def edge_step(bins, west, halo, edge, inner, seas, gains, stay, go_x, go_y, wide, adv_ref, last, corner=None):
    tiles = lane_tiles(bins)
    columns = inner.shape[0] + 2
    rows = edge.shape[0] - 2 * DEPTH
    used = rows if last else edge.shape[0]
    near, mine = (0, 0) if west else (columns - 3, columns - 1)
    across = across_edge(halo, [inner[near, :, lanes_of(t)] for t in range(tiles)], west, bins, rows, not last, corner)
    for t in range(tiles):
        here = lanes_of(t)
        adv = advect(edge[:, here], across[t], stay[:, here], go_x[:, here], go_y[0:1, here], bins, t)
        adv_ref[:used, here] = adv[:used]
    low = adv_ref[:used].astype(jnp.bfloat16)
    s, g = seas[mine, :used], gains[mine, :used]
    fresh = [None] * tiles
    keep = None
    for block in lane_blocks(tiles):
        product = jnp.dot(low, wide[:, block[0] * LANES : (block[-1] + 1) * LANES], preferred_element_type=jnp.float32)
        if keep is None:
            share = jnp.broadcast_to(product[:, -1:], (used, LANES)) * (dissipation / bins)
            keep = g - s * share
        for k, t in enumerate(block):
            fresh[t] = adv_ref[:used, lanes_of(t)] * keep + s * product[:, lanes_of(k)]
    return fresh


def lane_blocks(tiles):
    return [(t - 1, t) for t in range(tiles - 1, 0, -2)]


def inner_kernel(bins, edge_a, edge_b, inner, seas, gains, stay, go_x, go_y, wide, out, adv_ref, low_ref, keep_ref):
    tiles = lane_tiles(bins)
    count, tall = inner.shape[0], inner.shape[1]
    rows = adv_ref.shape[0] // count
    a_west = west_flag(False)
    parts = 1
    if count % parts:
        parts = 1
    for part in range(parts):
        group = range(part * count // parts, (part + 1) * count // parts)
        whole = slice(group[0] * rows, (group[-1] + 1) * rows)
        for t in range(tiles):
            here = lanes_of(t)
            found = kinds(bins, t, is_east(bins))
            for c in group:
                west = east = None
                if True in found:
                    west = inner[c - 1, :, here] if c else jnp.where(a_west, edge_a[:, here], edge_b[:, here])
                if False in found:
                    east = inner[c + 1, :, here] if c < count - 1 else jnp.where(a_west, edge_b[:, here], edge_a[:, here])
                if west is None:
                    across = east
                elif east is None:
                    across = west
                else:
                    across = jnp.where(eastward(bins, t, (tall, LANES)), west, east)
                adv = advect(inner[c, :, here], across, stay[:, here], go_x[:, here], go_y[0:1, here], bins, t)[:rows]
                adv_ref[c * rows : (c + 1) * rows, here] = adv
        low_ref[whole] = adv_ref[whole].astype(jnp.bfloat16)
        for block in lane_blocks(tiles):
            product = jnp.dot(
                low_ref[whole], wide[:, block[0] * LANES : (block[-1] + 1) * LANES], preferred_element_type=jnp.float32
            )
            for c in group:
                span = slice(c * rows, (c + 1) * rows)
                mine = slice((c - group[0]) * rows, (c - group[0] + 1) * rows)
                s = seas[c + 1, :rows]
                if block[-1] == tiles - 1:
                    share = jnp.broadcast_to(product[mine, -1:], (rows, LANES)) * (dissipation / bins)
                    keep_ref[span] = gains[c + 1, :rows] - s * share
                for k, t in enumerate(block):
                    value = adv_ref[span, lanes_of(t)] * keep_ref[span] + s * product[mine, lanes_of(k)]
                    if rows == tall:
                        out[c, :, lanes_of(t)] = value
                    else:
                        write_tile(out, (c,), bins, t, value)


def angle_table(bins, freqs):
    padded = lane_tiles(bins) * LANES
    table = np.zeros((8, padded), np.float32)
    theta = (np.arange(DIRS) + 0.5) * (2.0 * math.pi / DIRS)
    table[0, :bins] = np.repeat(0.225 * np.abs(np.cos(theta)), freqs)
    table[1, :bins] = np.repeat(0.45 * np.abs(np.sin(theta)), freqs)
    table[2, :] = -1.0
    table[2, :bins] = np.tile(np.arange(freqs), DIRS)
    return table


def steps(spectrum, sea_mask, ice_flags, wind_forcing, group_speed, coupling):
    columns, rows, bins = spectrum.shape
    tiles = lane_tiles(bins)
    padded = tiles * LANES
    tall = rows + 2 * DEPTH
    f32 = jnp.float32
    lon, lat = lax.axis_size("lon"), lax.axis_size("lat")
    lon_a, lon_b = swap_pairs(lon, 0, True), swap_pairs(lon, 1, True)
    lat_a, lat_b = swap_pairs(lat, 0, False), swap_pairs(lat, 1, False)
    vmem = pl.BlockSpec(memory_space=VMEM)
    smem = pl.BlockSpec(memory_space=SMEM)
    hbm = pl.BlockSpec(memory_space=pltpu.HBM)
    edge_shape = VMEM((tall, padded), f32)
    inner_shape = VMEM((columns - 2, tall, padded), f32)
    mask_shape = VMEM((columns, tall, LANES), f32)
    table_shape = VMEM((tall, padded), f32)

    def call(body, outs, ins, specs, scratch=(), aliases=None, flops=0, out_specs=None):
        return pl.pallas_call(
            body,
            out_shape=outs,
            in_specs=specs,
            out_specs=out_specs if out_specs is not None else jax.tree.map(lambda _: vmem, outs),
            scratch_shapes=list(scratch),
            input_output_aliases=aliases or {},
            cost_estimate=pl.CostEstimate(flops=flops, bytes_accessed=0, transcendentals=0),
            compiler_params=pltpu.CompilerParams(vmem_limit_bytes=24 * 1024 * 1024),
        )(*ins)

    send_a, send_b = call(
        functools.partial(first_kernel, bins),
        (VMEM((columns // 2 * (tiles - 1) + 1, 8, LANES), f32),) * 2,
        [pltpu.with_memory_space_constraint(x, pltpu.HBM) for x in (spectrum, sea_mask, ice_flags, wind_forcing)],
        [hbm] * 4,
        [VMEM((2, columns, 8, bins), f32), VMEM((columns, rows), sea_mask.dtype), VMEM((columns, rows), ice_flags.dtype),
         VMEM((columns, rows), f32), pltpu.SemaphoreType.DMA((5,))],
    )
    halo_b = lax.ppermute(send_b, "lat", lat_b)
    halo_a = lax.ppermute(send_a, "lat", lat_a)
    pack_own = VMEM((pack_count(rows, False), 8, LANES), f32)
    pack_shape = VMEM((pack_count(rows, True), 8, LANES), f32)
    corner_shape = VMEM((3, 8, LANES), f32)
    edge_a, edge_b, inner, seas, gains, pack_a, pack_b = call(
        functools.partial(load_kernel, bins),
        (edge_shape, edge_shape, inner_shape, mask_shape, mask_shape, pack_shape, pack_own),
        (spectrum, sea_mask, ice_flags, wind_forcing), [vmem] * 4, flops=1 << 24,
    )
    stay, go_x, go_y, wide = call(
        functools.partial(table_kernel, bins, rows),
        (table_shape, table_shape, VMEM((8, padded), f32), VMEM((padded, padded), jnp.bfloat16)),
        (group_speed, jnp.asarray(angle_table(bins, group_speed.shape[0])), coupling),
        [smem, vmem, vmem], flops=1 << 24,
    )
    edge_b, seas, gains, corner_b = call(
        functools.partial(corner_kernel, bins), (edge_shape, mask_shape, mask_shape, corner_shape),
        (go_y, halo_a, halo_b, edge_b, seas, gains), [vmem] * 6, aliases={3: 0, 4: 1, 5: 2},
    )
    edge_a, inner, seas, gains, pack_a = call(
        functools.partial(join_kernel, bins), (edge_shape, inner_shape, mask_shape, mask_shape, pack_shape),
        (halo_a, halo_b, edge_a, inner, seas, gains, pack_a), [vmem] * 7,
        aliases={2: 0, 3: 1, 4: 2, 5: 3, 6: 4},
    )
    tables = (seas, gains, stay, go_x, go_y, wide)
    for step in range(STEPS):
        last = step == STEPS - 1
        halo_b = lax.ppermute(pack_b, "lon", lon_b)
        halo_a = lax.ppermute(pack_a, "lon", lon_a)
        if step == 0:
            corner = lax.ppermute(corner_b, "lon", lon_b)
        used = rows if last else tall
        new_inner = call(
            functools.partial(inner_kernel, bins), VMEM((columns - 2, rows, bins), f32) if last else inner_shape,
            (edge_a, edge_b, inner) + tables, [vmem] * 9,
            [VMEM(((columns - 2) * used, padded), f32), VMEM(((columns - 2) * used, padded), jnp.bfloat16),
             VMEM(((columns - 2) * used, LANES), f32)],
            flops=1 << 28,
        )
        if last:
            column = VMEM((rows, bins), f32)
            scratch = [VMEM((tall, padded), f32)]
            done_b = call(
                functools.partial(ordered_late_kernel, bins, True), column,
                (new_inner, halo_b, edge_b, inner) + tables, [vmem] * 10, scratch, flops=1 << 26,
            )
            return call(
                functools.partial(last_edge_kernel, bins, False), pltpu.HBM((columns, rows, bins), f32),
                (halo_a, edge_a, inner) + tables + (new_inner, done_b), [vmem] * 11,
                scratch + [column, pltpu.SemaphoreType.DMA((3,))], flops=1 << 26, out_specs=hbm,
            )
        fresh = []
        pack_next = VMEM((pack_count(rows, False) + (1 if step < STEPS - 2 else 0), 8, LANES), f32)
        for second, halo, edge in ((False, halo_a, edge_a), (True, halo_b, edge_b)):
            body, ins = edge_kernel, (halo, edge, inner) + tables
            if step > 0:
                body, ins = ordered_edge_kernel, (new_inner,) + ins
            elif second:
                body, ins = ordered_first_kernel, (new_inner, corner) + ins
            fresh.append(call(
                functools.partial(body, bins, second), (edge_shape, pack_next),
                ins, [vmem] * len(ins), [VMEM((tall, padded), f32)], flops=1 << 26,
            ))
        inner = new_inner
        (edge_a, pack_a), (edge_b, pack_b) = fresh


def solution(mesh):
    placed = (P("lon", "lat", None), P("lon", "lat"), P("lon", "lat"), P("lon", "lat"), P(), P())
    return jax.shard_map(steps, mesh=mesh, in_specs=placed, out_specs=P("lon", "lat", None), check_vma=False)
```
